1024 devices in a mesh: ta: 4 (over x), gz: 64 (over y, z_lo, core), gy: 4 (over z_hi).
Axes of the slice: x: 4, y: 4, z: 32 (z_hi: 4, z_lo: 8; z = z_hi * 8 + z_lo), core: 2. Of those that a mesh axis runs over, the one named last changes fastest.
Arguments:
- propagator: bfloat16 [2, 4, 3, 12, 4, 64, 512], P(None, None, None, None, 'ta', 'gz', 'gy'), may hold values from -6 to 6
- links: bfloat16 [2, 3, 3, 4, 64, 512], P(None, None, None, 'ta', 'gz', 'gy'), may hold values from -2.5 to 2.5
- source_z: int32 [4, 4], replicated, may hold values from 0 to 63
- displacements: int32 [9], replicated, may hold values from 0 to 8, each once
- momenta: int32 [4], replicated, may hold values from 1 to 3
- gamma_perm: int32 [4, 4], replicated, may hold values from 0 to 3, each once within a row
- gamma_phase: int32 [4, 4], replicated, may hold values from 0 to 3
Outputs:
- correlator: float32 [4, 9, 4, 4, 2], replicated
The draws below stay inside these ranges and needn't reach their ends.
Inputs may be any that keep to these rules, and one draw needn't show every extreme that they name: `displacements`: every displacement from -4 to 4 appears exactly once. `gamma_perm`: each row is a permutation of the four spin indices.
All inputs are finite; a program needn't handle non-finite values.
Results may differ from the reference program's by a relative error of at most 0.0003.
Values may be sent and summed in bfloat16 or wider, within the bound.
A program may use at most 32 MiB of HBM per device.

```python
import math
import jax
import jax.numpy as jnp
from jax import lax

NX = 64
NG = 4
NP = 4
NSTEP = 4
NDISP = 9
NT = 4
NZ = 64
NY = 8
NYX = 512


def with_ends(array, rng, least, largest):
    longest = array.shape.index(max(array.shape))
    spots = []
    for shift in (0, 1):
        where = [jax.random.randint(jax.random.fold_in(rng, axis), (), 0, length) for axis, length in enumerate(array.shape)]
        where[longest] = (where[longest] + shift) % array.shape[longest]
        spots.append(tuple(where))
    return array.at[spots[0]].set(least).at[spots[1]].set(largest)


def block_levels(rng, dims, shards, least, high):
    level, own = 1.0, jax.random.fold_in(rng, 6)
    for axis_at, blocks in shards:
        steps = jnp.exp(jax.random.uniform(jax.random.fold_in(own, axis_at), (blocks,), jnp.float32, least / len(shards), high / len(shards)))
        level = level * jnp.repeat(steps, dims[axis_at] // blocks).reshape([-1 if axis == axis_at else 1 for axis in range(len(dims))])
    return level


def centred(own_key, extent, width, most, split=(), held_as=jnp.bfloat16):
    gain = block_levels(own_key, extent, split, -0.22, 0.18) if split else 1.0
    array = jax.random.normal(own_key, extent, jnp.float32) * width * gain
    return jnp.minimum(jnp.maximum(array, -most), most).astype(held_as)


def setup_inputs(seed: int = 0) -> dict:
    key_of = jax.random.split(jax.random.key(seed), 8)
    return {
        "propagator": centred(key_of[0], (2, 4, 3, 12, NT, NZ, NYX), 1.0, 6.0, ((4, 4), (5, 64), (6, 4))),
        "links": centred(key_of[1], (2, 3, 3, NT, NZ, NYX), 6 ** -0.5, 2.5, ((3, 4), (4, 64), (5, 4))),
        "source_z": with_ends(jax.random.randint(key_of[2], (NT, NP), 0, NZ), jax.random.fold_in(key_of[2], 1), 0, NZ - 1).astype(jnp.int32),
        "displacements": jax.random.permutation(key_of[3], NDISP).astype(jnp.int32),
        "momenta": with_ends(jax.random.randint(key_of[4], (NP,), 1, 4), jax.random.fold_in(key_of[4], 1), 1, 3).astype(jnp.int32),
        "gamma_perm": jax.vmap(lambda own: jax.random.permutation(own, 4))(jax.random.split(key_of[5], NG)).reshape((NG, 4)).astype(jnp.int32),
        "gamma_phase": with_ends(jax.random.randint(key_of[6], (NG, 4), 0, 4), jax.random.fold_in(key_of[6], 1), 0, 3).astype(jnp.int32),
    }


highest = lax.Precision.HIGHEST

def colour_apply(wilson, field_now):
    form = 'ab...,sbc...->sac...'
    real_part = jnp.einsum(form, wilson[0], field_now[0], precision=highest) - jnp.einsum(form, wilson[1], field_now[1], precision=highest)
    imag_part = jnp.einsum(form, wilson[0], field_now[1], precision=highest) + jnp.einsum(form, wilson[1], field_now[0], precision=highest)
    return jnp.stack([real_part, imag_part])

def link_product(left_link, right_link):
    form = 'ab...,bc...->ac...'
    real_part = jnp.einsum(form, left_link[0], right_link[0], precision=highest) - jnp.einsum(form, left_link[1], right_link[1], precision=highest)
    imag_part = jnp.einsum(form, left_link[0], right_link[1], precision=highest) + jnp.einsum(form, left_link[1], right_link[0], precision=highest)
    return jnp.stack([real_part, imag_part])

def dagger(link_field):
    return jnp.stack([jnp.swapaxes(link_field[0], 0, 1), -jnp.swapaxes(link_field[1], 0, 1)])

def spin_pairs(source, field_now):
    form = 'sac...,uac...->su...'
    real_part = jnp.einsum(form, source[0], field_now[0], precision=highest) + jnp.einsum(form, source[1], field_now[1], precision=highest)
    imag_part = jnp.einsum(form, source[0], field_now[1], precision=highest) - jnp.einsum(form, source[1], field_now[0], precision=highest)
    return (real_part, imag_part)

def insert(gamma_real, gamma_imag, pairs):
    pair_real, pair_imag = pairs
    form = 'gsu,su...->g...'
    real_part = jnp.einsum(form, gamma_real, pair_real, precision=highest) - jnp.einsum(form, gamma_imag, pair_imag, precision=highest)
    imag_part = jnp.einsum(form, gamma_real, pair_imag, precision=highest) + jnp.einsum(form, gamma_imag, pair_real, precision=highest)
    return (real_part, imag_part)

def gamma_tables(gamma_perm, gamma_phase):
    columns = jnp.arange(4, dtype=jnp.int32)
    hits = (gamma_perm[:, :, None] == columns[None, None, :]).astype(jnp.float32)
    real_part = (gamma_phase == 0).astype(jnp.float32) - (gamma_phase == 2).astype(jnp.float32)
    imag_part = (gamma_phase == 1).astype(jnp.float32) - (gamma_phase == 3).astype(jnp.float32)
    return (hits * real_part[:, :, None], hits * imag_part[:, :, None])

def reference(propagator, links, source_z, displacements, momenta, gamma_perm, gamma_phase):
    gamma_real, gamma_imag = gamma_tables(gamma_perm, gamma_phase)
    depth_index = jnp.arange(NZ, dtype=jnp.int32)
    turn_count = momenta[None, :, None] * (depth_index[None, None, :] - source_z[:, :, None]) % NZ
    angles = turn_count.astype(jnp.float32) * (2.0 * math.pi / NZ)
    cosine_all = jnp.cos(angles)
    sine_all = jnp.sin(angles)
    scaling = 1.0 / (24.0 * math.sqrt(NX * NY * NZ))
    unit = jnp.broadcast_to(jnp.eye(3, dtype=jnp.float32)[:, :, None, None], (3, 3, NZ, NYX))
    identity = jnp.stack([unit, jnp.zeros_like(unit)])

    def one_slice(slice_pack):
        source = slice_pack[0].astype(jnp.float32)
        link_field = slice_pack[1].astype(jnp.float32)
        cosine = slice_pack[2]
        sine_table = slice_pack[3]

        def project(field_now):
            trace_real, trace_imag = insert(gamma_real, gamma_imag, spin_pairs(source, field_now))
            line_real = lax.optimization_barrier(jnp.sum(trace_real, axis=-1))
            line_imag = lax.optimization_barrier(jnp.sum(trace_imag, axis=-1))
            real_part = jnp.dot(line_real, cosine.T, precision=highest) + jnp.dot(line_imag, sine_table.T, precision=highest)
            imag_part = jnp.dot(line_imag, cosine.T, precision=highest) - jnp.dot(line_real, sine_table.T, precision=highest)
            return jnp.stack([real_part, imag_part], axis=-1) * scaling
        results = {0: project(source)}
        wilson = identity
        for reach in range(1, NSTEP + 1):
            wilson = link_product(wilson, jnp.roll(link_field, -(reach - 1), axis=3))
            results[reach] = project(colour_apply(wilson, jnp.roll(source, -reach, axis=4)))
        wilson = identity
        for reach in range(1, NSTEP + 1):
            wilson = link_product(wilson, dagger(jnp.roll(link_field, reach, axis=3)))
            results[-reach] = project(colour_apply(wilson, jnp.roll(source, reach, axis=4)))
        return jnp.stack([results[offset] for offset in range(-NSTEP, NSTEP + 1)])
    slices = lax.map(one_slice, (jnp.moveaxis(propagator, 4, 0), jnp.moveaxis(links, 3, 0), cosine_all, sine_all))
    return jnp.take(slices, displacements.astype(jnp.int32), axis=1)
```

```python
import functools
import math

import jax
import jax.numpy as jnp
from jax import lax
from jax.experimental import pallas as pl
from jax.experimental.pallas import tpu as pltpu
from jax.sharding import Mesh
from jax.sharding import PartitionSpec as P

GZ = ("gz_0", "gz_1", "gz_2")
MESH = pl.DeviceIdType.MESH
F32 = jnp.float32
I32 = jnp.int32


def roll4(x, r):
    if r == 0:
        return x
    spin = lax.broadcasted_iota(I32, (8, 128), 0) % 4
    return jnp.where(spin < 4 - r, pltpu.roll(x, 8 - r, 0), pltpu.roll(x, 4 - r, 0))


def kernel(
    nz, scaling, s_hbm, u_hbm, source_z, displacements, momenta, perm, phase, out,
    sbuf, ubuf, left, fields, wil, table, kind, mine, slot_a, sum_a, slot_b, sum_b, slot_c,
    load_sem, send_sem, recv_sem, ready, send_a, recv_a, send_b, recv_b, send_c, recv_c,
):
    x = lax.axis_index("ta")
    gy0 = lax.axis_index("gz_0")
    lo = lax.axis_index("gz_1")
    core = lax.axis_index("gz_2")
    hi = lax.axis_index("gy")
    z = gy0 * 16 + lo * 2 + core
    r = gy0 * 2 + core
    is_root = r == lo

    def along(offset):
        w = (z + (offset + nz)) % nz
        return {"gz_0": w // 16, "gz_1": (w // 2) % 8, "gz_2": w % 2}

    def replica(dx, dr):
        q = (r + dr) % 8
        return {"ta": (x + dx) % 4, "gz_0": q // 2, "gz_2": q % 2}

    load_s = pltpu.make_async_copy(s_hbm, sbuf.at[0], load_sem.at[0])
    load_u = pltpu.make_async_copy(u_hbm, ubuf.at[0], load_sem.at[1])
    load_s.start()
    load_u.start()

    barrier = pltpu.get_barrier_semaphore()
    for offset in (-2, -1, 1, 2):
        pl.semaphore_signal(barrier, inc=1, device_id=along(offset), device_id_type=MESH)

    @pl.loop(1, 32)
    def _(n):
        pl.semaphore_signal(barrier, inc=1, device_id=replica(n // 8, n % 8), device_id_type=MESH)

    lower = (hi + jnp.where(lo >= r, 0, 3)) % 4
    for step in (0, 1):
        seat = jnp.where(is_root, (hi + 3 + 2 * step) % 4, (lower + step) % 4)
        pl.semaphore_signal(barrier, inc=1, device_id={"gy": seat, "gz_1": r}, device_id_type=MESH)

    sub = lax.broadcasted_iota(I32, (8, 128), 0)
    lane = lax.broadcasted_iota(I32, (8, 128), 1)
    u_id = sub % 4
    g_id = (lane % 32) // 8
    p_id = (lane // 2) % 4
    c_id = lane % 2
    perm_t = jnp.zeros((8, 128), I32)
    phase_t = jnp.zeros((8, 128), I32)
    for g in range(4):
        for s in range(4):
            here = (g_id == g) & (u_id == s)
            perm_t = jnp.where(here, perm[g, s], perm_t)
            phase_t = jnp.where(here, phase[g, s], phase_t)
    mom = jnp.zeros((8, 128), I32)
    src = jnp.zeros((8, 128), I32)
    for p in range(4):
        mom = jnp.where(p_id == p, momenta[p], mom)
        src = jnp.where(p_id == p, source_z[x, p], src)
    for m in range(3):
        j_id = m * 4 + lane // 32
        shift = jnp.zeros((8, 128), I32)
        for j in range(4 * m, min(4 * m + 4, 9)):
            shift = jnp.where(j_id == j, displacements[j] - 4, shift)
        neg = shift < 0
        k_id = jnp.where(neg, -shift, shift)
        at = z - jnp.where(k_id >= 3, 2, 0) + jnp.where(neg, k_id, 0)
        turns = (mom * (at - src)) & (nz - 1)
        angle = turns.astype(F32) * (2.0 * math.pi / nz)
        cosine = jnp.cos(angle) * scaling
        sine = jnp.sin(angle) * scaling
        kind[m] = k_id
        for rr in range(4):
            s_id = (u_id + rr) % 4
            perm_r = pltpu.roll(perm_t, 8 - rr, 0) if rr else perm_t
            phase_r = pltpu.roll(phase_t, 8 - rr, 0) if rr else phase_t
            match = jnp.where(neg, perm_t, perm_r) == jnp.where(neg, s_id, u_id)
            power = jnp.where(neg, phase_t, phase_r)
            for ri in range(2):
                if ri == 0:
                    turn = jnp.where(c_id == 0, 0, 3)
                else:
                    turn = jnp.where(c_id == 0, jnp.where(neg, 3, 1), jnp.where(neg, 2, 0))
                h = (power + turn) & 3
                value = jnp.where((h & 1) == 1, sine, cosine)
                value = jnp.where(h >= 2, -value, value)
                table[m, rr * 2 + ri] = jnp.where(match & (j_id < 9), value, 0.0)

    load_s.wait()
    load_u.wait()

    @pl.loop(0, 18)
    def _(n):
        rows = sbuf[0, pl.ds(pl.multiple_of(n * 16, 16), 16), :].astype(F32)
        for half in range(2):
            for rr in range(4):
                left[rr, 2 * n + half] = roll4(rows[half * 8 : half * 8 + 8], rr)

    pl.semaphore_wait(barrier, 35 + jnp.where(is_root, 16, 0))

    def to(buf, n, dst, offset):
        return pltpu.make_async_remote_copy(
            src_ref=buf.at[0], dst_ref=buf.at[dst], send_sem=send_sem.at[n], recv_sem=recv_sem.at[n],
            device_id=along(offset), device_id_type=MESH,
        )

    halo = [
        to(sbuf, 0, 2, -2), to(sbuf, 1, 1, -1), to(sbuf, 2, 3, 2),
        to(ubuf, 3, 1, -1), to(ubuf, 4, 2, 1), to(ubuf, 5, 3, 2),
    ]
    for n in (3, 4, 5, 0, 1, 2):
        halo[n].start()

    @pl.when(is_root)
    def _():
        for step in (1, 3):
            pl.semaphore_signal(ready, inc=1, device_id={"gy": (hi + step) % 4}, device_id_type=MESH)

    def link(slot):
        block = ubuf[slot].astype(F32)
        return [
            [tuple(jnp.broadcast_to(block[3 * a + b, ri : ri + 1, :], (8, 128)) for ri in range(2)) for b in range(3)]
            for a in range(3)
        ]

    def product(one, two):
        def entry(a, c):
            re = im = None
            for b in range(3):
                (pr, pi), (qr, qi) = one[a][b], two[b][c]
                r2, i2 = pr * qr - pi * qi, pr * qi + pi * qr
                re, im = (r2, i2) if b == 0 else (re + r2, im + i2)
            return re, im

        return [[entry(a, c) for c in range(3)] for a in range(3)]

    for n in (3, 4, 5):
        halo[n].wait()
    base = link(0)
    ahead = product(base, link(1))
    back = product(link(3), link(2))
    for a in range(3):
        for b in range(3):
            for ri in range(2):
                wil[0, (a * 3 + b) * 2 + ri] = base[a][b][ri]
                wil[1, (a * 3 + b) * 2 + ri] = ahead[a][b][ri]
                wil[2, (a * 3 + b) * 2 + ri] = back[b][a][ri] if ri == 0 else -back[b][a][ri]

    def transport(slot, line):
        @pl.loop(0, 3)
        def _(q):
            got = [
                [sbuf[slot, pl.ds(pl.multiple_of((ri * 3 + b) * 48 + q * 16, 16), 16), :].astype(F32) for ri in range(2)]
                for b in range(3)
            ]
            for half in range(2):
                part = [[v[half * 8 : half * 8 + 8] for v in pair] for pair in got]
                for a in range(3):
                    re = im = None
                    for b in range(3):
                        wr, wi = wil[line, (a * 3 + b) * 2], wil[line, (a * 3 + b) * 2 + 1]
                        vr, vi = part[b]
                        r2, i2 = wr * vr - wi * vi, wr * vi + wi * vr
                        re, im = (r2, i2) if b == 0 else (re + r2, im + i2)
                    fields[line, a * 6 + q * 2 + half] = re
                    fields[line, 18 + a * 6 + q * 2 + half] = im

    halo[1].wait()
    transport(1, 0)
    halo[0].wait()
    transport(2, 1)
    halo[2].wait()
    transport(3, 2)

    kinds = [kind[m] for m in range(3)]
    total = [jnp.zeros((8, 128), F32) for _ in range(3)]
    for rr in range(4):
        def add(n, acc):
            acc = list(acc)
            for a in range(3):
                re_at, im_at = n + 6 * a, 18 + n + 6 * a
                sr, si = left[rr, re_at], left[rr, im_at]
                lr, li = roll4(fields[2, re_at], rr), roll4(fields[2, im_at], rr)
                right = [
                    (left[0, re_at], left[0, im_at]),
                    (fields[0, re_at], fields[0, im_at]),
                    (fields[1, re_at], fields[1, im_at]),
                ]
                for k, ((ar, ai), (br, bi)) in enumerate(
                    [((sr, si), right[0]), ((sr, si), right[1]), ((sr, si), right[2]), ((lr, li), right[1]), ((lr, li), right[2])]
                ):
                    acc[2 * k] = acc[2 * k] + (ar * br + ai * bi)
                    acc[2 * k + 1] = acc[2 * k + 1] + (ar * bi - ai * br)
            return tuple(acc)

        sums = lax.fori_loop(0, 6, add, tuple(jnp.zeros((8, 128), F32) for _ in range(10)))
        for ri in range(2):
            lines = [jnp.broadcast_to(jnp.sum(sums[2 * k + ri], axis=1, keepdims=True), (8, 128)) for k in range(5)]
            for m in range(3):
                value = lines[0]
                for k in range(1, 5):
                    value = jnp.where(kinds[m] == k, lines[k], value)
                total[m] = total[m] + table[m, rr * 2 + ri] * value
    flat = [jnp.sum(t, axis=0, keepdims=True) for t in total]
    flat.append(jnp.zeros((1, 128), F32))
    partial = jnp.concatenate(flat, axis=0)

    mine[...] = partial

    def to_root(slot):
        return pltpu.make_async_remote_copy(
            src_ref=mine, dst_ref=slot_a.at[slot], send_sem=send_a, recv_sem=recv_a.at[slot],
            device_id={"gz_0": lo // 2, "gz_2": lo % 2}, device_id_type=MESH,
        )

    def to_column(step):
        seat = (hi * 8 + lo + step) % 32
        return pltpu.make_async_remote_copy(
            src_ref=sum_a, dst_ref=slot_b.at[hi], send_sem=send_b.at[step], recv_sem=recv_b.at[hi],
            device_id={"gy": seat // 8, "gz_1": seat % 8}, device_id_type=MESH,
        )

    @pl.when(jnp.logical_not(is_root))
    def _():
        to_root(r).start()

    @pl.when(is_root)
    def _():
        acc = None
        slot_a[r] = partial
        for q in range(8):
            @pl.when(q != r)
            def _():
                to_root(q).wait_recv()
        for q in range(8):
            acc = slot_a[q] if q == 0 else acc + slot_a[q]
        sum_a[...] = acc
        slot_b[hi] = acc
        pl.semaphore_wait(ready, 2)

        @pl.loop(1, 32)
        def _(step):
            to_column(step).start()

    for q in range(4):
        @pl.when(jnp.logical_not(is_root & (hi == q)))
        def _():
            pltpu.make_async_remote_copy(
                src_ref=sum_a, dst_ref=slot_b.at[q], send_sem=send_b.at[0], recv_sem=recv_b.at[q],
                device_id={"gy": (hi + 1) % 4}, device_id_type=MESH,
            ).wait_recv()
    acc = slot_b[0]
    for q in range(1, 4):
        acc = acc + slot_b[q]
    sum_b[...] = acc

    def to_plane(n):
        return pltpu.make_async_remote_copy(
            src_ref=sum_b, dst_ref=slot_c.at[x * 8 + r], send_sem=send_c.at[n], recv_sem=recv_c.at[x * 8 + r],
            device_id=replica(n // 8, n % 8), device_id_type=MESH,
        )

    @pl.loop(1, 32)
    def _(n):
        to_plane(n).start()

    slot_c[x * 8 + r] = acc

    @pl.loop(1, 32)
    def _(n):
        other = ((x + n // 8) % 4) * 8 + (r + n % 8) % 8
        pltpu.make_async_remote_copy(
            src_ref=sum_b, dst_ref=slot_c.at[other], send_sem=send_c.at[n], recv_sem=recv_c.at[other],
            device_id=replica(n // 8, n % 8), device_id_type=MESH,
        ).wait_recv()

    slices = []
    for t in range(4):
        acc = slot_c[8 * t]
        for q in range(1, 8):
            acc = acc + slot_c[8 * t + q]
        slices.append(acc)
    quarter = lax.broadcasted_iota(I32, (4, 128), 1) // 32
    for q in range(4):
        rows = slices[0] if q == 0 else pltpu.roll(slices[0], (128 - 32 * q) % 128, 1)
        for t in range(1, 4):
            turned = slices[t] if t == q else pltpu.roll(slices[t], (128 + 32 * (t - q)) % 128, 1)
            rows = jnp.where(quarter == t, turned, rows)
        for m in range(3):
            if m * 4 + q < 9:
                out[m * 4 + q : m * 4 + q + 1, :] = rows[m : m + 1, :]

    @pl.when(jnp.logical_not(is_root))
    def _():
        to_root(r).wait_send()

    @pl.when(is_root)
    def _():
        @pl.loop(1, 32)
        def _(step):
            to_column(step).wait_send()

    @pl.loop(1, 32)
    def _(n):
        to_plane(n).wait_send()


def body(propagator, links, source_z, displacements, momenta, gamma_perm, gamma_phase):
    nz = lax.axis_size(GZ)
    sites_total = propagator.shape[6] * lax.axis_size("gy") * nz
    scaling = 1.0 / (24.0 * math.sqrt(sites_total))
    prop = jnp.transpose(propagator, (0, 2, 3, 1, 4, 5, 6)).reshape(288, 128)
    link = jnp.transpose(links, (1, 2, 0, 3, 4, 5)).reshape(9, 2, 128)
    smem = pl.BlockSpec(memory_space=pltpu.SMEM)
    hbm = pl.BlockSpec(memory_space=pl.ANY)
    dma = pltpu.SemaphoreType.DMA
    out = pl.pallas_call(
        functools.partial(kernel, nz, scaling),
        out_shape=jax.ShapeDtypeStruct((9, 128), F32),
        in_specs=[hbm, hbm, smem, smem, smem, smem, smem],
        out_specs=pl.BlockSpec(memory_space=pltpu.VMEM),
        scratch_shapes=[
            pltpu.VMEM((4, 288, 128), jnp.bfloat16),
            pltpu.VMEM((4, 9, 2, 128), jnp.bfloat16),
            pltpu.VMEM((4, 36, 8, 128), F32),
            pltpu.VMEM((3, 36, 8, 128), F32),
            pltpu.VMEM((3, 18, 8, 128), F32),
            pltpu.VMEM((3, 8, 8, 128), F32),
            pltpu.VMEM((3, 8, 128), I32),
            pltpu.VMEM((4, 128), F32),
            pltpu.VMEM((8, 4, 128), F32),
            pltpu.VMEM((4, 128), F32),
            pltpu.VMEM((4, 4, 128), F32),
            pltpu.VMEM((4, 128), F32),
            pltpu.VMEM((32, 4, 128), F32),
            dma((2,)),
            dma((6,)),
            dma((6,)),
            pltpu.SemaphoreType.REGULAR,
            dma,
            dma((8,)),
            dma((32,)),
            dma((4,)),
            dma((32,)),
            dma((32,)),
        ],
        compiler_params=pltpu.CompilerParams(collective_id=0, has_side_effects=True),
    )(prop, link, source_z, displacements, momenta, gamma_perm, gamma_phase)
    return jnp.transpose(out.reshape(9, 4, 4, 4, 2), (1, 0, 2, 3, 4))


def solution(mesh):
    torus = Mesh(
        mesh.devices.reshape(mesh.shape["ta"], 4, 8, 2, mesh.shape["gy"]),
        ("ta", "gz_0", "gz_1", "gz_2", "gy"),
    )
    in_specs = (
        P(None, None, None, None, "ta", GZ, "gy"),
        P(None, None, None, "ta", GZ, "gy"),
        P(),
        P(),
        P(),
        P(),
        P(),
    )
    return jax.shard_map(body, mesh=torus, in_specs=in_specs, out_specs=P(), check_vma=False)
```

```python
import functools
import math

import jax
import jax.numpy as jnp
from jax import lax
from jax.experimental import pallas as pl
from jax.experimental.pallas import tpu as pltpu
from jax.sharding import Mesh
from jax.sharding import PartitionSpec as P

GZ = ("gz_0", "gz_1", "gz_2")
MESH = pl.DeviceIdType.MESH
F32 = jnp.float32
I32 = jnp.int32


def roll4(x, r):
    if r == 0:
        return x
    spin = lax.broadcasted_iota(I32, (8, 128), 0) % 4
    return jnp.where(spin < 4 - r, pltpu.roll(x, 8 - r, 0), pltpu.roll(x, 4 - r, 0))


ORDER = (1, 2, 3, 4, 5, 6, 7, 8, 31, 30, 29, 28, 27, 26, 25, 24, 9, 10, 11, 12, 13, 14, 15, 23, 22, 21, 20, 19, 18, 17, 16)


def kernel(
    nz, scaling, s_hbm, u_hbm, *refs,
):
    ints_hbm, out, ints = refs[:5], refs[5], refs[6:11]
    sbuf, ubuf, left, fields, wil, table, kind, mine, slot_b, sum_b, slot_c, final = refs[11:23]
    load_sem, send_sem, recv_sem, send_b, recv_b, send_c, recv_c, send_d, recv_d = refs[23:]
    source_z, displacements, momenta, perm, phase = ints
    x = lax.axis_index("ta")
    gy0 = lax.axis_index("gz_0")
    lo = lax.axis_index("gz_1")
    core = lax.axis_index("gz_2")
    hi = lax.axis_index("gy")
    z = gy0 * 16 + lo * 2 + core
    r = gy0 * 2 + core
    chip = hi * 8 + lo
    is_centre = chip == 0

    def along(offset):
        w = (z + (offset + nz)) % nz
        return {"gz_0": w // 16, "gz_1": (w // 2) % 8, "gz_2": w % 2}

    def replica(dx, dr):
        q = (r + dr) % 8
        return {"ta": (x + dx) % 4, "gz_0": q // 2, "gz_2": q % 2}

    loads = [pltpu.make_async_copy(s_hbm, sbuf.at[0], load_sem.at[0]), pltpu.make_async_copy(u_hbm, ubuf.at[0], load_sem.at[1])]
    loads += [pltpu.make_async_copy(ints_hbm[n], ints[n], load_sem.at[2 + n]) for n in range(5)]
    for load in loads:
        load.start()

    barrier = pltpu.get_barrier_semaphore()
    for offset in (-2, -1, 1, 2):
        pl.semaphore_signal(barrier, inc=1, device_id=along(offset), device_id_type=MESH)

    @pl.when(is_centre)
    def _():
        @pl.loop(1, 32)
        def _(n):
            pl.semaphore_signal(barrier, inc=1, device_id={"gy": n // 8, "gz_1": n % 8}, device_id_type=MESH)

        @pl.loop(1, 32)
        def _(n):
            pl.semaphore_signal(barrier, inc=1, device_id=replica(n // 8, n % 8), device_id_type=MESH)

    loads[0].wait()
    loads[1].wait()
    pl.semaphore_wait(barrier, jnp.where(is_centre, 35, 5))

    def to(buf, n, dst, offset):
        return pltpu.make_async_remote_copy(
            src_ref=buf.at[0], dst_ref=buf.at[dst], send_sem=send_sem.at[n], recv_sem=recv_sem.at[n],
            device_id=along(offset), device_id_type=MESH,
        )

    halo = [
        to(sbuf, 0, 2, -2), to(sbuf, 1, 1, -1), to(sbuf, 2, 3, 2),
        to(ubuf, 3, 1, -1), to(ubuf, 4, 2, 1), to(ubuf, 5, 3, 2),
    ]
    for n in (3, 4, 5, 0, 1, 2):
        halo[n].start()

    for load in loads[2:]:
        load.wait()

    sub = lax.broadcasted_iota(I32, (8, 128), 0)
    lane = lax.broadcasted_iota(I32, (8, 128), 1)
    u_id = sub % 4
    g_id = (lane % 32) // 8
    p_id = (lane // 2) % 4
    c_id = lane % 2
    perm_t = jnp.zeros((8, 128), I32)
    phase_t = jnp.zeros((8, 128), I32)
    for g in range(4):
        for s in range(4):
            here = (g_id == g) & (u_id == s)
            perm_t = jnp.where(here, perm[g, s], perm_t)
            phase_t = jnp.where(here, phase[g, s], phase_t)
    mom = jnp.zeros((8, 128), I32)
    src = jnp.zeros((8, 128), I32)
    for p in range(4):
        mom = jnp.where(p_id == p, momenta[p], mom)
        src = jnp.where(p_id == p, source_z[x, p], src)
    for m in range(3):
        j_id = m * 4 + lane // 32
        shift = jnp.zeros((8, 128), I32)
        for j in range(4 * m, min(4 * m + 4, 9)):
            shift = jnp.where(j_id == j, displacements[j] - 4, shift)
        neg = shift < 0
        k_id = jnp.where(neg, -shift, shift)
        at = z - jnp.where(k_id >= 3, 2, 0) + jnp.where(neg, k_id, 0)
        turns = (mom * (at - src)) & (nz - 1)
        angle = turns.astype(F32) * (2.0 * math.pi / nz)
        cosine = jnp.cos(angle) * scaling
        sine = jnp.sin(angle) * scaling
        kind[m] = k_id
        for rr in range(4):
            s_id = (u_id + rr) % 4
            perm_r = pltpu.roll(perm_t, 8 - rr, 0) if rr else perm_t
            phase_r = pltpu.roll(phase_t, 8 - rr, 0) if rr else phase_t
            match = jnp.where(neg, perm_t, perm_r) == jnp.where(neg, s_id, u_id)
            power = jnp.where(neg, phase_t, phase_r)
            for ri in range(2):
                if ri == 0:
                    turn = jnp.where(c_id == 0, 0, 3)
                else:
                    turn = jnp.where(c_id == 0, jnp.where(neg, 3, 1), jnp.where(neg, 2, 0))
                h = (power + turn) & 3
                value = jnp.where((h & 1) == 1, sine, cosine)
                value = jnp.where(h >= 2, -value, value)
                table[m, rr * 2 + ri] = jnp.where(match & (j_id < 9), value, 0.0)

    @pl.loop(0, 18)
    def _(n):
        rows = sbuf[0, pl.ds(pl.multiple_of(n * 16, 16), 16), :].astype(F32)
        for half in range(2):
            for rr in range(4):
                left[rr, 2 * n + half] = roll4(rows[half * 8 : half * 8 + 8], rr)

    def link(slot):
        block = ubuf[slot].astype(F32)
        return [
            [tuple(jnp.broadcast_to(block[3 * a + b, ri : ri + 1, :], (8, 128)) for ri in range(2)) for b in range(3)]
            for a in range(3)
        ]

    def product(one, two):
        def entry(a, c):
            re = im = None
            for b in range(3):
                (pr, pi), (qr, qi) = one[a][b], two[b][c]
                r2, i2 = pr * qr - pi * qi, pr * qi + pi * qr
                re, im = (r2, i2) if b == 0 else (re + r2, im + i2)
            return re, im

        return [[entry(a, c) for c in range(3)] for a in range(3)]

    for n in (3, 4, 5):
        halo[n].wait()
    base = link(0)
    ahead = product(base, link(1))
    back = product(link(3), link(2))
    for a in range(3):
        for b in range(3):
            for ri in range(2):
                wil[0, (a * 3 + b) * 2 + ri] = base[a][b][ri]
                wil[1, (a * 3 + b) * 2 + ri] = ahead[a][b][ri]
                wil[2, (a * 3 + b) * 2 + ri] = back[b][a][ri] if ri == 0 else -back[b][a][ri]

    def transport(slot, line):
        @pl.loop(0, 3)
        def _(q):
            got = [
                [sbuf[slot, pl.ds(pl.multiple_of((ri * 3 + b) * 48 + q * 16, 16), 16), :].astype(F32) for ri in range(2)]
                for b in range(3)
            ]
            for half in range(2):
                part = [[v[half * 8 : half * 8 + 8] for v in pair] for pair in got]
                for a in range(3):
                    re = im = None
                    for b in range(3):
                        wr, wi = wil[line, (a * 3 + b) * 2], wil[line, (a * 3 + b) * 2 + 1]
                        vr, vi = part[b]
                        r2, i2 = wr * vr - wi * vi, wr * vi + wi * vr
                        re, im = (r2, i2) if b == 0 else (re + r2, im + i2)
                    fields[line, a * 6 + q * 2 + half] = re
                    fields[line, 18 + a * 6 + q * 2 + half] = im

    halo[1].wait()
    transport(1, 0)
    halo[0].wait()
    transport(2, 1)
    halo[2].wait()
    transport(3, 2)

    kinds = [kind[m] for m in range(3)]
    total = [jnp.zeros((8, 128), F32) for _ in range(3)]
    for rr in range(4):
        def add(n, acc):
            acc = list(acc)
            for a in range(3):
                re_at, im_at = n + 6 * a, 18 + n + 6 * a
                sr, si = left[rr, re_at], left[rr, im_at]
                lr, li = roll4(fields[2, re_at], rr), roll4(fields[2, im_at], rr)
                right = [
                    (left[0, re_at], left[0, im_at]),
                    (fields[0, re_at], fields[0, im_at]),
                    (fields[1, re_at], fields[1, im_at]),
                ]
                for k, ((ar, ai), (br, bi)) in enumerate(
                    [((sr, si), right[0]), ((sr, si), right[1]), ((sr, si), right[2]), ((lr, li), right[1]), ((lr, li), right[2])]
                ):
                    acc[2 * k] = acc[2 * k] + (ar * br + ai * bi)
                    acc[2 * k + 1] = acc[2 * k + 1] + (ar * bi - ai * br)
            return tuple(acc)

        sums = lax.fori_loop(0, 6, add, tuple(jnp.zeros((8, 128), F32) for _ in range(10)))
        for ri in range(2):
            lines = [jnp.broadcast_to(jnp.sum(sums[2 * k + ri], axis=1, keepdims=True), (8, 128)) for k in range(5)]
            for m in range(3):
                value = lines[0]
                for k in range(1, 5):
                    value = jnp.where(kinds[m] == k, lines[k], value)
                total[m] = total[m] + table[m, rr * 2 + ri] * value
    flat = [jnp.sum(t, axis=0, keepdims=True) for t in total]
    flat.append(jnp.zeros((1, 128), F32))
    partial = jnp.concatenate(flat, axis=0)

    mine[...] = partial

    def to_centre():
        return pltpu.make_async_remote_copy(
            src_ref=mine, dst_ref=slot_b.at[chip], send_sem=send_b, recv_sem=recv_b.at[chip],
            device_id={"gy": 0, "gz_1": 0}, device_id_type=MESH,
        )

    def to_plane(n):
        return pltpu.make_async_remote_copy(
            src_ref=sum_b, dst_ref=slot_c.at[x * 8 + r], send_sem=send_c.at[n], recv_sem=recv_c.at[x * 8 + r],
            device_id=replica(n // 8, n % 8), device_id_type=MESH,
        )

    def to_chip(n, dst):
        return pltpu.make_async_remote_copy(
            src_ref=final, dst_ref=final, send_sem=send_d.at[n], recv_sem=recv_d,
            device_id={"gy": dst // 8, "gz_1": dst % 8}, device_id_type=MESH,
        )

    outward = (1, 2, 3, 4, 28, 8, 24, 12, 20, 16)

    @pl.when(jnp.logical_not(is_centre))
    def _():
        to_centre().start()
        to_chip(0, 0).wait_recv()

        @pl.when(chip % 4 == 0)
        def _():
            for n in range(1, 4):
                to_chip(n, chip + n).start()

    @pl.when(is_centre)
    def _():
        acc = partial
        for n in ORDER:
            pltpu.make_async_remote_copy(
                src_ref=mine, dst_ref=slot_b.at[n], send_sem=send_b, recv_sem=recv_b.at[n],
                device_id={"gy": 1}, device_id_type=MESH,
            ).wait_recv()
            acc = acc + slot_b[n]
        sum_b[...] = acc

        @pl.loop(1, 32)
        def _(n):
            to_plane(n).start()

        slot_c[x * 8 + r] = acc

        @pl.loop(1, 32)
        def _(n):
            other = ((x + n // 8) % 4) * 8 + (r + n % 8) % 8
            pltpu.make_async_remote_copy(
                src_ref=sum_b, dst_ref=slot_c.at[other], send_sem=send_c.at[n], recv_sem=recv_c.at[other],
                device_id=replica(n // 8, n % 8), device_id_type=MESH,
            ).wait_recv()

        slices = []
        for t in range(4):
            acc = slot_c[8 * t]
            for q in range(1, 8):
                acc = acc + slot_c[8 * t + q]
            slices.append(acc)
        quarter = lax.broadcasted_iota(I32, (4, 128), 1) // 32
        for q in range(4):
            rows = slices[0] if q == 0 else pltpu.roll(slices[0], (128 - 32 * q) % 128, 1)
            for t in range(1, 4):
                turned = slices[t] if t == q else pltpu.roll(slices[t], (128 + 32 * (t - q)) % 128, 1)
                rows = jnp.where(quarter == t, turned, rows)
            for m in range(3):
                if m * 4 + q < 9:
                    final[m * 4 + q] = rows[m : m + 1, :]
        for n, dst in enumerate(outward):
            to_chip(n, dst).start()

    for j in range(9):
        out[j : j + 1, :] = final[j]

    @pl.when(jnp.logical_not(is_centre))
    def _():
        to_centre().wait_send()

        @pl.when(chip % 4 == 0)
        def _():
            for n in range(1, 4):
                to_chip(n, chip + n).wait_send()

    @pl.when(is_centre)
    def _():
        @pl.loop(1, 32)
        def _(n):
            to_plane(n).wait_send()

        for n, dst in enumerate(outward):
            to_chip(n, dst).wait_send()


def body(propagator, links, source_z, displacements, momenta, gamma_perm, gamma_phase):
    nz = lax.axis_size(GZ)
    sites_total = propagator.shape[6] * lax.axis_size("gy") * nz
    scaling = 1.0 / (24.0 * math.sqrt(sites_total))
    prop = jnp.transpose(propagator, (0, 2, 3, 1, 4, 5, 6)).reshape(288, 128)
    link = jnp.transpose(links, (1, 2, 0, 3, 4, 5)).reshape(9, 2, 128)
    hbm = pl.BlockSpec(memory_space=pl.ANY)
    dma = pltpu.SemaphoreType.DMA
    out = pl.pallas_call(
        functools.partial(kernel, nz, scaling),
        out_shape=jax.ShapeDtypeStruct((9, 128), F32),
        in_specs=[hbm] * 7,
        out_specs=pl.BlockSpec(memory_space=pltpu.VMEM),
        scratch_shapes=[
            pltpu.SMEM((4, 4), I32),
            pltpu.SMEM((9,), I32),
            pltpu.SMEM((4,), I32),
            pltpu.SMEM((4, 4), I32),
            pltpu.SMEM((4, 4), I32),
            pltpu.VMEM((4, 288, 128), jnp.bfloat16),
            pltpu.VMEM((4, 9, 2, 128), jnp.bfloat16),
            pltpu.VMEM((4, 36, 8, 128), F32),
            pltpu.VMEM((3, 36, 8, 128), F32),
            pltpu.VMEM((3, 18, 8, 128), F32),
            pltpu.VMEM((3, 8, 8, 128), F32),
            pltpu.VMEM((3, 8, 128), I32),
            pltpu.VMEM((4, 128), F32),
            pltpu.VMEM((32, 4, 128), F32),
            pltpu.VMEM((4, 128), F32),
            pltpu.VMEM((32, 4, 128), F32),
            pltpu.VMEM((9, 1, 128), F32),
            dma((7,)),
            dma((6,)),
            dma((6,)),
            dma,
            dma((32,)),
            dma((32,)),
            dma((32,)),
            dma((10,)),
            dma,
        ],
        compiler_params=pltpu.CompilerParams(collective_id=0, has_side_effects=True),
    )(prop, link, source_z, displacements, momenta, gamma_perm, gamma_phase)
    return jnp.transpose(out.reshape(9, 4, 4, 4, 2), (1, 0, 2, 3, 4))


def solution(mesh):
    torus = Mesh(
        mesh.devices.reshape(mesh.shape["ta"], 4, 8, 2, mesh.shape["gy"]),
        ("ta", "gz_0", "gz_1", "gz_2", "gy"),
    )
    in_specs = (
        P(None, None, None, None, "ta", GZ, "gy"),
        P(None, None, None, "ta", GZ, "gy"),
        P(),
        P(),
        P(),
        P(),
        P(),
    )
    return jax.shard_map(body, mesh=torus, in_specs=in_specs, out_specs=P(), check_vma=False)
```

```python
import functools
import math

import jax
import jax.numpy as jnp
from jax import lax
from jax.experimental import pallas as pl
from jax.experimental.pallas import tpu as pltpu
from jax.sharding import Mesh
from jax.sharding import PartitionSpec as P

GZ = ("gz_0", "gz_1", "gz_2")
MESH = pl.DeviceIdType.MESH
F32 = jnp.float32
I32 = jnp.int32


def roll4(x, r):
    if r == 0:
        return x
    spin = lax.broadcasted_iota(I32, (8, 128), 0) % 4
    return jnp.where(spin < 4 - r, pltpu.roll(x, 8 - r, 0), pltpu.roll(x, 4 - r, 0))


ORDER = (1, 2, 3, 4, 5, 6, 7, 8, 31, 30, 29, 28, 27, 26, 25, 24, 9, 10, 11, 12, 13, 14, 15, 23, 22, 21, 20, 19, 18, 17, 16)


def kernel(
    nz, scaling, s_hbm, u_hbm, *refs,
):
    ints_hbm, out, ints = refs[:5], refs[5], refs[6:11]
    sbuf, ubuf, left, fields, wil, table, kind, mine, slot_b, sum_b, slot_c, final, xbuf, xlink, xfields, xwil, rot = refs[11:28]
    load_sem, send_sem, recv_sem, send_b, recv_b, send_c, recv_c, send_d, recv_d, send_x, recv_x, recv_l = refs[28:]
    source_z, displacements, momenta, perm, phase = ints
    x = lax.axis_index("ta")
    gy0 = lax.axis_index("gz_0")
    lo = lax.axis_index("gz_1")
    core = lax.axis_index("gz_2")
    hi = lax.axis_index("gy")
    z = gy0 * 16 + lo * 2 + core
    r = gy0 * 2 + core
    chip = hi * 8 + lo
    is_centre = chip == 0
    place = lo * 2 + core
    at_end = hi >= 2
    is_member = (place >= 12) | (place < 4)
    member = jnp.where(place >= 12, place - 12, place + 4)
    row_a = jnp.where(place >= 12, gy0, (gy0 + 3) % 4)
    is_worker = jnp.where(at_end, place >= 13, place < 3)
    first = jnp.where(at_end, 13, 0)

    def seat(row, spot):
        return {"gz_0": row % 4, "gz_1": spot // 2, "gz_2": spot % 2}

    def along(offset):
        w = (z + (offset + nz)) % nz
        return {"gz_0": w // 16, "gz_1": (w // 2) % 8, "gz_2": w % 2}

    def replica(dx, dr):
        q = (r + dr) % 8
        return {"ta": (x + dx) % 4, "gz_0": q // 2, "gz_2": q % 2}

    loads = [pltpu.make_async_copy(s_hbm, sbuf.at[0], load_sem.at[0]), pltpu.make_async_copy(u_hbm, ubuf.at[0], load_sem.at[1])]
    loads += [pltpu.make_async_copy(ints_hbm[n], ints[n], load_sem.at[2 + n]) for n in range(5)]
    for load in loads:
        load.start()

    barrier = pltpu.get_barrier_semaphore()
    heard = jnp.where(is_centre, 31, 1) + jnp.where(is_member, 3, 0) - jnp.where(is_worker, 1, 0)
    for offset in (-2, -1, 1, 2):
        inside = (place + offset >= 0) & (place + offset < 16)
        heard = heard + jnp.where(inside, 1, 0)

        @pl.when(inside)
        def _():
            pl.semaphore_signal(barrier, inc=1, device_id=along(offset), device_id_type=MESH)

    for n in range(8):
        @pl.when(is_worker & (n != member))
        def _():
            other = seat(row_a, 12 + n) if n < 4 else seat(row_a + 1, n - 4)
            pl.semaphore_signal(barrier, inc=1, device_id=other, device_id_type=MESH)

    @pl.when(is_centre)
    def _():
        @pl.loop(1, 32)
        def _(n):
            pl.semaphore_signal(barrier, inc=1, device_id={"gy": n // 8, "gz_1": n % 8}, device_id_type=MESH)

        @pl.loop(1, 32)
        def _(n):
            pl.semaphore_signal(barrier, inc=1, device_id=replica(n // 8, n % 8), device_id_type=MESH)

    loads[0].wait()
    loads[1].wait()
    pl.semaphore_wait(barrier, heard)

    def to(buf, n, dst, offset):
        return pltpu.make_async_remote_copy(
            src_ref=buf.at[0], dst_ref=buf.at[dst], send_sem=send_sem.at[n], recv_sem=recv_sem.at[n],
            device_id=along(offset), device_id_type=MESH,
        )

    halo = [
        to(sbuf, 0, 2, -2), to(sbuf, 1, 1, -1), to(sbuf, 2, 3, 2),
        to(ubuf, 3, 1, -1), to(ubuf, 4, 2, 1), to(ubuf, 5, 3, 2),
    ]
    offsets = (-2, -1, 2, -1, 1, 2)
    goes = [(place + o >= 0) & (place + o < 16) for o in offsets]
    comes = [(place - o >= 0) & (place - o < 16) for o in offsets]
    for n in (3, 4, 5, 1, 0, 2):
        pl.when(goes[n])(halo[n].start)

    def to_worker(n):
        third, spot = n % 3, first + n % 3
        row = row_a + jnp.where(at_end, 0, 1)
        src = sbuf.at[0, :, pl.ds(third * 16, 16), :] if n < 3 else ubuf.at[0]
        dst, sem = (xbuf, recv_x) if n < 3 else (xlink, recv_l)
        near = pltpu.make_async_copy(src, dst.at[member], sem.at[member])
        far = pltpu.make_async_remote_copy(
            src_ref=src, dst_ref=dst.at[member], send_sem=send_x.at[n], recv_sem=sem.at[member],
            device_id=seat(row, spot), device_id_type=MESH,
        )
        return near, far, is_member & (place == spot), is_member & (place != spot)

    for n in (3, 4, 5, 0, 1, 2):
        near, far, here, there = to_worker(n)
        pl.when(here)(near.start)
        pl.when(there)(far.start)

    for load in loads[2:]:
        load.wait()

    sub = lax.broadcasted_iota(I32, (8, 128), 0)
    lane = lax.broadcasted_iota(I32, (8, 128), 1)
    u_id = sub % 4
    g_id = (lane % 32) // 8
    p_id = (lane // 2) % 4
    c_id = lane % 2
    perm_t = jnp.zeros((8, 128), I32)
    phase_t = jnp.zeros((8, 128), I32)
    for g in range(4):
        for s in range(4):
            here = (g_id == g) & (u_id == s)
            perm_t = jnp.where(here, perm[g, s], perm_t)
            phase_t = jnp.where(here, phase[g, s], phase_t)
    mom = jnp.zeros((8, 128), I32)
    src = jnp.zeros((8, 128), I32)
    for p in range(4):
        mom = jnp.where(p_id == p, momenta[p], mom)
        src = jnp.where(p_id == p, source_z[x, p], src)
    corner = jnp.where(at_end, 12 - place, -4 - place)
    for n in range(5):
        turns = (mom * (corner + n if n < 4 else -2)) & (nz - 1)
        angle = turns.astype(F32) * (2.0 * math.pi / nz)
        sine = jnp.sin(angle)
        rot[n, 0] = jnp.cos(angle)
        rot[n, 1] = jnp.where(c_id == 0, sine, -sine)
    for m in range(3):
        j_id = m * 4 + lane // 32
        shift = jnp.zeros((8, 128), I32)
        for j in range(4 * m, min(4 * m + 4, 9)):
            shift = jnp.where(j_id == j, displacements[j] - 4, shift)
        neg = shift < 0
        k_id = jnp.where(neg, -shift, shift)
        at = z + jnp.where(neg, k_id, 0)
        turns = (mom * (at - src)) & (nz - 1)
        angle = turns.astype(F32) * (2.0 * math.pi / nz)
        cosine = jnp.cos(angle) * scaling
        sine = jnp.sin(angle) * scaling
        kind[m] = k_id
        for rr in range(4):
            s_id = (u_id + rr) % 4
            perm_r = pltpu.roll(perm_t, 8 - rr, 0) if rr else perm_t
            phase_r = pltpu.roll(phase_t, 8 - rr, 0) if rr else phase_t
            match = jnp.where(neg, perm_t, perm_r) == jnp.where(neg, s_id, u_id)
            power = jnp.where(neg, phase_t, phase_r)
            for ri in range(2):
                if ri == 0:
                    turn = jnp.where(c_id == 0, 0, 3)
                else:
                    turn = jnp.where(c_id == 0, jnp.where(neg, 3, 1), jnp.where(neg, 2, 0))
                h = (power + turn) & 3
                value = jnp.where((h & 1) == 1, sine, cosine)
                value = jnp.where(h >= 2, -value, value)
                table[m, rr * 2 + ri] = jnp.where(match & (j_id < 9), value, 0.0)

    @pl.loop(0, 18)
    def _(n):
        rows = sbuf[0, n // 3, pl.ds(pl.multiple_of(n % 3 * 16, 16), 16), :].astype(F32)
        for half in range(2):
            for rr in range(4):
                left[rr, 2 * n + half] = roll4(rows[half * 8 : half * 8 + 8], rr)

    def link(ref, slot):
        block = ref[slot].astype(F32)
        return [
            [tuple(jnp.broadcast_to(block[3 * a + b, ri : ri + 1, :], (8, 128)) for ri in range(2)) for b in range(3)]
            for a in range(3)
        ]

    def product(one, two):
        def entry(a, c):
            re = im = None
            for b in range(3):
                (pr, pi), (qr, qi) = one[a][b], two[b][c]
                r2, i2 = pr * qr - pi * qi, pr * qi + pi * qr
                re, im = (r2, i2) if b == 0 else (re + r2, im + i2)
            return re, im

        return [[entry(a, c) for c in range(3)] for a in range(3)]

    def keep(ref, line, matrix, dagger=False):
        for a in range(3):
            for b in range(3):
                re, im = matrix[b][a] if dagger else matrix[a][b]
                ref[line, (a * 3 + b) * 2] = re
                ref[line, (a * 3 + b) * 2 + 1] = -im if dagger else im

    def transport(load, lines, line, store):
        got = [[load(ri * 3 + b) for ri in range(2)] for b in range(3)]
        for half in range(2):
            part = [[v[half * 8 : half * 8 + 8] for v in pair] for pair in got]
            for a in range(3):
                re = im = None
                for b in range(3):
                    if lines is None:
                        re, im = part[a]
                        break
                    wr, wi = lines[line, (a * 3 + b) * 2], lines[line, (a * 3 + b) * 2 + 1]
                    vr, vi = part[b]
                    r2, i2 = wr * vr - wi * vi, wr * vi + wi * vr
                    re, im = (r2, i2) if b == 0 else (re + r2, im + i2)
                store(a, half, re, im)

    def bring(slot, line):
        @pl.loop(0, 3)
        def _(q):
            def load(block):
                return sbuf[slot, block, pl.ds(pl.multiple_of(q * 16, 16), 16), :].astype(F32)

            def store(a, half, re, im):
                fields[line, a * 6 + q * 2 + half] = re
                fields[line, 18 + a * 6 + q * 2 + half] = im

            transport(load, wil, line, store)

    def clear(line):
        @pl.loop(0, 36)
        def _(n):
            fields[line, n] = jnp.zeros((8, 128), F32)

    keep(wil, 0, link(ubuf, 0))
    for n in (3, 4, 5):
        pl.when(comes[n])(halo[n].wait_recv)

    @pl.when(comes[1])
    def _():
        halo[1].wait_recv()
        bring(1, 0)

    @pl.when(comes[0])
    def _():
        keep(wil, 1, product(link(ubuf, 0), link(ubuf, 1)))
        halo[0].wait_recv()
        bring(2, 1)

    @pl.when(comes[2])
    def _():
        keep(wil, 2, product(link(ubuf, 3), link(ubuf, 2)), dagger=True)
        halo[2].wait_recv()
        bring(3, 2)

    for line, n in ((0, 1), (1, 0), (2, 2)):
        @pl.when(jnp.logical_not(comes[n]))
        def _():
            clear(line)

    kinds = [kind[m] for m in range(3)]

    def lane_sum(v):
        return jnp.broadcast_to(jnp.sum(v, axis=1, keepdims=True), (8, 128))

    def pick(lines, m):
        value = jnp.zeros((8, 128), F32)
        for k, line in lines.items():
            value = jnp.where(kinds[m] == k, line, value)
        return value

    def turned(total, n):
        rows = jnp.concatenate([jnp.sum(t, axis=0, keepdims=True) for t in total] + [jnp.zeros((1, 128), F32)], axis=0)
        if n is None:
            return rows
        odd = lax.broadcasted_iota(I32, (4, 128), 1) % 2 == 1
        swapped = jnp.where(odd, pltpu.roll(rows, 1, 1), pltpu.roll(rows, 127, 1))
        return rows * rot[n, 0][0:4] + swapped * rot[n, 1][0:4]

    def mac(acc, n, a_pair, b_pair):
        (ar, ai), (br, bi) = a_pair, b_pair
        acc[2 * n] = acc[2 * n] + (ar * br + ai * bi)
        acc[2 * n + 1] = acc[2 * n + 1] + (ar * bi - ai * br)

    total = [[jnp.zeros((8, 128), F32) for _ in range(3)] for _ in range(2)]
    for rr in range(4):
        def add(n, acc):
            acc = list(acc)
            for a in range(3):
                re_at, im_at = n + 6 * a, 18 + n + 6 * a
                here = (left[rr, re_at], left[rr, im_at])
                behind = (roll4(fields[2, re_at], rr), roll4(fields[2, im_at], rr))
                one, two = (fields[0, re_at], fields[0, im_at]), (fields[1, re_at], fields[1, im_at])
                mac(acc, 0, here, (left[0, re_at], left[0, im_at]))
                mac(acc, 1, here, one)
                mac(acc, 2, here, two)
                mac(acc, 3, behind, one)
                mac(acc, 4, behind, two)
            return tuple(acc)

        sums = lax.fori_loop(0, 6, add, tuple(jnp.zeros((8, 128), F32) for _ in range(10)))
        for ri in range(2):
            lines = {k: lane_sum(sums[2 * k + ri]) for k in range(5)}
            for m in range(3):
                entry = table[m, rr * 2 + ri]
                total[0][m] = total[0][m] + entry * pick({k: lines[k] for k in (0, 1, 2)}, m)
                total[1][m] = total[1][m] + entry * pick({k: lines[k] for k in (3, 4)}, m)
    mine[...] = turned(total[0], None) + turned(total[1], 4)

    @pl.when(is_worker)
    def _():
        def arrived(n, dst, sem):
            return pltpu.make_async_remote_copy(
                src_ref=dst.at[n], dst_ref=dst.at[n], send_sem=send_x.at[0], recv_sem=sem.at[n],
                device_id=seat(gy0 + 1, place), device_id_type=MESH,
            )

        for n in range(8):
            arrived(n, xlink, recv_l).wait_recv()
        line = link(xlink, 3)
        keep(xwil, 3, line, dagger=True)
        for n in (2, 1, 0):
            line = product(link(xlink, n), line)
            keep(xwil, n, line, dagger=True)
        line = link(xlink, 4)
        keep(xwil, 4, line)
        for n in (5, 6):
            line = product(line, link(xlink, n))
            keep(xwil, n, line)
        for n in range(8):
            arrived(n, xbuf, recv_x).wait_recv()

            def load(block):
                return xbuf[n, block].astype(F32)

            def store(a, half, re, im):
                xfields[n, a * 2 + half] = re
                xfields[n, 6 + a * 2 + half] = im

            transport(load, None if n == 4 else xwil, n if n < 4 else n - 1, store)

        cross = [(i, j) for i in range(4) for j in range(i + 1)]
        total = [[jnp.zeros((8, 128), F32) for _ in range(3)] for _ in range(4)]
        for rr in range(4):
            def add(n, acc):
                acc = list(acc)
                ahead = [(xfields[4 + j, n], xfields[4 + j, 6 + n]) for j in range(4)]
                for i in range(4):
                    behind = (roll4(xfields[i, n], rr), roll4(xfields[i, 6 + n], rr))
                    for j in range(i + 1):
                        mac(acc, cross.index((i, j)), behind, ahead[j])
                return tuple(acc)

            sums = lax.fori_loop(0, 6, add, tuple(jnp.zeros((8, 128), F32) for _ in range(20)))
            for ri in range(2):
                lines = [lane_sum(sums[2 * n + ri]) for n in range(10)]
                for m in range(3):
                    entry = table[m, rr * 2 + ri]
                    for i in range(4):
                        at_k = {4 - i + j: lines[cross.index((i, j))] for j in range(i + 1)}
                        total[i][m] = total[i][m] + entry * pick(at_k, m)
        mine[...] = mine[...] + ((turned(total[0], 0) + turned(total[1], 1)) + (turned(total[2], 2) + turned(total[3], 3)))

    def to_centre():
        return pltpu.make_async_remote_copy(
            src_ref=mine, dst_ref=slot_b.at[chip], send_sem=send_b, recv_sem=recv_b.at[chip],
            device_id={"gy": 0, "gz_1": 0}, device_id_type=MESH,
        )

    def to_plane(n):
        return pltpu.make_async_remote_copy(
            src_ref=sum_b, dst_ref=slot_c.at[x * 8 + r], send_sem=send_c.at[n], recv_sem=recv_c.at[x * 8 + r],
            device_id=replica(n // 8, n % 8), device_id_type=MESH,
        )

    def to_chip(n, dst):
        return pltpu.make_async_remote_copy(
            src_ref=final, dst_ref=final, send_sem=send_d.at[n], recv_sem=recv_d,
            device_id={"gy": dst // 8, "gz_1": dst % 8}, device_id_type=MESH,
        )

    outward = (1, 2, 3, 4, 28, 8, 24, 12, 20, 16)

    @pl.when(jnp.logical_not(is_centre))
    def _():
        to_centre().start()
        to_chip(0, 0).wait_recv()

        @pl.when(chip % 4 == 0)
        def _():
            for n in range(1, 4):
                to_chip(n, chip + n).start()

    @pl.when(is_centre)
    def _():
        acc = mine[...]
        for n in ORDER:
            pltpu.make_async_remote_copy(
                src_ref=mine, dst_ref=slot_b.at[n], send_sem=send_b, recv_sem=recv_b.at[n],
                device_id={"gy": 1}, device_id_type=MESH,
            ).wait_recv()
            acc = acc + slot_b[n]
        sum_b[...] = acc

        @pl.loop(1, 32)
        def _(n):
            to_plane(n).start()

        slot_c[x * 8 + r] = acc

        @pl.loop(1, 32)
        def _(n):
            other = ((x + n // 8) % 4) * 8 + (r + n % 8) % 8
            pltpu.make_async_remote_copy(
                src_ref=sum_b, dst_ref=slot_c.at[other], send_sem=send_c.at[n], recv_sem=recv_c.at[other],
                device_id=replica(n // 8, n % 8), device_id_type=MESH,
            ).wait_recv()

        slices = []
        for t in range(4):
            acc = slot_c[8 * t]
            for q in range(1, 8):
                acc = acc + slot_c[8 * t + q]
            slices.append(acc)
        quarter = lax.broadcasted_iota(I32, (4, 128), 1) // 32
        for q in range(4):
            rows = slices[0] if q == 0 else pltpu.roll(slices[0], (128 - 32 * q) % 128, 1)
            for t in range(1, 4):
                turned = slices[t] if t == q else pltpu.roll(slices[t], (128 + 32 * (t - q)) % 128, 1)
                rows = jnp.where(quarter == t, turned, rows)
            for m in range(3):
                if m * 4 + q < 9:
                    final[m * 4 + q] = rows[m : m + 1, :]
        for n, dst in enumerate(outward):
            to_chip(n, dst).start()

    for j in range(9):
        out[j : j + 1, :] = final[j]

    for n in range(6):
        pl.when(goes[n])(halo[n].wait_send)
    for n in range(6):
        _, far, _, there = to_worker(n)
        pl.when(there)(far.wait_send)

    @pl.when(jnp.logical_not(is_centre))
    def _():
        to_centre().wait_send()

        @pl.when(chip % 4 == 0)
        def _():
            for n in range(1, 4):
                to_chip(n, chip + n).wait_send()

    @pl.when(is_centre)
    def _():
        @pl.loop(1, 32)
        def _(n):
            to_plane(n).wait_send()

        for n, dst in enumerate(outward):
            to_chip(n, dst).wait_send()


def body(propagator, links, source_z, displacements, momenta, gamma_perm, gamma_phase):
    nz = lax.axis_size(GZ)
    sites_total = propagator.shape[6] * lax.axis_size("gy") * nz
    scaling = 1.0 / (24.0 * math.sqrt(sites_total))
    prop = jnp.transpose(propagator, (0, 2, 3, 1, 4, 5, 6)).reshape(6, 48, 128)
    link = jnp.transpose(links, (1, 2, 0, 3, 4, 5)).reshape(9, 2, 128)
    hbm = pl.BlockSpec(memory_space=pl.ANY)
    dma = pltpu.SemaphoreType.DMA
    out = pl.pallas_call(
        functools.partial(kernel, nz, scaling),
        out_shape=jax.ShapeDtypeStruct((9, 128), F32),
        in_specs=[hbm] * 7,
        out_specs=pl.BlockSpec(memory_space=pltpu.VMEM),
        scratch_shapes=[
            pltpu.SMEM((4, 4), I32),
            pltpu.SMEM((9,), I32),
            pltpu.SMEM((4,), I32),
            pltpu.SMEM((4, 4), I32),
            pltpu.SMEM((4, 4), I32),
            pltpu.VMEM((4, 6, 48, 128), jnp.bfloat16),
            pltpu.VMEM((4, 9, 2, 128), jnp.bfloat16),
            pltpu.VMEM((4, 36, 8, 128), F32),
            pltpu.VMEM((3, 36, 8, 128), F32),
            pltpu.VMEM((3, 18, 8, 128), F32),
            pltpu.VMEM((3, 8, 8, 128), F32),
            pltpu.VMEM((3, 8, 128), I32),
            pltpu.VMEM((4, 128), F32),
            pltpu.VMEM((32, 4, 128), F32),
            pltpu.VMEM((4, 128), F32),
            pltpu.VMEM((32, 4, 128), F32),
            pltpu.VMEM((9, 1, 128), F32),
            pltpu.VMEM((8, 6, 16, 128), jnp.bfloat16),
            pltpu.VMEM((8, 9, 2, 128), jnp.bfloat16),
            pltpu.VMEM((8, 12, 8, 128), F32),
            pltpu.VMEM((7, 18, 8, 128), F32),
            pltpu.VMEM((5, 2, 8, 128), F32),
            dma((7,)),
            dma((6,)),
            dma((6,)),
            dma,
            dma((32,)),
            dma((32,)),
            dma((32,)),
            dma((10,)),
            dma,
            dma((6,)),
            dma((8,)),
            dma((8,)),
        ],
        compiler_params=pltpu.CompilerParams(collective_id=0, has_side_effects=True),
    )(prop, link, source_z, displacements, momenta, gamma_perm, gamma_phase)
    return jnp.transpose(out.reshape(9, 4, 4, 4, 2), (1, 0, 2, 3, 4))


def solution(mesh):
    torus = Mesh(
        mesh.devices.reshape(mesh.shape["ta"], 4, 8, 2, mesh.shape["gy"]),
        ("ta", "gz_0", "gz_1", "gz_2", "gy"),
    )
    in_specs = (
        P(None, None, None, None, "ta", GZ, "gy"),
        P(None, None, None, "ta", GZ, "gy"),
        P(),
        P(),
        P(),
        P(),
        P(),
    )
    return jax.shard_map(body, mesh=torus, in_specs=in_specs, out_specs=P(), check_vma=False)
```

```python
import functools
import math

import jax
import jax.numpy as jnp
from jax import lax
from jax.experimental import pallas as pl
from jax.experimental.pallas import tpu as pltpu
from jax.sharding import Mesh
from jax.sharding import PartitionSpec as P

GZ = ("gz_0", "gz_1", "gz_2")
MESH = pl.DeviceIdType.MESH
F32 = jnp.float32
I32 = jnp.int32


def roll4(x, r):
    if r == 0:
        return x
    spin = lax.broadcasted_iota(I32, (8, 128), 0) % 4
    return jnp.where(spin < 4 - r, pltpu.roll(x, 8 - r, 0), pltpu.roll(x, 4 - r, 0))


def kernel(
    nz, scaling, s_hbm, u_hbm, *refs,
):
    ints_hbm, out, ints = refs[:5], refs[5], refs[6:11]
    sbuf, ubuf, left, fields, wil, table, kind, mine, slot_b, sum_b, slot_c, final, xbuf, xlink, xfields, xwil, rot = refs[11:28]
    load_sem, send_sem, recv_sem, send_b, recv_b, send_c, recv_c, send_d, recv_d, send_x, recv_x, recv_l = refs[28:]
    source_z, displacements, momenta, perm, phase = ints
    x = lax.axis_index("ta")
    gy0 = lax.axis_index("gz_0")
    lo = lax.axis_index("gz_1")
    core = lax.axis_index("gz_2")
    hi = lax.axis_index("gy")
    z = gy0 * 16 + lo * 2 + core
    r = gy0 * 2 + core
    chip = hi * 8 + lo
    is_centre = chip == 0
    place = lo * 2 + core
    at_end = hi >= 2
    is_member = (place >= 12) | (place < 4)
    member = jnp.where(place >= 12, place - 12, place + 4)
    row_a = jnp.where(place >= 12, gy0, (gy0 + 3) % 4)
    is_worker = jnp.where(at_end, place >= 13, place < 3)
    first = jnp.where(at_end, 13, 0)

    def seat(row, spot):
        return {"gz_0": row % 4, "gz_1": spot // 2, "gz_2": spot % 2}

    def along(offset):
        w = (z + (offset + nz)) % nz
        return {"gz_0": w // 16, "gz_1": (w // 2) % 8, "gz_2": w % 2}

    def replica(dx, dr):
        q = (r + dr) % 8
        return {"ta": (x + dx) % 4, "gz_0": q // 2, "gz_2": q % 2}

    loads = [pltpu.make_async_copy(s_hbm, sbuf.at[0], load_sem.at[0]), pltpu.make_async_copy(u_hbm, ubuf.at[0], load_sem.at[1])]
    loads += [pltpu.make_async_copy(ints_hbm[n], ints[n], load_sem.at[2 + n]) for n in range(5)]
    for load in loads:
        load.start()

    barrier = pltpu.get_barrier_semaphore()
    heard = jnp.where(is_centre, 31, 1) + jnp.where(is_member, 3, 0) - jnp.where(is_worker, 1, 0)
    for offset in (-2, -1, 1, 2):
        inside = (place + offset >= 0) & (place + offset < 16)
        heard = heard + jnp.where(inside, 1, 0)

        @pl.when(inside)
        def _():
            pl.semaphore_signal(barrier, inc=1, device_id=along(offset), device_id_type=MESH)

    for n in range(8):
        @pl.when(is_worker & (n != member))
        def _():
            other = seat(row_a, 12 + n) if n < 4 else seat(row_a + 1, n - 4)
            pl.semaphore_signal(barrier, inc=1, device_id=other, device_id_type=MESH)

    @pl.when(is_centre)
    def _():
        @pl.loop(1, 32)
        def _(n):
            pl.semaphore_signal(barrier, inc=1, device_id={"gy": n // 8, "gz_1": n % 8}, device_id_type=MESH)

        @pl.loop(1, 32)
        def _(n):
            pl.semaphore_signal(barrier, inc=1, device_id=replica(n // 8, n % 8), device_id_type=MESH)

    loads[0].wait()
    loads[1].wait()
    pl.semaphore_wait(barrier, heard)

    def to(buf, n, dst, offset):
        return pltpu.make_async_remote_copy(
            src_ref=buf.at[0], dst_ref=buf.at[dst], send_sem=send_sem.at[n], recv_sem=recv_sem.at[n],
            device_id=along(offset), device_id_type=MESH,
        )

    halo = [
        to(sbuf, 0, 2, -2), to(sbuf, 1, 1, -1), to(sbuf, 2, 3, 2),
        to(ubuf, 3, 1, -1), to(ubuf, 4, 2, 1), to(ubuf, 5, 3, 2),
    ]
    offsets = (-2, -1, 2, -1, 1, 2)
    goes = [(place + o >= 0) & (place + o < 16) for o in offsets]
    comes = [(place - o >= 0) & (place - o < 16) for o in offsets]
    for n in (3, 4, 5, 1, 0, 2):
        pl.when(goes[n])(halo[n].start)

    def bulk(ref, sem):
        return pltpu.make_async_remote_copy(
            src_ref=ref, dst_ref=ref, send_sem=sem, recv_sem=sem, device_id={"gy": (hi + 1) % 4}, device_id_type=MESH
        )

    def to_worker(n):
        third, spot = n % 3, first + n % 3
        row = row_a + jnp.where(at_end, 0, 1)
        src = sbuf.at[0, :, pl.ds(third * 16, 16), :] if n < 3 else ubuf.at[0]
        dst, sem = (xbuf, recv_x) if n < 3 else (xlink, recv_l)
        side = jnp.where(place >= 12, 0, 1)
        near = pltpu.make_async_copy(src, dst.at[member], sem.at[side])
        far = pltpu.make_async_remote_copy(
            src_ref=src, dst_ref=dst.at[member], send_sem=send_x.at[n // 3], recv_sem=sem.at[side],
            device_id=seat(row, spot), device_id_type=MESH,
        )
        return near, far, is_member & (place == spot), is_member & (place != spot)

    for n in (3, 4, 5, 0, 1, 2):
        near, far, here, there = to_worker(n)
        pl.when(here)(near.start)
        pl.when(there)(far.start)

    for load in loads[2:]:
        load.wait()

    sub = lax.broadcasted_iota(I32, (8, 128), 0)
    lane = lax.broadcasted_iota(I32, (8, 128), 1)
    u_id = sub % 4
    g_id = (lane % 32) // 8
    p_id = (lane // 2) % 4
    c_id = lane % 2
    perm_t = jnp.zeros((8, 128), I32)
    phase_t = jnp.zeros((8, 128), I32)
    for g in range(4):
        for s in range(4):
            here = (g_id == g) & (u_id == s)
            perm_t = jnp.where(here, perm[g, s], perm_t)
            phase_t = jnp.where(here, phase[g, s], phase_t)
    mom = jnp.zeros((8, 128), I32)
    src = jnp.zeros((8, 128), I32)
    for p in range(4):
        mom = jnp.where(p_id == p, momenta[p], mom)
        src = jnp.where(p_id == p, source_z[x, p], src)
    corner = jnp.where(at_end, 12 - place, -4 - place)
    for n in range(5):
        turns = (mom * (corner + n if n < 4 else -2)) & (nz - 1)
        angle = turns.astype(F32) * (2.0 * math.pi / nz)
        sine = jnp.sin(angle)
        rot[n, 0] = jnp.cos(angle)
        rot[n, 1] = jnp.where(c_id == 0, sine, -sine)
    for m in range(3):
        j_id = m * 4 + lane // 32
        shift = jnp.zeros((8, 128), I32)
        for j in range(4 * m, min(4 * m + 4, 9)):
            shift = jnp.where(j_id == j, displacements[j] - 4, shift)
        neg = shift < 0
        k_id = jnp.where(neg, -shift, shift)
        at = z + jnp.where(neg, k_id, 0)
        turns = (mom * (at - src)) & (nz - 1)
        angle = turns.astype(F32) * (2.0 * math.pi / nz)
        cosine = jnp.cos(angle) * scaling
        sine = jnp.sin(angle) * scaling
        kind[m] = k_id
        for rr in range(4):
            s_id = (u_id + rr) % 4
            perm_r = pltpu.roll(perm_t, 8 - rr, 0) if rr else perm_t
            phase_r = pltpu.roll(phase_t, 8 - rr, 0) if rr else phase_t
            match = jnp.where(neg, perm_t, perm_r) == jnp.where(neg, s_id, u_id)
            power = jnp.where(neg, phase_t, phase_r)
            for ri in range(2):
                if ri == 0:
                    turn = jnp.where(c_id == 0, 0, 3)
                else:
                    turn = jnp.where(c_id == 0, jnp.where(neg, 3, 1), jnp.where(neg, 2, 0))
                h = (power + turn) & 3
                value = jnp.where((h & 1) == 1, sine, cosine)
                value = jnp.where(h >= 2, -value, value)
                table[m, rr * 2 + ri] = jnp.where(match & (j_id < 9), value, 0.0)

    @pl.loop(0, 18)
    def _(n):
        rows = sbuf[0, n // 3, pl.ds(pl.multiple_of(n % 3 * 16, 16), 16), :].astype(F32)
        for half in range(2):
            for rr in range(4):
                left[rr, 2 * n + half] = roll4(rows[half * 8 : half * 8 + 8], rr)

    kinds = [kind[m] for m in range(3)]

    def lane_sum(v):
        return jnp.broadcast_to(jnp.sum(v, axis=1, keepdims=True), (8, 128))

    def pick(lines, m):
        value = jnp.zeros((8, 128), F32)
        for k, line in lines.items():
            value = jnp.where(kinds[m] == k, line, value)
        return value

    def turned(total, n):
        rows = jnp.concatenate([jnp.sum(t, axis=0, keepdims=True) for t in total] + [jnp.zeros((1, 128), F32)], axis=0)
        if n is None:
            return rows
        odd = lax.broadcasted_iota(I32, (4, 128), 1) % 2 == 1
        swapped = jnp.where(odd, pltpu.roll(rows, 1, 1), pltpu.roll(rows, 127, 1))
        return rows * rot[n, 0][0:4] + swapped * rot[n, 1][0:4]

    def mac(acc, n, a_pair, b_pair):
        (ar, ai), (br, bi) = a_pair, b_pair
        acc[2 * n] = acc[2 * n] + (ar * br + ai * bi)
        acc[2 * n + 1] = acc[2 * n + 1] + (ar * bi - ai * br)

    total = [[jnp.zeros((8, 128), F32) for _ in range(3)] for _ in range(2)]

    def own_pairs(rr, n, acc):
        acc = list(acc)
        for a in range(3):
            re_at, im_at = n + 6 * a, 18 + n + 6 * a
            mac(acc, 0, (left[rr, re_at], left[rr, im_at]), (left[0, re_at], left[0, im_at]))
        return tuple(acc)

    def regular(kinds_at, add, groups, total):
        for rr in range(4):
            zero = tuple(jnp.zeros((8, 128), F32) for _ in range(2 * len(kinds_at)))
            sums = lax.fori_loop(0, 6, functools.partial(add, rr), zero, unroll=True)
            for ri in range(2):
                lines = {k: lane_sum(sums[2 * n + ri]) for n, k in enumerate(kinds_at)}
                for m in range(3):
                    entry = table[m, rr * 2 + ri]
                    for g, ks in enumerate(groups):
                        if ks:
                            total[g][m] = total[g][m] + entry * pick({k: lines[k] for k in ks}, m)

    regular((0,), own_pairs, ((0,), ()), total)

    def link(ref, slot):
        block = ref[slot].astype(F32)
        return [
            [tuple(jnp.broadcast_to(block[3 * a + b, ri : ri + 1, :], (8, 128)) for ri in range(2)) for b in range(3)]
            for a in range(3)
        ]

    def product(one, two):
        def entry(a, c):
            re = im = None
            for b in range(3):
                (pr, pi), (qr, qi) = one[a][b], two[b][c]
                r2, i2 = pr * qr - pi * qi, pr * qi + pi * qr
                re, im = (r2, i2) if b == 0 else (re + r2, im + i2)
            return re, im

        return [[entry(a, c) for c in range(3)] for a in range(3)]

    def keep(ref, line, matrix, dagger=False):
        for a in range(3):
            for b in range(3):
                re, im = matrix[b][a] if dagger else matrix[a][b]
                ref[line, (a * 3 + b) * 2] = re
                ref[line, (a * 3 + b) * 2 + 1] = -im if dagger else im

    def transport(load, lines, line, store):
        got = [[load(ri * 3 + b) for ri in range(2)] for b in range(3)]
        for half in range(2):
            part = [[v[half * 8 : half * 8 + 8] for v in pair] for pair in got]
            for a in range(3):
                re = im = None
                for b in range(3):
                    if lines is None:
                        re, im = part[a]
                        break
                    wr, wi = lines[line, (a * 3 + b) * 2], lines[line, (a * 3 + b) * 2 + 1]
                    vr, vi = part[b]
                    r2, i2 = wr * vr - wi * vi, wr * vi + wi * vr
                    re, im = (r2, i2) if b == 0 else (re + r2, im + i2)
                store(a, half, re, im)

    def bring(slot, line):
        @pl.loop(0, 3)
        def _(q):
            def load(block):
                return sbuf[slot, block, pl.ds(pl.multiple_of(q * 16, 16), 16), :].astype(F32)

            def store(a, half, re, im):
                fields[line, a * 6 + q * 2 + half] = re
                fields[line, 18 + a * 6 + q * 2 + half] = im

            transport(load, wil, line, store)

    def clear(line):
        @pl.loop(0, 36)
        def _(n):
            fields[line, n] = jnp.zeros((8, 128), F32)

    keep(wil, 0, link(ubuf, 0))
    for n in (3, 4, 5):
        pl.when(comes[n])(halo[n].wait_recv)

    @pl.when(comes[1])
    def _():
        halo[1].wait_recv()
        bring(1, 0)

    @pl.when(comes[0])
    def _():
        keep(wil, 1, product(link(ubuf, 0), link(ubuf, 1)))
        halo[0].wait_recv()
        bring(2, 1)

    @pl.when(comes[2])
    def _():
        keep(wil, 2, product(link(ubuf, 3), link(ubuf, 2)), dagger=True)
        halo[2].wait_recv()
        bring(3, 2)

    for line, n in ((0, 1), (1, 0), (2, 2)):
        @pl.when(jnp.logical_not(comes[n]))
        def _():
            clear(line)

    def moved_pairs(rr, n, acc):
        acc = list(acc)
        for a in range(3):
            re_at, im_at = n + 6 * a, 18 + n + 6 * a
            here = (left[rr, re_at], left[rr, im_at])
            behind = (roll4(fields[2, re_at], rr), roll4(fields[2, im_at], rr))
            one, two = (fields[0, re_at], fields[0, im_at]), (fields[1, re_at], fields[1, im_at])
            mac(acc, 0, here, one)
            mac(acc, 1, here, two)
            mac(acc, 2, behind, one)
            mac(acc, 3, behind, two)
        return tuple(acc)

    regular((1, 2, 3, 4), moved_pairs, ((1, 2), (3, 4)), total)
    mine[...] = turned(total[0], None) + turned(total[1], 4)

    @pl.when(is_worker)
    def _():
        def bring_cross(n, line):
            def load(block):
                return xbuf[n, block].astype(F32)

            def store(a, half, re, im):
                xfields[n, a * 2 + half] = re
                xfields[n, 6 + a * 2 + half] = im

            transport(load, None if line is None else xwil, line, store)

        bulk(xlink.at[pl.ds(0, 4)], recv_l.at[0]).wait_recv()
        line = link(xlink, 3)
        keep(xwil, 3, line, dagger=True)
        for n in (2, 1, 0):
            line = product(link(xlink, n), line)
            keep(xwil, n, line, dagger=True)
        bulk(xbuf.at[pl.ds(0, 4)], recv_x.at[0]).wait_recv()
        for n in range(4):
            bring_cross(n, n)
        bulk(xlink.at[pl.ds(4, 4)], recv_l.at[1]).wait_recv()
        line = link(xlink, 4)
        keep(xwil, 4, line)
        for n in (5, 6):
            line = product(line, link(xlink, n))
            keep(xwil, n, line)
        bulk(xbuf.at[pl.ds(4, 4)], recv_x.at[1]).wait_recv()
        for n in range(4, 8):
            bring_cross(n, None if n == 4 else n - 1)

        cross = [(i, j) for i in range(4) for j in range(i + 1)]
        total = [[jnp.zeros((8, 128), F32) for _ in range(3)] for _ in range(4)]
        for rr in range(4):
            def add(n, acc):
                acc = list(acc)
                ahead = [(xfields[4 + j, n], xfields[4 + j, 6 + n]) for j in range(4)]
                for i in range(4):
                    behind = (roll4(xfields[i, n], rr), roll4(xfields[i, 6 + n], rr))
                    for j in range(i + 1):
                        mac(acc, cross.index((i, j)), behind, ahead[j])
                return tuple(acc)

            sums = lax.fori_loop(0, 6, add, tuple(jnp.zeros((8, 128), F32) for _ in range(20)), unroll=True)
            for ri in range(2):
                lines = [lane_sum(sums[2 * n + ri]) for n in range(10)]
                for m in range(3):
                    entry = table[m, rr * 2 + ri]
                    for i in range(4):
                        at_k = {4 - i + j: lines[cross.index((i, j))] for j in range(i + 1)}
                        total[i][m] = total[i][m] + entry * pick(at_k, m)
        mine[...] = mine[...] + ((turned(total[0], 0) + turned(total[1], 1)) + (turned(total[2], 2) + turned(total[3], 3)))

    def to_centre():
        return pltpu.make_async_remote_copy(
            src_ref=mine, dst_ref=slot_b.at[chip], send_sem=send_b, recv_sem=recv_b,
            device_id={"gy": 0, "gz_1": 0}, device_id_type=MESH,
        )

    def to_plane(n):
        return pltpu.make_async_remote_copy(
            src_ref=sum_b, dst_ref=slot_c.at[x * 8 + r], send_sem=send_c, recv_sem=recv_c,
            device_id={"ta": n // 8, "gz_0": n % 8 // 2, "gz_2": n % 2}, device_id_type=MESH,
        )

    def to_chip(dst):
        return pltpu.make_async_remote_copy(
            src_ref=final.at[0], dst_ref=final.at[0], send_sem=send_d, recv_sem=recv_d,
            device_id={"gy": dst // 8, "gz_1": dst % 8}, device_id_type=MESH,
        )

    outward = (1, 2, 3, 4, 5, 6, 7, 28, 8, 24, 12, 20, 16)
    is_head = (chip % 4 == 0) & (chip >= 8)

    @pl.when(jnp.logical_not(is_centre))
    def _():
        to_centre().start()
        to_chip(0).wait_recv()

        @pl.when(is_head)
        def _():
            for n in range(1, 4):
                to_chip(chip + n).start()

    @pl.when(is_centre)
    def _():
        acc = mine[...]
        bulk(slot_b.at[pl.ds(1, 31)], recv_b).wait_recv()
        for n in range(1, 32):
            acc = acc + slot_b[n]
        sum_b[...] = acc

        for n in range(32):
            pl.when(x * 8 + r != n)(to_plane(n).start)
        slot_c[x * 8 + r] = acc
        bulk(slot_c.at[pl.ds(0, 31)], recv_c).wait_recv()
        slices = []
        for t in range(4):
            acc = slot_c[8 * t]
            for q in range(1, 8):
                acc = acc + slot_c[8 * t + q]
            slices.append(acc)
        quarter = lax.broadcasted_iota(I32, (4, 128), 1) // 32
        for q in range(4):
            rows = slices[0] if q == 0 else pltpu.roll(slices[0], (128 - 32 * q) % 128, 1)
            for t in range(1, 4):
                turned = slices[t] if t == q else pltpu.roll(slices[t], (128 + 32 * (t - q)) % 128, 1)
                rows = jnp.where(quarter == t, turned, rows)
            for m in range(3):
                if m * 4 + q < 9:
                    final[0, m * 4 + q] = rows[m : m + 1, :]
        for dst in outward:
            to_chip(dst).start()

    for j in range(9):
        out[j : j + 1, :] = final[0, j]

    for n in range(6):
        pl.when(goes[n])(halo[n].wait_send)
    @pl.when(is_member & is_worker)
    def _():
        bulk(sbuf.at[0, :, pl.ds(0, 32), :], send_x.at[0]).wait_send()
        bulk(ubuf.at[pl.ds(0, 2)], send_x.at[1]).wait_send()

    @pl.when(is_member & jnp.logical_not(is_worker))
    def _():
        bulk(sbuf.at[0], send_x.at[0]).wait_send()
        bulk(ubuf.at[pl.ds(0, 3)], send_x.at[1]).wait_send()

    @pl.when(jnp.logical_not(is_centre))
    def _():
        to_centre().wait_send()

        @pl.when(is_head)
        def _():
            bulk(final.at[pl.ds(0, 3)], send_d).wait_send()

    @pl.when(is_centre)
    def _():
        bulk(slot_c.at[pl.ds(0, 31)], send_c).wait_send()
        bulk(final, send_d).wait_send()


def body(propagator, links, source_z, displacements, momenta, gamma_perm, gamma_phase):
    nz = lax.axis_size(GZ)
    sites_total = propagator.shape[6] * lax.axis_size("gy") * nz
    scaling = 1.0 / (24.0 * math.sqrt(sites_total))
    prop = jnp.transpose(propagator, (0, 2, 3, 1, 4, 5, 6)).reshape(6, 48, 128)
    link = jnp.transpose(links, (1, 2, 0, 3, 4, 5)).reshape(9, 2, 128)
    hbm = pl.BlockSpec(memory_space=pl.ANY)
    dma = pltpu.SemaphoreType.DMA
    out = pl.pallas_call(
        functools.partial(kernel, nz, scaling),
        out_shape=jax.ShapeDtypeStruct((9, 128), F32),
        in_specs=[hbm] * 7,
        out_specs=pl.BlockSpec(memory_space=pltpu.VMEM),
        scratch_shapes=[
            pltpu.SMEM((4, 4), I32),
            pltpu.SMEM((9,), I32),
            pltpu.SMEM((4,), I32),
            pltpu.SMEM((4, 4), I32),
            pltpu.SMEM((4, 4), I32),
            pltpu.VMEM((4, 6, 48, 128), jnp.bfloat16),
            pltpu.VMEM((4, 9, 2, 128), jnp.bfloat16),
            pltpu.VMEM((4, 36, 8, 128), F32),
            pltpu.VMEM((3, 36, 8, 128), F32),
            pltpu.VMEM((3, 18, 8, 128), F32),
            pltpu.VMEM((3, 8, 8, 128), F32),
            pltpu.VMEM((3, 8, 128), I32),
            pltpu.VMEM((4, 128), F32),
            pltpu.VMEM((32, 4, 128), F32),
            pltpu.VMEM((4, 128), F32),
            pltpu.VMEM((32, 4, 128), F32),
            pltpu.VMEM((13, 9, 1, 128), F32),
            pltpu.VMEM((8, 6, 16, 128), jnp.bfloat16),
            pltpu.VMEM((8, 9, 2, 128), jnp.bfloat16),
            pltpu.VMEM((8, 12, 8, 128), F32),
            pltpu.VMEM((7, 18, 8, 128), F32),
            pltpu.VMEM((5, 2, 8, 128), F32),
            dma((7,)),
            dma((6,)),
            dma((6,)),
            dma,
            dma,
            dma,
            dma,
            dma,
            dma,
            dma((2,)),
            dma((2,)),
            dma((2,)),
        ],
        compiler_params=pltpu.CompilerParams(collective_id=0, has_side_effects=True),
    )(prop, link, source_z, displacements, momenta, gamma_perm, gamma_phase)
    return jnp.transpose(out.reshape(9, 4, 4, 4, 2), (1, 0, 2, 3, 4))


def solution(mesh):
    torus = Mesh(
        mesh.devices.reshape(mesh.shape["ta"], 4, 8, 2, mesh.shape["gy"]),
        ("ta", "gz_0", "gz_1", "gz_2", "gy"),
    )
    in_specs = (
        P(None, None, None, None, "ta", GZ, "gy"),
        P(None, None, None, "ta", GZ, "gy"),
        P(),
        P(),
        P(),
        P(),
        P(),
    )
    return jax.shard_map(body, mesh=torus, in_specs=in_specs, out_specs=P(), check_vma=False)
```

```python
import functools
import math

import jax
import jax.numpy as jnp
from jax import lax
from jax.experimental import pallas as pl
from jax.experimental.pallas import tpu as pltpu
from jax.sharding import Mesh
from jax.sharding import PartitionSpec as P

GZ = ("gz_0", "gz_1", "gz_2")
MESH = pl.DeviceIdType.MESH
F32 = jnp.float32
I32 = jnp.int32


def roll4(x, r):
    if r == 0:
        return x
    spin = lax.broadcasted_iota(I32, (8, 128), 0) % 4
    return jnp.where(spin < 4 - r, pltpu.roll(x, 8 - r, 0), pltpu.roll(x, 4 - r, 0))


def kernel(
    nz, scaling, s_hbm, u_hbm, *refs,
):
    ints_hbm, out, ints = refs[:5], refs[5], refs[6:11]
    sbuf, ubuf, left, fields, wil, table, kind, mine, slot_b, sum_b, slot_c, final, xbuf, xlink, xfields, xwil, rot = refs[11:28]
    load_sem, send_sem, recv_sem, send_b, recv_b, send_c, recv_c, send_d, recv_d, send_x, recv_x, recv_l = refs[28:]
    source_z, displacements, momenta, perm, phase = ints
    x = lax.axis_index("ta")
    gy0 = lax.axis_index("gz_0")
    lo = lax.axis_index("gz_1")
    core = lax.axis_index("gz_2")
    hi = lax.axis_index("gy")
    z = gy0 * 16 + lo * 2 + core
    chip = hi * 8 + lo
    is_centre = (chip == 0) & (core == 1)
    column = x * 4 + gy0
    place = lo * 2 + core
    at_end = hi >= 2
    is_member = (place >= 12) | (place < 4)
    member = jnp.where(place >= 12, place - 12, place + 4)
    row_a = jnp.where(place >= 12, gy0, (gy0 + 3) % 4)
    is_worker = jnp.where(at_end, place >= 13, place < 3)
    first = jnp.where(at_end, 13, 0)

    def seat(row, spot):
        return {"gz_0": row % 4, "gz_1": spot // 2, "gz_2": spot % 2}

    def along(offset):
        w = (z + (offset + nz)) % nz
        return {"gz_0": w // 16, "gz_1": (w // 2) % 8, "gz_2": w % 2}

    loads = [pltpu.make_async_copy(s_hbm, sbuf.at[0], load_sem.at[0]), pltpu.make_async_copy(u_hbm, ubuf.at[0], load_sem.at[1])]
    loads += [pltpu.make_async_copy(ints_hbm[n], ints[n], load_sem.at[2 + n]) for n in range(5)]
    for load in loads:
        load.start()

    barrier = pltpu.get_barrier_semaphore()
    heard = jnp.where(is_centre, 15, 1) + jnp.where(is_member, 3, 0) - jnp.where(is_worker, 1, 0)
    for offset in (-2, -1, 1, 2):
        inside = (place + offset >= 0) & (place + offset < 16)
        heard = heard + jnp.where(inside, 1, 0)

        @pl.when(inside)
        def _():
            pl.semaphore_signal(barrier, inc=1, device_id=along(offset), device_id_type=MESH)

    for n in range(8):
        @pl.when(is_worker & (n != member))
        def _():
            other = seat(row_a, 12 + n) if n < 4 else seat(row_a + 1, n - 4)
            pl.semaphore_signal(barrier, inc=1, device_id=other, device_id_type=MESH)

    @pl.when(is_centre)
    def _():
        @pl.loop(1, 64)
        def _(n):
            other = {"gy": (64 - n) // 16, "gz_1": (64 - n) // 2 % 8, "gz_2": (64 - n) % 2}
            pl.when(n != 63)(lambda: pl.semaphore_signal(barrier, inc=1, device_id=other, device_id_type=MESH))

        pl.semaphore_signal(barrier, inc=1, device_id={"gz_2": 0}, device_id_type=MESH)
        for n in range(16):
            other = {"ta": n // 4, "gz_0": n % 4}
            pl.when(column != n)(
                functools.partial(pl.semaphore_signal, barrier, inc=1, device_id=other, device_id_type=MESH)
            )

    loads[0].wait()
    loads[1].wait()
    pl.semaphore_wait(barrier, heard)

    def to(buf, n, dst, offset):
        return pltpu.make_async_remote_copy(
            src_ref=buf.at[0], dst_ref=buf.at[dst], send_sem=send_sem.at[n], recv_sem=recv_sem.at[n],
            device_id=along(offset), device_id_type=MESH,
        )

    halo = [
        to(sbuf, 0, 2, -2), to(sbuf, 1, 1, -1), to(sbuf, 2, 3, 2),
        to(ubuf, 3, 1, -1), to(ubuf, 4, 2, 1), to(ubuf, 5, 3, 2),
    ]
    offsets = (-2, -1, 2, -1, 1, 2)
    goes = [(place + o >= 0) & (place + o < 16) for o in offsets]
    comes = [(place - o >= 0) & (place - o < 16) for o in offsets]
    for n in (3, 4, 5, 1, 0, 2):
        pl.when(goes[n])(halo[n].start)

    def bulk(ref, sem):
        return pltpu.make_async_remote_copy(
            src_ref=ref, dst_ref=ref, send_sem=sem, recv_sem=sem, device_id={"gy": (hi + 1) % 4}, device_id_type=MESH
        )

    def to_worker(n):
        third, spot = n % 3, first + n % 3
        row = row_a + jnp.where(at_end, 0, 1)
        src = sbuf.at[0, :, pl.ds(third * 16, 16), :] if n < 3 else ubuf.at[0]
        dst, sem = (xbuf, recv_x) if n < 3 else (xlink, recv_l)
        side = jnp.where(place >= 12, 0, 1)
        near = pltpu.make_async_copy(src, dst.at[member], sem.at[side])
        far = pltpu.make_async_remote_copy(
            src_ref=src, dst_ref=dst.at[member], send_sem=send_x.at[n // 3], recv_sem=sem.at[side],
            device_id=seat(row, spot), device_id_type=MESH,
        )
        return near, far, is_member & (place == spot), is_member & (place != spot)

    for n in (3, 4, 5, 0, 1, 2):
        near, far, here, there = to_worker(n)
        pl.when(here)(near.start)
        pl.when(there)(far.start)

    for load in loads[2:]:
        load.wait()

    sub = lax.broadcasted_iota(I32, (8, 128), 0)
    lane = lax.broadcasted_iota(I32, (8, 128), 1)
    u_id = sub % 4
    g_id = (lane % 32) // 8
    p_id = (lane // 2) % 4
    c_id = lane % 2
    perm_t = jnp.zeros((8, 128), I32)
    phase_t = jnp.zeros((8, 128), I32)
    for g in range(4):
        for s in range(4):
            here = (g_id == g) & (u_id == s)
            perm_t = jnp.where(here, perm[g, s], perm_t)
            phase_t = jnp.where(here, phase[g, s], phase_t)
    mom = jnp.zeros((8, 128), I32)
    src = jnp.zeros((8, 128), I32)
    for p in range(4):
        mom = jnp.where(p_id == p, momenta[p], mom)
        src = jnp.where(p_id == p, source_z[x, p], src)
    corner = jnp.where(at_end, 12 - place, -4 - place)
    for n in range(5):
        turns = (mom * (corner + n if n < 4 else -2)) & (nz - 1)
        angle = turns.astype(F32) * (2.0 * math.pi / nz)
        sine = jnp.sin(angle)
        rot[n, 0] = jnp.cos(angle)
        rot[n, 1] = jnp.where(c_id == 0, sine, -sine)
    for m in range(3):
        j_id = m * 4 + lane // 32
        shift = jnp.zeros((8, 128), I32)
        for j in range(4 * m, min(4 * m + 4, 9)):
            shift = jnp.where(j_id == j, displacements[j] - 4, shift)
        neg = shift < 0
        k_id = jnp.where(neg, -shift, shift)
        at = z + jnp.where(neg, k_id, 0)
        turns = (mom * (at - src)) & (nz - 1)
        angle = turns.astype(F32) * (2.0 * math.pi / nz)
        cosine = jnp.cos(angle) * scaling
        sine = jnp.sin(angle) * scaling
        kind[m] = k_id
        for rr in range(4):
            s_id = (u_id + rr) % 4
            perm_r = pltpu.roll(perm_t, 8 - rr, 0) if rr else perm_t
            phase_r = pltpu.roll(phase_t, 8 - rr, 0) if rr else phase_t
            match = jnp.where(neg, perm_t, perm_r) == jnp.where(neg, s_id, u_id)
            power = jnp.where(neg, phase_t, phase_r)
            for ri in range(2):
                if ri == 0:
                    turn = jnp.where(c_id == 0, 0, 3)
                else:
                    turn = jnp.where(c_id == 0, jnp.where(neg, 3, 1), jnp.where(neg, 2, 0))
                h = (power + turn) & 3
                value = jnp.where((h & 1) == 1, sine, cosine)
                value = jnp.where(h >= 2, -value, value)
                table[m, rr * 2 + ri] = jnp.where(match & (j_id < 9), value, 0.0)

    @pl.loop(0, 18)
    def _(n):
        rows = sbuf[0, n // 3, pl.ds(pl.multiple_of(n % 3 * 16, 16), 16), :].astype(F32)
        for half in range(2):
            for rr in range(4):
                left[rr, 2 * n + half] = roll4(rows[half * 8 : half * 8 + 8], rr)

    kinds = [kind[m] for m in range(3)]

    def lane_sum(v):
        return jnp.broadcast_to(jnp.sum(v, axis=1, keepdims=True), (8, 128))

    def pick(lines, m):
        value = jnp.zeros((8, 128), F32)
        for k, line in lines.items():
            value = jnp.where(kinds[m] == k, line, value)
        return value

    def turned(total, n):
        rows = jnp.concatenate([jnp.sum(t, axis=0, keepdims=True) for t in total] + [jnp.zeros((1, 128), F32)], axis=0)
        if n is None:
            return rows
        odd = lax.broadcasted_iota(I32, (4, 128), 1) % 2 == 1
        swapped = jnp.where(odd, pltpu.roll(rows, 1, 1), pltpu.roll(rows, 127, 1))
        return rows * rot[n, 0][0:4] + swapped * rot[n, 1][0:4]

    def mac(acc, n, a_pair, b_pair):
        (ar, ai), (br, bi) = a_pair, b_pair
        acc[2 * n] = acc[2 * n] + (ar * br + ai * bi)
        acc[2 * n + 1] = acc[2 * n + 1] + (ar * bi - ai * br)

    total = [[jnp.zeros((8, 128), F32) for _ in range(3)] for _ in range(2)]

    def own_pairs(rr, n, acc):
        acc = list(acc)
        for a in range(3):
            re_at, im_at = n + 6 * a, 18 + n + 6 * a
            mac(acc, 0, (left[rr, re_at], left[rr, im_at]), (left[0, re_at], left[0, im_at]))
        return tuple(acc)

    def regular(kinds_at, add, groups, total):
        for rr in range(4):
            zero = tuple(jnp.zeros((8, 128), F32) for _ in range(2 * len(kinds_at)))
            sums = lax.fori_loop(0, 6, functools.partial(add, rr), zero, unroll=True)
            for ri in range(2):
                lines = {k: lane_sum(sums[2 * n + ri]) for n, k in enumerate(kinds_at)}
                for m in range(3):
                    entry = table[m, rr * 2 + ri]
                    for g, ks in enumerate(groups):
                        if ks:
                            total[g][m] = total[g][m] + entry * pick({k: lines[k] for k in ks}, m)

    regular((0,), own_pairs, ((0,), ()), total)

    def link(ref, slot):
        block = ref[slot].astype(F32)
        return [
            [tuple(jnp.broadcast_to(block[3 * a + b, ri : ri + 1, :], (8, 128)) for ri in range(2)) for b in range(3)]
            for a in range(3)
        ]

    def product(one, two):
        def entry(a, c):
            re = im = None
            for b in range(3):
                (pr, pi), (qr, qi) = one[a][b], two[b][c]
                r2, i2 = pr * qr - pi * qi, pr * qi + pi * qr
                re, im = (r2, i2) if b == 0 else (re + r2, im + i2)
            return re, im

        return [[entry(a, c) for c in range(3)] for a in range(3)]

    def keep(ref, line, matrix, dagger=False):
        for a in range(3):
            for b in range(3):
                re, im = matrix[b][a] if dagger else matrix[a][b]
                ref[line, (a * 3 + b) * 2] = re
                ref[line, (a * 3 + b) * 2 + 1] = -im if dagger else im

    def transport(load, lines, line, store):
        got = [[load(ri * 3 + b) for ri in range(2)] for b in range(3)]
        for half in range(2):
            part = [[v[half * 8 : half * 8 + 8] for v in pair] for pair in got]
            for a in range(3):
                re = im = None
                for b in range(3):
                    if lines is None:
                        re, im = part[a]
                        break
                    wr, wi = lines[line, (a * 3 + b) * 2], lines[line, (a * 3 + b) * 2 + 1]
                    vr, vi = part[b]
                    r2, i2 = wr * vr - wi * vi, wr * vi + wi * vr
                    re, im = (r2, i2) if b == 0 else (re + r2, im + i2)
                store(a, half, re, im)

    def bring(slot, line):
        @pl.loop(0, 3)
        def _(q):
            def load(block):
                return sbuf[slot, block, pl.ds(pl.multiple_of(q * 16, 16), 16), :].astype(F32)

            def store(a, half, re, im):
                fields[line, a * 6 + q * 2 + half] = re
                fields[line, 18 + a * 6 + q * 2 + half] = im

            transport(load, wil, line, store)

    def clear(line):
        @pl.loop(0, 36)
        def _(n):
            fields[line, n] = jnp.zeros((8, 128), F32)

    keep(wil, 0, link(ubuf, 0))
    for n in (3, 4, 5):
        pl.when(comes[n])(halo[n].wait_recv)

    @pl.when(comes[1])
    def _():
        halo[1].wait_recv()
        bring(1, 0)

    @pl.when(comes[0])
    def _():
        keep(wil, 1, product(link(ubuf, 0), link(ubuf, 1)))
        halo[0].wait_recv()
        bring(2, 1)

    @pl.when(comes[2])
    def _():
        keep(wil, 2, product(link(ubuf, 3), link(ubuf, 2)), dagger=True)
        halo[2].wait_recv()
        bring(3, 2)

    for line, n in ((0, 1), (1, 0), (2, 2)):
        @pl.when(jnp.logical_not(comes[n]))
        def _():
            clear(line)

    def moved_pairs(rr, n, acc):
        acc = list(acc)
        for a in range(3):
            re_at, im_at = n + 6 * a, 18 + n + 6 * a
            here = (left[rr, re_at], left[rr, im_at])
            behind = (roll4(fields[2, re_at], rr), roll4(fields[2, im_at], rr))
            one, two = (fields[0, re_at], fields[0, im_at]), (fields[1, re_at], fields[1, im_at])
            mac(acc, 0, here, one)
            mac(acc, 1, here, two)
            mac(acc, 2, behind, one)
            mac(acc, 3, behind, two)
        return tuple(acc)

    regular((1, 2, 3, 4), moved_pairs, ((1, 2), (3, 4)), total)
    mine[...] = turned(total[0], None) + turned(total[1], 4)

    @pl.when(is_worker)
    def _():
        def bring_cross(n, line):
            def load(block):
                return xbuf[n, block].astype(F32)

            def store(a, half, re, im):
                xfields[n, a * 2 + half] = re
                xfields[n, 6 + a * 2 + half] = im

            transport(load, None if line is None else xwil, line, store)

        bulk(xlink.at[pl.ds(0, 4)], recv_l.at[0]).wait_recv()
        line = link(xlink, 3)
        keep(xwil, 3, line, dagger=True)
        for n in (2, 1, 0):
            line = product(link(xlink, n), line)
            keep(xwil, n, line, dagger=True)
        bulk(xbuf.at[pl.ds(0, 4)], recv_x.at[0]).wait_recv()
        for n in range(4):
            bring_cross(n, n)
        bulk(xlink.at[pl.ds(4, 4)], recv_l.at[1]).wait_recv()
        line = link(xlink, 4)
        keep(xwil, 4, line)
        for n in (5, 6):
            line = product(line, link(xlink, n))
            keep(xwil, n, line)
        bulk(xbuf.at[pl.ds(4, 4)], recv_x.at[1]).wait_recv()
        for n in range(4, 8):
            bring_cross(n, None if n == 4 else n - 1)

        cross = [(i, j) for i in range(4) for j in range(i + 1)]
        total = [[jnp.zeros((8, 128), F32) for _ in range(3)] for _ in range(4)]
        for rr in range(4):
            def add(n, acc):
                acc = list(acc)
                ahead = [(xfields[4 + j, n], xfields[4 + j, 6 + n]) for j in range(4)]
                for i in range(4):
                    behind = (roll4(xfields[i, n], rr), roll4(xfields[i, 6 + n], rr))
                    for j in range(i + 1):
                        mac(acc, cross.index((i, j)), behind, ahead[j])
                return tuple(acc)

            sums = lax.fori_loop(0, 6, add, tuple(jnp.zeros((8, 128), F32) for _ in range(20)), unroll=True)
            for ri in range(2):
                lines = [lane_sum(sums[2 * n + ri]) for n in range(10)]
                for m in range(3):
                    entry = table[m, rr * 2 + ri]
                    for i in range(4):
                        at_k = {4 - i + j: lines[cross.index((i, j))] for j in range(i + 1)}
                        total[i][m] = total[i][m] + entry * pick(at_k, m)
        mine[...] = mine[...] + ((turned(total[0], 0) + turned(total[1], 1)) + (turned(total[2], 2) + turned(total[3], 3)))

    def to_centre():
        return pltpu.make_async_remote_copy(
            src_ref=mine, dst_ref=slot_b.at[chip * 2 + core], send_sem=send_b, recv_sem=recv_b,
            device_id={"gy": 0, "gz_1": 0, "gz_2": 1}, device_id_type=MESH,
        )

    def to_plane(n):
        return pltpu.make_async_remote_copy(
            src_ref=sum_b, dst_ref=slot_c.at[column], send_sem=send_c, recv_sem=recv_c,
            device_id={"ta": n // 4, "gz_0": n % 4}, device_id_type=MESH,
        )

    def to_chip(dst, side):
        return pltpu.make_async_remote_copy(
            src_ref=final.at[0], dst_ref=final.at[0], send_sem=send_d, recv_sem=recv_d,
            device_id={"gy": dst // 8, "gz_1": dst % 8, "gz_2": side}, device_id_type=MESH,
        )

    outward = [(0, 0)] + [(c, side) for c in (1, 2, 3, 4, 5, 6, 7, 28, 8, 24, 12, 20, 16) for side in (0, 1)]
    is_head = (chip % 4 == 0) & (chip >= 8)

    @pl.when(jnp.logical_not(is_centre))
    def _():
        to_centre().start()
        to_chip(0, 1).wait_recv()

        @pl.when(is_head)
        def _():
            for n in range(1, 4):
                to_chip(chip + n, core).start()

    @pl.when(is_centre)
    def _():
        acc = mine[...]
        bulk(slot_b.at[pl.ds(0, 63)], recv_b).wait_recv()
        for n in range(64):
            if n != 1:
                acc = acc + slot_b[n]
        sum_b[...] = acc

        for n in range(16):
            pl.when(column != n)(to_plane(n).start)
        slot_c[column] = acc
        bulk(slot_c.at[pl.ds(0, 15)], recv_c).wait_recv()
        slices = []
        for t in range(4):
            acc = slot_c[4 * t]
            for q in range(1, 4):
                acc = acc + slot_c[4 * t + q]
            slices.append(acc)
        quarter = lax.broadcasted_iota(I32, (4, 128), 1) // 32
        for q in range(4):
            rows = slices[0] if q == 0 else pltpu.roll(slices[0], (128 - 32 * q) % 128, 1)
            for t in range(1, 4):
                turned = slices[t] if t == q else pltpu.roll(slices[t], (128 + 32 * (t - q)) % 128, 1)
                rows = jnp.where(quarter == t, turned, rows)
            for m in range(3):
                if m * 4 + q < 9:
                    final[0, m * 4 + q] = rows[m : m + 1, :]
        for dst, side in outward:
            to_chip(dst, side).start()

    for j in range(9):
        out[j : j + 1, :] = final[0, j]

    for n in range(6):
        pl.when(goes[n])(halo[n].wait_send)
    @pl.when(is_member & is_worker)
    def _():
        bulk(sbuf.at[0, :, pl.ds(0, 32), :], send_x.at[0]).wait_send()
        bulk(ubuf.at[pl.ds(0, 2)], send_x.at[1]).wait_send()

    @pl.when(is_member & jnp.logical_not(is_worker))
    def _():
        bulk(sbuf.at[0], send_x.at[0]).wait_send()
        bulk(ubuf.at[pl.ds(0, 3)], send_x.at[1]).wait_send()

    @pl.when(jnp.logical_not(is_centre))
    def _():
        to_centre().wait_send()

        @pl.when(is_head)
        def _():
            bulk(final.at[pl.ds(0, 3)], send_d).wait_send()

    @pl.when(is_centre)
    def _():
        bulk(slot_c.at[pl.ds(0, 15)], send_c).wait_send()
        bulk(final, send_d).wait_send()


def body(propagator, links, source_z, displacements, momenta, gamma_perm, gamma_phase):
    nz = lax.axis_size(GZ)
    sites_total = propagator.shape[6] * lax.axis_size("gy") * nz
    scaling = 1.0 / (24.0 * math.sqrt(sites_total))
    prop = jnp.transpose(propagator, (0, 2, 3, 1, 4, 5, 6)).reshape(6, 48, 128)
    link = jnp.transpose(links, (1, 2, 0, 3, 4, 5)).reshape(9, 2, 128)
    hbm = pl.BlockSpec(memory_space=pl.ANY)
    dma = pltpu.SemaphoreType.DMA
    out = pl.pallas_call(
        functools.partial(kernel, nz, scaling),
        out_shape=jax.ShapeDtypeStruct((9, 128), F32),
        in_specs=[hbm] * 7,
        out_specs=pl.BlockSpec(memory_space=pltpu.VMEM),
        scratch_shapes=[
            pltpu.SMEM((4, 4), I32),
            pltpu.SMEM((9,), I32),
            pltpu.SMEM((4,), I32),
            pltpu.SMEM((4, 4), I32),
            pltpu.SMEM((4, 4), I32),
            pltpu.VMEM((4, 6, 48, 128), jnp.bfloat16),
            pltpu.VMEM((4, 9, 2, 128), jnp.bfloat16),
            pltpu.VMEM((4, 36, 8, 128), F32),
            pltpu.VMEM((3, 36, 8, 128), F32),
            pltpu.VMEM((3, 18, 8, 128), F32),
            pltpu.VMEM((3, 8, 8, 128), F32),
            pltpu.VMEM((3, 8, 128), I32),
            pltpu.VMEM((4, 128), F32),
            pltpu.VMEM((64, 4, 128), F32),
            pltpu.VMEM((4, 128), F32),
            pltpu.VMEM((16, 4, 128), F32),
            pltpu.VMEM((27, 9, 1, 128), F32),
            pltpu.VMEM((8, 6, 16, 128), jnp.bfloat16),
            pltpu.VMEM((8, 9, 2, 128), jnp.bfloat16),
            pltpu.VMEM((8, 12, 8, 128), F32),
            pltpu.VMEM((7, 18, 8, 128), F32),
            pltpu.VMEM((5, 2, 8, 128), F32),
            dma((7,)),
            dma((6,)),
            dma((6,)),
            dma,
            dma,
            dma,
            dma,
            dma,
            dma,
            dma((2,)),
            dma((2,)),
            dma((2,)),
        ],
        compiler_params=pltpu.CompilerParams(collective_id=0, has_side_effects=True),
    )(prop, link, source_z, displacements, momenta, gamma_perm, gamma_phase)
    return jnp.transpose(out.reshape(9, 4, 4, 4, 2), (1, 0, 2, 3, 4))


def solution(mesh):
    torus = Mesh(
        mesh.devices.reshape(mesh.shape["ta"], 4, 8, 2, mesh.shape["gy"]),
        ("ta", "gz_0", "gz_1", "gz_2", "gy"),
    )
    in_specs = (
        P(None, None, None, None, "ta", GZ, "gy"),
        P(None, None, None, "ta", GZ, "gy"),
        P(),
        P(),
        P(),
        P(),
        P(),
    )
    return jax.shard_map(body, mesh=torus, in_specs=in_specs, out_specs=P(), check_vma=False)
```

```python
import functools
import math

import jax
import jax.numpy as jnp
from jax import lax
from jax.experimental import pallas as pl
from jax.experimental.pallas import tpu as pltpu
from jax.sharding import Mesh
from jax.sharding import PartitionSpec as P

GZ = ("gz_0", "gz_1", "gz_2")
MESH = pl.DeviceIdType.MESH
F32 = jnp.float32
I32 = jnp.int32


def roll4(x, r):
    if r == 0:
        return x
    spin = lax.broadcasted_iota(I32, (8, 128), 0) % 4
    return jnp.where(spin < 4 - r, pltpu.roll(x, 8 - r, 0), pltpu.roll(x, 4 - r, 0))


def kernel(
    nz, scaling, s_hbm, u_hbm, *refs,
):
    ints_hbm, out, ints = refs[:5], refs[5], refs[6:11]
    sbuf, ubuf, left, fields, wil, table, kind, mine, slot_b, sum_b, slot_c, final, xbuf, xlink, xfields, xwil, rot = refs[11:28]
    load_sem, send_sem, recv_sem, send_b, recv_b, send_c, recv_c, send_d, recv_d, send_x, recv_x, recv_l = refs[28:]
    source_z, displacements, momenta, perm, phase = ints
    x = lax.axis_index("ta")
    gy0 = lax.axis_index("gz_0")
    lo = lax.axis_index("gz_1")
    core = lax.axis_index("gz_2")
    hi = lax.axis_index("gy")
    z = gy0 * 16 + lo * 2 + core
    chip = hi * 8 + lo
    is_centre = (chip == 0) & (core == 1)
    column = x * 4 + gy0
    place = lo * 2 + core
    at_end = hi >= 2
    is_member = (place >= 12) | (place < 4)
    member = jnp.where(place >= 12, place - 12, place + 4)
    row_a = jnp.where(place >= 12, gy0, (gy0 + 3) % 4)
    is_worker = jnp.where(at_end, place >= 13, place < 3)
    first = jnp.where(at_end, 13, 0)

    def seat(row, spot):
        return {"gz_0": row % 4, "gz_1": spot // 2, "gz_2": spot % 2}

    def along(offset):
        w = (z + (offset + nz)) % nz
        return {"gz_0": w // 16, "gz_1": (w // 2) % 8, "gz_2": w % 2}

    loads = [pltpu.make_async_copy(s_hbm, sbuf.at[0], load_sem.at[0]), pltpu.make_async_copy(u_hbm, ubuf.at[0], load_sem.at[1])]
    loads += [pltpu.make_async_copy(ints_hbm[n], ints[n], load_sem.at[2 + n]) for n in range(5)]
    for load in loads:
        load.start()

    barrier = pltpu.get_barrier_semaphore()
    @pl.when(is_worker)
    def _():
        row_w = gy0 + jnp.where(at_end, 3, 0)
        for n in range(4):
            other = seat(row_w + jnp.where(at_end, 1, 0), jnp.where(at_end, n, 12 + n))
            pl.semaphore_signal(barrier, inc=1, device_id=other, device_id_type=MESH)
        for n in range(4):
            other = seat(row_w + jnp.where(at_end, 0, 1), jnp.where(at_end, 12 + n, n))
            pl.semaphore_signal(barrier, inc=1, device_id=other, device_id_type=MESH)

    heard = jnp.where(is_centre, 15, 1) + jnp.where(is_member, 3, 0)
    for offset in (-2, -1, 1, 2):
        inside = (place + offset >= 0) & (place + offset < 16)
        heard = heard + jnp.where(inside, 1, 0)

        @pl.when(inside)
        def _():
            pl.semaphore_signal(barrier, inc=1, device_id=along(offset), device_id_type=MESH)

    @pl.when(is_centre)
    def _():
        @pl.loop(1, 64)
        def _(n):
            other = {"gy": (64 - n) // 16, "gz_1": (64 - n) // 2 % 8, "gz_2": (64 - n) % 2}
            pl.when(n != 63)(lambda: pl.semaphore_signal(barrier, inc=1, device_id=other, device_id_type=MESH))

        pl.semaphore_signal(barrier, inc=1, device_id={"gz_2": 0}, device_id_type=MESH)
        for n in range(16):
            other = {"ta": n // 4, "gz_0": n % 4}
            pl.when(column != n)(
                functools.partial(pl.semaphore_signal, barrier, inc=1, device_id=other, device_id_type=MESH)
            )

    loads[0].wait()
    loads[1].wait()
    pl.semaphore_wait(barrier, heard)

    def to(buf, n, dst, offset):
        return pltpu.make_async_remote_copy(
            src_ref=buf.at[0], dst_ref=buf.at[dst], send_sem=send_sem.at[n], recv_sem=recv_sem.at[n],
            device_id=along(offset), device_id_type=MESH,
        )

    halo = [
        to(sbuf, 0, 2, -2), to(sbuf, 1, 1, -1), to(sbuf, 2, 3, 2),
        to(ubuf, 3, 1, -1), to(ubuf, 4, 2, 1), to(ubuf, 5, 3, 2),
    ]
    offsets = (-2, -1, 2, -1, 1, 2)
    goes = [(place + o >= 0) & (place + o < 16) for o in offsets]
    comes = [(place - o >= 0) & (place - o < 16) for o in offsets]
    def bulk(ref, sem):
        return pltpu.make_async_remote_copy(
            src_ref=ref, dst_ref=ref, send_sem=sem, recv_sem=sem, device_id={"gy": (hi + 1) % 4}, device_id_type=MESH
        )

    def to_worker(n):
        third, spot = n % 3, first + n % 3
        row = row_a + jnp.where(at_end, 1, 0)
        src = sbuf.at[0, :, pl.ds(third * 16, 16), :] if n < 3 else ubuf.at[0]
        dst, sem = (xbuf, recv_x) if n < 3 else (xlink, recv_l)
        side = jnp.where(place >= 12, 0, 1)
        return pltpu.make_async_remote_copy(
            src_ref=src, dst_ref=dst.at[member], send_sem=send_x.at[n // 3], recv_sem=sem.at[side],
            device_id=seat(row, spot), device_id_type=MESH,
        )
    @pl.when(is_member)
    def _():
        for n in (3, 4, 5, 0, 1, 2):
            to_worker(n).start()

    for n in (3, 4, 5, 1, 0, 2):
        pl.when(goes[n])(halo[n].start)

    for load in loads[2:]:
        load.wait()

    sub = lax.broadcasted_iota(I32, (8, 128), 0)
    lane = lax.broadcasted_iota(I32, (8, 128), 1)
    u_id = sub % 4
    g_id = (lane % 32) // 8
    p_id = (lane // 2) % 4
    c_id = lane % 2
    perm_t = jnp.zeros((8, 128), I32)
    phase_t = jnp.zeros((8, 128), I32)
    for g in range(4):
        for s in range(4):
            here = (g_id == g) & (u_id == s)
            perm_t = jnp.where(here, perm[g, s], perm_t)
            phase_t = jnp.where(here, phase[g, s], phase_t)
    mom = jnp.zeros((8, 128), I32)
    src = jnp.zeros((8, 128), I32)
    for p in range(4):
        mom = jnp.where(p_id == p, momenta[p], mom)
        src = jnp.where(p_id == p, source_z[x, p], src)
    corner = jnp.where(at_end, -4 - place, 12 - place)
    for n in range(5):
        turns = (mom * (corner + n if n < 4 else -2)) & (nz - 1)
        angle = turns.astype(F32) * (2.0 * math.pi / nz)
        sine = jnp.sin(angle)
        rot[n, 0] = jnp.cos(angle)
        rot[n, 1] = jnp.where(c_id == 0, sine, -sine)
    for m in range(3):
        j_id = m * 4 + lane // 32
        shift = jnp.zeros((8, 128), I32)
        for j in range(4 * m, min(4 * m + 4, 9)):
            shift = jnp.where(j_id == j, displacements[j] - 4, shift)
        neg = shift < 0
        k_id = jnp.where(neg, -shift, shift)
        at = z + jnp.where(neg, k_id, 0)
        turns = (mom * (at - src)) & (nz - 1)
        angle = turns.astype(F32) * (2.0 * math.pi / nz)
        cosine = jnp.cos(angle) * scaling
        sine = jnp.sin(angle) * scaling
        kind[m] = k_id
        for rr in range(4):
            s_id = (u_id + rr) % 4
            perm_r = pltpu.roll(perm_t, 8 - rr, 0) if rr else perm_t
            phase_r = pltpu.roll(phase_t, 8 - rr, 0) if rr else phase_t
            match = jnp.where(neg, perm_t, perm_r) == jnp.where(neg, s_id, u_id)
            power = jnp.where(neg, phase_t, phase_r)
            for ri in range(2):
                if ri == 0:
                    turn = jnp.where(c_id == 0, 0, 3)
                else:
                    turn = jnp.where(c_id == 0, jnp.where(neg, 3, 1), jnp.where(neg, 2, 0))
                h = (power + turn) & 3
                value = jnp.where((h & 1) == 1, sine, cosine)
                value = jnp.where(h >= 2, -value, value)
                table[m, rr * 2 + ri] = jnp.where(match & (j_id < 9), value, 0.0)

    @pl.loop(0, 18)
    def _(n):
        rows = sbuf[0, n // 3, pl.ds(pl.multiple_of(n % 3 * 16, 16), 16), :].astype(F32)
        for half in range(2):
            for rr in range(4):
                left[rr, 2 * n + half] = roll4(rows[half * 8 : half * 8 + 8], rr)

    kinds = [kind[m] for m in range(3)]

    def lane_sum(v):
        return jnp.broadcast_to(jnp.sum(v, axis=1, keepdims=True), (8, 128))

    def pick(lines, m):
        value = jnp.zeros((8, 128), F32)
        for k, line in lines.items():
            value = jnp.where(kinds[m] == k, line, value)
        return value

    def turned(total, n):
        rows = jnp.concatenate([jnp.sum(t, axis=0, keepdims=True) for t in total] + [jnp.zeros((1, 128), F32)], axis=0)
        if n is None:
            return rows
        odd = lax.broadcasted_iota(I32, (4, 128), 1) % 2 == 1
        swapped = jnp.where(odd, pltpu.roll(rows, 1, 1), pltpu.roll(rows, 127, 1))
        return rows * rot[n, 0][0:4] + swapped * rot[n, 1][0:4]

    def mac(acc, n, a_pair, b_pair):
        (ar, ai), (br, bi) = a_pair, b_pair
        acc[2 * n] = acc[2 * n] + (ar * br + ai * bi)
        acc[2 * n + 1] = acc[2 * n + 1] + (ar * bi - ai * br)

    total = [[jnp.zeros((8, 128), F32) for _ in range(3)] for _ in range(2)]

    def own_pairs(rr, n, acc):
        acc = list(acc)
        for a in range(3):
            re_at, im_at = n + 6 * a, 18 + n + 6 * a
            mac(acc, 0, (left[rr, re_at], left[rr, im_at]), (left[0, re_at], left[0, im_at]))
        return tuple(acc)

    def regular(kinds_at, add, groups, total):
        for rr in range(4):
            zero = tuple(jnp.zeros((8, 128), F32) for _ in range(2 * len(kinds_at)))
            sums = lax.fori_loop(0, 6, functools.partial(add, rr), zero, unroll=True)
            for ri in range(2):
                lines = {k: lane_sum(sums[2 * n + ri]) for n, k in enumerate(kinds_at)}
                for m in range(3):
                    entry = table[m, rr * 2 + ri]
                    for g, ks in enumerate(groups):
                        if ks:
                            total[g][m] = total[g][m] + entry * pick({k: lines[k] for k in ks}, m)

    regular((0,), own_pairs, ((0,), ()), total)

    def link(ref, slot):
        block = ref[slot].astype(F32)
        return [
            [tuple(jnp.broadcast_to(block[3 * a + b, ri : ri + 1, :], (8, 128)) for ri in range(2)) for b in range(3)]
            for a in range(3)
        ]

    def product(one, two):
        def entry(a, c):
            re = im = None
            for b in range(3):
                (pr, pi), (qr, qi) = one[a][b], two[b][c]
                r2, i2 = pr * qr - pi * qi, pr * qi + pi * qr
                re, im = (r2, i2) if b == 0 else (re + r2, im + i2)
            return re, im

        return [[entry(a, c) for c in range(3)] for a in range(3)]

    def keep(ref, line, matrix, dagger=False):
        for a in range(3):
            for b in range(3):
                re, im = matrix[b][a] if dagger else matrix[a][b]
                ref[line, (a * 3 + b) * 2] = re
                ref[line, (a * 3 + b) * 2 + 1] = -im if dagger else im

    def transport(load, lines, line, store):
        got = [[load(ri * 3 + b) for ri in range(2)] for b in range(3)]
        for half in range(2):
            part = [[v[half * 8 : half * 8 + 8] for v in pair] for pair in got]
            for a in range(3):
                re = im = None
                for b in range(3):
                    if lines is None:
                        re, im = part[a]
                        break
                    wr, wi = lines[line, (a * 3 + b) * 2], lines[line, (a * 3 + b) * 2 + 1]
                    vr, vi = part[b]
                    r2, i2 = wr * vr - wi * vi, wr * vi + wi * vr
                    re, im = (r2, i2) if b == 0 else (re + r2, im + i2)
                store(a, half, re, im)

    def bring(slot, line):
        @pl.loop(0, 3)
        def _(q):
            def load(block):
                return sbuf[slot, block, pl.ds(pl.multiple_of(q * 16, 16), 16), :].astype(F32)

            def store(a, half, re, im):
                fields[line, a * 6 + q * 2 + half] = re
                fields[line, 18 + a * 6 + q * 2 + half] = im

            transport(load, wil, line, store)

    def clear(line):
        @pl.loop(0, 36)
        def _(n):
            fields[line, n] = jnp.zeros((8, 128), F32)

    keep(wil, 0, link(ubuf, 0))
    for n in (3, 4, 5):
        pl.when(comes[n])(halo[n].wait_recv)

    @pl.when(comes[1])
    def _():
        halo[1].wait_recv()
        bring(1, 0)

    @pl.when(comes[0])
    def _():
        keep(wil, 1, product(link(ubuf, 0), link(ubuf, 1)))
        halo[0].wait_recv()
        bring(2, 1)

    @pl.when(comes[2])
    def _():
        keep(wil, 2, product(link(ubuf, 3), link(ubuf, 2)), dagger=True)
        halo[2].wait_recv()
        bring(3, 2)

    for line, n in ((0, 1), (1, 0), (2, 2)):
        @pl.when(jnp.logical_not(comes[n]))
        def _():
            clear(line)

    def moved_pairs(rr, n, acc):
        acc = list(acc)
        for a in range(3):
            re_at, im_at = n + 6 * a, 18 + n + 6 * a
            here = (left[rr, re_at], left[rr, im_at])
            behind = (roll4(fields[2, re_at], rr), roll4(fields[2, im_at], rr))
            one, two = (fields[0, re_at], fields[0, im_at]), (fields[1, re_at], fields[1, im_at])
            mac(acc, 0, here, one)
            mac(acc, 1, here, two)
            mac(acc, 2, behind, one)
            mac(acc, 3, behind, two)
        return tuple(acc)

    regular((1, 2, 3, 4), moved_pairs, ((1, 2), (3, 4)), total)
    mine[...] = turned(total[0], None) + turned(total[1], 4)

    @pl.when(is_worker)
    def _():
        def bring_cross(n, line):
            def load(block):
                return xbuf[n, block].astype(F32)

            def store(a, half, re, im):
                xfields[n, a * 2 + half] = re
                xfields[n, 6 + a * 2 + half] = im

            transport(load, None if line is None else xwil, line, store)

        bulk(xlink.at[pl.ds(0, 4)], recv_l.at[0]).wait_recv()
        line = link(xlink, 3)
        keep(xwil, 3, line, dagger=True)
        for n in (2, 1, 0):
            line = product(link(xlink, n), line)
            keep(xwil, n, line, dagger=True)
        bulk(xbuf.at[pl.ds(0, 4)], recv_x.at[0]).wait_recv()
        for n in range(4):
            bring_cross(n, n)
        bulk(xlink.at[pl.ds(4, 4)], recv_l.at[1]).wait_recv()
        line = link(xlink, 4)
        keep(xwil, 4, line)
        for n in (5, 6):
            line = product(line, link(xlink, n))
            keep(xwil, n, line)
        bulk(xbuf.at[pl.ds(4, 4)], recv_x.at[1]).wait_recv()
        for n in range(4, 8):
            bring_cross(n, None if n == 4 else n - 1)

        cross = [(i, j) for i in range(4) for j in range(i + 1)]
        total = [[jnp.zeros((8, 128), F32) for _ in range(3)] for _ in range(4)]
        for rr in range(4):
            def add(n, acc):
                acc = list(acc)
                ahead = [(xfields[4 + j, n], xfields[4 + j, 6 + n]) for j in range(4)]
                for i in range(4):
                    behind = (roll4(xfields[i, n], rr), roll4(xfields[i, 6 + n], rr))
                    for j in range(i + 1):
                        mac(acc, cross.index((i, j)), behind, ahead[j])
                return tuple(acc)

            sums = lax.fori_loop(0, 6, add, tuple(jnp.zeros((8, 128), F32) for _ in range(20)), unroll=True)
            for ri in range(2):
                lines = [lane_sum(sums[2 * n + ri]) for n in range(10)]
                for m in range(3):
                    entry = table[m, rr * 2 + ri]
                    for i in range(4):
                        at_k = {4 - i + j: lines[cross.index((i, j))] for j in range(i + 1)}
                        total[i][m] = total[i][m] + entry * pick(at_k, m)
        mine[...] = mine[...] + ((turned(total[0], 0) + turned(total[1], 1)) + (turned(total[2], 2) + turned(total[3], 3)))

    def to_centre():
        return pltpu.make_async_remote_copy(
            src_ref=mine, dst_ref=slot_b.at[chip * 2 + core], send_sem=send_b, recv_sem=recv_b,
            device_id={"gy": 0, "gz_1": 0, "gz_2": 1}, device_id_type=MESH,
        )

    def to_plane(n):
        return pltpu.make_async_remote_copy(
            src_ref=sum_b, dst_ref=slot_c.at[column], send_sem=send_c, recv_sem=recv_c,
            device_id={"ta": n // 4, "gz_0": n % 4}, device_id_type=MESH,
        )

    def to_chip(dst, side):
        return pltpu.make_async_remote_copy(
            src_ref=final.at[0], dst_ref=final.at[0], send_sem=send_d, recv_sem=recv_d,
            device_id={"gy": dst // 8, "gz_1": dst % 8, "gz_2": side}, device_id_type=MESH,
        )

    outward = [(0, 0)] + [(c, side) for c in (1, 2, 3, 4, 5, 6, 7, 28, 8, 24, 12, 20, 16) for side in (0, 1)]
    is_head = (chip % 4 == 0) & (chip >= 8)

    @pl.when(jnp.logical_not(is_centre))
    def _():
        to_centre().start()
        to_chip(0, 1).wait_recv()

        @pl.when(is_head)
        def _():
            for n in range(1, 4):
                to_chip(chip + n, core).start()

    @pl.when(is_centre)
    def _():
        acc = mine[...]
        bulk(slot_b.at[pl.ds(0, 63)], recv_b).wait_recv()
        for n in range(64):
            if n != 1:
                acc = acc + slot_b[n]
        sum_b[...] = acc

        for n in range(16):
            pl.when(column != n)(to_plane(n).start)
        slot_c[column] = acc
        bulk(slot_c.at[pl.ds(0, 15)], recv_c).wait_recv()
        slices = []
        for t in range(4):
            acc = slot_c[4 * t]
            for q in range(1, 4):
                acc = acc + slot_c[4 * t + q]
            slices.append(acc)
        quarter = lax.broadcasted_iota(I32, (4, 128), 1) // 32
        for q in range(4):
            rows = slices[0] if q == 0 else pltpu.roll(slices[0], (128 - 32 * q) % 128, 1)
            for t in range(1, 4):
                turned = slices[t] if t == q else pltpu.roll(slices[t], (128 + 32 * (t - q)) % 128, 1)
                rows = jnp.where(quarter == t, turned, rows)
            for m in range(3):
                if m * 4 + q < 9:
                    final[0, m * 4 + q] = rows[m : m + 1, :]
        for dst, side in outward:
            to_chip(dst, side).start()

    for j in range(9):
        out[j : j + 1, :] = final[0, j]

    for n in range(6):
        pl.when(goes[n])(halo[n].wait_send)
    @pl.when(is_member)
    def _():
        bulk(sbuf.at[0], send_x.at[0]).wait_send()
        bulk(ubuf.at[pl.ds(0, 3)], send_x.at[1]).wait_send()

    @pl.when(jnp.logical_not(is_centre))
    def _():
        to_centre().wait_send()

        @pl.when(is_head)
        def _():
            bulk(final.at[pl.ds(0, 3)], send_d).wait_send()

    @pl.when(is_centre)
    def _():
        bulk(slot_c.at[pl.ds(0, 15)], send_c).wait_send()
        bulk(final, send_d).wait_send()


def body(propagator, links, source_z, displacements, momenta, gamma_perm, gamma_phase):
    nz = lax.axis_size(GZ)
    sites_total = propagator.shape[6] * lax.axis_size("gy") * nz
    scaling = 1.0 / (24.0 * math.sqrt(sites_total))
    prop = jnp.transpose(propagator, (0, 2, 3, 1, 4, 5, 6)).reshape(6, 48, 128)
    link = jnp.transpose(links, (1, 2, 0, 3, 4, 5)).reshape(9, 2, 128)
    hbm = pl.BlockSpec(memory_space=pl.ANY)
    dma = pltpu.SemaphoreType.DMA
    out = pl.pallas_call(
        functools.partial(kernel, nz, scaling),
        out_shape=jax.ShapeDtypeStruct((9, 128), F32),
        in_specs=[hbm] * 7,
        out_specs=pl.BlockSpec(memory_space=pltpu.VMEM),
        scratch_shapes=[
            pltpu.SMEM((4, 4), I32),
            pltpu.SMEM((9,), I32),
            pltpu.SMEM((4,), I32),
            pltpu.SMEM((4, 4), I32),
            pltpu.SMEM((4, 4), I32),
            pltpu.VMEM((4, 6, 48, 128), jnp.bfloat16),
            pltpu.VMEM((4, 9, 2, 128), jnp.bfloat16),
            pltpu.VMEM((4, 36, 8, 128), F32),
            pltpu.VMEM((3, 36, 8, 128), F32),
            pltpu.VMEM((3, 18, 8, 128), F32),
            pltpu.VMEM((3, 8, 8, 128), F32),
            pltpu.VMEM((3, 8, 128), I32),
            pltpu.VMEM((4, 128), F32),
            pltpu.VMEM((64, 4, 128), F32),
            pltpu.VMEM((4, 128), F32),
            pltpu.VMEM((16, 4, 128), F32),
            pltpu.VMEM((27, 9, 1, 128), F32),
            pltpu.VMEM((8, 6, 16, 128), jnp.bfloat16),
            pltpu.VMEM((8, 9, 2, 128), jnp.bfloat16),
            pltpu.VMEM((8, 12, 8, 128), F32),
            pltpu.VMEM((7, 18, 8, 128), F32),
            pltpu.VMEM((5, 2, 8, 128), F32),
            dma((7,)),
            dma((6,)),
            dma((6,)),
            dma,
            dma,
            dma,
            dma,
            dma,
            dma,
            dma((2,)),
            dma((2,)),
            dma((2,)),
        ],
        compiler_params=pltpu.CompilerParams(collective_id=0, has_side_effects=True),
    )(prop, link, source_z, displacements, momenta, gamma_perm, gamma_phase)
    return jnp.transpose(out.reshape(9, 4, 4, 4, 2), (1, 0, 2, 3, 4))


def solution(mesh):
    torus = Mesh(
        mesh.devices.reshape(mesh.shape["ta"], 4, 8, 2, mesh.shape["gy"]),
        ("ta", "gz_0", "gz_1", "gz_2", "gy"),
    )
    in_specs = (
        P(None, None, None, None, "ta", GZ, "gy"),
        P(None, None, None, "ta", GZ, "gy"),
        P(),
        P(),
        P(),
        P(),
        P(),
    )
    return jax.shard_map(body, mesh=torus, in_specs=in_specs, out_specs=P(), check_vma=False)
```

```python
import functools
import math

import jax
import jax.numpy as jnp
from jax import lax
from jax.experimental import pallas as pl
from jax.experimental.pallas import tpu as pltpu
from jax.sharding import Mesh
from jax.sharding import PartitionSpec as P

GZ = ("gz_0", "gz_1", "gz_2")
MESH = pl.DeviceIdType.MESH
F32 = jnp.float32
I32 = jnp.int32


def roll4(x, r):
    if r == 0:
        return x
    spin = lax.broadcasted_iota(I32, (8, 128), 0) % 4
    return jnp.where(spin < 4 - r, pltpu.roll(x, 8 - r, 0), pltpu.roll(x, 4 - r, 0))


def kernel(
    nz, scaling, s_hbm, u_hbm, *refs,
):
    ints_hbm, out, ints = refs[:5], refs[5], refs[6:11]
    sbuf, ubuf, left, fields, wil, table, kind, mine, slot_b, sum_b, slot_c, final, xbuf, xlink, xfields, xwil, rot = refs[11:28]
    load_sem, send_sem, recv_sem, send_b, recv_b, send_c, recv_c, send_d, recv_d, send_x, recv_x, recv_l = refs[28:]
    source_z, displacements, momenta, perm, phase = ints
    x = lax.axis_index("ta")
    gy0 = lax.axis_index("gz_0")
    lo = lax.axis_index("gz_1")
    core = lax.axis_index("gz_2")
    hi = lax.axis_index("gy")
    z = gy0 * 16 + lo * 2 + core
    chip = hi * 8 + lo
    is_centre = (chip == 0) & (core == 1)
    column = x * 4 + gy0
    place = lo * 2 + core
    at_end = hi >= 2
    is_member = (place >= 12) | (place < 4)
    member = jnp.where(place >= 12, place - 12, place + 4)
    row_a = jnp.where(place >= 12, gy0, (gy0 + 3) % 4)
    is_worker = jnp.where(at_end, place >= 13, place < 3)
    first = jnp.where(at_end, 13, 0)

    def seat(row, spot):
        return {"gz_0": row % 4, "gz_1": spot // 2, "gz_2": spot % 2}

    def along(offset):
        w = (z + (offset + nz)) % nz
        return {"gz_0": w // 16, "gz_1": (w // 2) % 8, "gz_2": w % 2}

    loads = [pltpu.make_async_copy(s_hbm, sbuf.at[0], load_sem.at[0]), pltpu.make_async_copy(u_hbm, ubuf.at[0], load_sem.at[1])]
    loads += [pltpu.make_async_copy(ints_hbm[n], ints[n], load_sem.at[2 + n]) for n in range(5)]
    for load in loads:
        load.start()

    barrier = pltpu.get_barrier_semaphore()
    @pl.when(is_worker)
    def _():
        row_w = gy0 + jnp.where(at_end, 3, 0)
        for n in range(4):
            other = seat(row_w + jnp.where(at_end, 1, 0), jnp.where(at_end, n, 12 + n))
            pl.semaphore_signal(barrier, inc=1, device_id=other, device_id_type=MESH)
        for n in range(4):
            other = seat(row_w + jnp.where(at_end, 0, 1), jnp.where(at_end, 12 + n, n))
            pl.semaphore_signal(barrier, inc=1, device_id=other, device_id_type=MESH)

    heard = jnp.where(is_centre, 15, 1) + jnp.where(is_member, 3, 0)
    for offset in (-2, -1, 1, 2):
        inside = (place + offset >= 0) & (place + offset < 16)
        heard = heard + jnp.where(inside, 1, 0)

        @pl.when(inside)
        def _():
            pl.semaphore_signal(barrier, inc=1, device_id=along(offset), device_id_type=MESH)

    @pl.when(is_centre)
    def _():
        @pl.loop(1, 64)
        def _(n):
            other = {"gy": (64 - n) // 16, "gz_1": (64 - n) // 2 % 8, "gz_2": (64 - n) % 2}
            pl.when(n != 63)(lambda: pl.semaphore_signal(barrier, inc=1, device_id=other, device_id_type=MESH))

        pl.semaphore_signal(barrier, inc=1, device_id={"gz_2": 0}, device_id_type=MESH)
        for n in range(16):
            other = {"ta": n // 4, "gz_0": n % 4}
            pl.when(column != n)(
                functools.partial(pl.semaphore_signal, barrier, inc=1, device_id=other, device_id_type=MESH)
            )

    loads[0].wait()
    loads[1].wait()
    pl.semaphore_wait(barrier, heard)

    def to(buf, n, dst, offset):
        return pltpu.make_async_remote_copy(
            src_ref=buf.at[0], dst_ref=buf.at[dst], send_sem=send_sem.at[n], recv_sem=recv_sem.at[n],
            device_id=along(offset), device_id_type=MESH,
        )

    halo = [
        to(sbuf, 0, 2, -2), to(sbuf, 1, 1, -1), to(sbuf, 2, 3, 2),
        to(ubuf, 3, 1, -1), to(ubuf, 4, 2, 1), to(ubuf, 5, 3, 2),
    ]
    offsets = (-2, -1, 2, -1, 1, 2)
    goes = [(place + o >= 0) & (place + o < 16) for o in offsets]
    comes = [(place - o >= 0) & (place - o < 16) for o in offsets]
    def bulk(ref, sem):
        return pltpu.make_async_remote_copy(
            src_ref=ref, dst_ref=ref, send_sem=sem, recv_sem=sem, device_id={"gy": (hi + 1) % 4}, device_id_type=MESH
        )

    def to_worker(n):
        third, spot = n % 3, first + n % 3
        row = row_a + jnp.where(at_end, 1, 0)
        src = sbuf.at[0, :, pl.ds(third * 16, 16), :] if n < 3 else ubuf.at[0]
        dst, sem = (xbuf, recv_x) if n < 3 else (xlink, recv_l)
        side = jnp.where(place >= 12, 0, 1)
        return pltpu.make_async_remote_copy(
            src_ref=src, dst_ref=dst.at[member], send_sem=send_x.at[n // 3], recv_sem=sem.at[side],
            device_id=seat(row, spot), device_id_type=MESH,
        )
    @pl.when(is_member)
    def _():
        for n in (3, 4, 5, 0, 1, 2):
            to_worker(n).start()

    for n in (3, 4, 5, 1, 0, 2):
        pl.when(goes[n])(halo[n].start)

    for load in loads[2:]:
        load.wait()

    sub = lax.broadcasted_iota(I32, (8, 128), 0)
    lane = lax.broadcasted_iota(I32, (8, 128), 1)
    u_id = sub % 4
    g_id = (lane % 32) // 8
    p_id = (lane // 2) % 4
    c_id = lane % 2
    perm_t = jnp.zeros((8, 128), I32)
    phase_t = jnp.zeros((8, 128), I32)
    for g in range(4):
        for s in range(4):
            here = (g_id == g) & (u_id == s)
            perm_t = jnp.where(here, perm[g, s], perm_t)
            phase_t = jnp.where(here, phase[g, s], phase_t)
    mom = jnp.zeros((8, 128), I32)
    src = jnp.zeros((8, 128), I32)
    for p in range(4):
        mom = jnp.where(p_id == p, momenta[p], mom)
        src = jnp.where(p_id == p, source_z[x, p], src)
    corner = jnp.where(at_end, -4 - place, 12 - place)
    for n in range(5):
        turns = (mom * (corner + n if n < 4 else -2)) & (nz - 1)
        angle = turns.astype(F32) * (2.0 * math.pi / nz)
        sine = jnp.sin(angle)
        rot[n, 0] = jnp.cos(angle)
        rot[n, 1] = jnp.where(c_id == 0, sine, -sine)
    for m in range(3):
        j_id = m * 4 + lane // 32
        shift = jnp.zeros((8, 128), I32)
        for j in range(4 * m, min(4 * m + 4, 9)):
            shift = jnp.where(j_id == j, displacements[j] - 4, shift)
        neg = shift < 0
        k_id = jnp.where(neg, -shift, shift)
        at = z + jnp.where(neg, k_id, 0)
        turns = (mom * (at - src)) & (nz - 1)
        angle = turns.astype(F32) * (2.0 * math.pi / nz)
        cosine = jnp.cos(angle) * scaling
        sine = jnp.sin(angle) * scaling
        kind[m] = k_id
        for rr in range(4):
            s_id = (u_id + rr) % 4
            perm_r = pltpu.roll(perm_t, 8 - rr, 0) if rr else perm_t
            phase_r = pltpu.roll(phase_t, 8 - rr, 0) if rr else phase_t
            match = jnp.where(neg, perm_t, perm_r) == jnp.where(neg, s_id, u_id)
            power = jnp.where(neg, phase_t, phase_r)
            for ri in range(2):
                if ri == 0:
                    turn = jnp.where(c_id == 0, 0, 3)
                else:
                    turn = jnp.where(c_id == 0, jnp.where(neg, 3, 1), jnp.where(neg, 2, 0))
                h = (power + turn) & 3
                value = jnp.where((h & 1) == 1, sine, cosine)
                value = jnp.where(h >= 2, -value, value)
                table[m, rr * 2 + ri] = jnp.where(match & (j_id < 9), value, 0.0)

    @pl.loop(0, 18)
    def _(n):
        rows = sbuf[0, n // 3, pl.ds(pl.multiple_of(n % 3 * 16, 16), 16), :].astype(F32)
        for half in range(2):
            for rr in range(4):
                left[rr, 2 * n + half] = roll4(rows[half * 8 : half * 8 + 8], rr)

    kinds = [kind[m] for m in range(3)]

    def lane_sum(v):
        return jnp.broadcast_to(jnp.sum(v, axis=1, keepdims=True), (8, 128))

    def pick(lines, m):
        value = jnp.zeros((8, 128), F32)
        for k, line in lines.items():
            value = jnp.where(kinds[m] == k, line, value)
        return value

    def turned(total, n):
        rows = jnp.concatenate([jnp.sum(t, axis=0, keepdims=True) for t in total] + [jnp.zeros((1, 128), F32)], axis=0)
        if n is None:
            return rows
        odd = lax.broadcasted_iota(I32, (4, 128), 1) % 2 == 1
        swapped = jnp.where(odd, pltpu.roll(rows, 1, 1), pltpu.roll(rows, 127, 1))
        return rows * rot[n, 0][0:4] + swapped * rot[n, 1][0:4]

    def mac(acc, n, a_pair, b_pair):
        (ar, ai), (br, bi) = a_pair, b_pair
        acc[2 * n] = acc[2 * n] + (ar * br + ai * bi)
        acc[2 * n + 1] = acc[2 * n + 1] + (ar * bi - ai * br)

    total = [[jnp.zeros((8, 128), F32) for _ in range(3)] for _ in range(2)]

    def own_pairs(rr, n, acc):
        acc = list(acc)
        for a in range(3):
            re_at, im_at = n + 6 * a, 18 + n + 6 * a
            mac(acc, 0, (left[rr, re_at], left[rr, im_at]), (left[0, re_at], left[0, im_at]))
        return tuple(acc)

    def regular(kinds_at, add, groups, total):
        for rr in range(4):
            zero = tuple(jnp.zeros((8, 128), F32) for _ in range(2 * len(kinds_at)))
            sums = lax.fori_loop(0, 6, functools.partial(add, rr), zero, unroll=True)
            for ri in range(2):
                lines = {k: lane_sum(sums[2 * n + ri]) for n, k in enumerate(kinds_at)}
                for m in range(3):
                    entry = table[m, rr * 2 + ri]
                    for g, ks in enumerate(groups):
                        if ks:
                            total[g][m] = total[g][m] + entry * pick({k: lines[k] for k in ks}, m)

    regular((0,), own_pairs, ((0,), ()), total)

    def link(ref, slot):
        block = ref[slot].astype(F32)
        return [
            [tuple(jnp.broadcast_to(block[3 * a + b, ri : ri + 1, :], (8, 128)) for ri in range(2)) for b in range(3)]
            for a in range(3)
        ]

    def product(one, two):
        def entry(a, c):
            re = im = None
            for b in range(3):
                (pr, pi), (qr, qi) = one[a][b], two[b][c]
                r2, i2 = pr * qr - pi * qi, pr * qi + pi * qr
                re, im = (r2, i2) if b == 0 else (re + r2, im + i2)
            return re, im

        return [[entry(a, c) for c in range(3)] for a in range(3)]

    def keep(ref, line, matrix, dagger=False):
        for a in range(3):
            for b in range(3):
                re, im = matrix[b][a] if dagger else matrix[a][b]
                ref[line, (a * 3 + b) * 2] = re
                ref[line, (a * 3 + b) * 2 + 1] = -im if dagger else im

    def transport(load, lines, line, store):
        got = [[load(ri * 3 + b) for ri in range(2)] for b in range(3)]
        for half in range(2):
            part = [[v[half * 8 : half * 8 + 8] for v in pair] for pair in got]
            for a in range(3):
                re = im = None
                for b in range(3):
                    if lines is None:
                        re, im = part[a]
                        break
                    wr, wi = lines[line, (a * 3 + b) * 2], lines[line, (a * 3 + b) * 2 + 1]
                    vr, vi = part[b]
                    r2, i2 = wr * vr - wi * vi, wr * vi + wi * vr
                    re, im = (r2, i2) if b == 0 else (re + r2, im + i2)
                store(a, half, re, im)

    def bring(slot, line):
        @pl.loop(0, 3)
        def _(q):
            def load(block):
                return sbuf[slot, block, pl.ds(pl.multiple_of(q * 16, 16), 16), :].astype(F32)

            def store(a, half, re, im):
                fields[line, a * 6 + q * 2 + half] = re
                fields[line, 18 + a * 6 + q * 2 + half] = im

            transport(load, wil, line, store)

    def clear(line):
        @pl.loop(0, 36)
        def _(n):
            fields[line, n] = jnp.zeros((8, 128), F32)

    keep(wil, 0, link(ubuf, 0))
    for n in (3, 4, 5):
        pl.when(comes[n])(halo[n].wait_recv)

    @pl.when(comes[1])
    def _():
        halo[1].wait_recv()
        bring(1, 0)

    @pl.when(comes[0])
    def _():
        keep(wil, 1, product(link(ubuf, 0), link(ubuf, 1)))
        halo[0].wait_recv()
        bring(2, 1)

    for line, n in ((0, 1), (1, 0)):
        @pl.when(jnp.logical_not(comes[n]))
        def _():
            clear(line)

    def ahead_pairs(rr, n, acc):
        acc = list(acc)
        for a in range(3):
            re_at, im_at = n + 6 * a, 18 + n + 6 * a
            here = (left[rr, re_at], left[rr, im_at])
            mac(acc, 0, here, (fields[0, re_at], fields[0, im_at]))
            mac(acc, 1, here, (fields[1, re_at], fields[1, im_at]))
        return tuple(acc)

    def behind_pairs(rr, n, acc):
        acc = list(acc)
        for a in range(3):
            re_at, im_at = n + 6 * a, 18 + n + 6 * a
            behind = (roll4(fields[2, re_at], rr), roll4(fields[2, im_at], rr))
            mac(acc, 0, behind, (fields[0, re_at], fields[0, im_at]))
            mac(acc, 1, behind, (fields[1, re_at], fields[1, im_at]))
        return tuple(acc)

    regular((1, 2), ahead_pairs, ((1, 2), ()), total)

    @pl.when(comes[2])
    def _():
        keep(wil, 2, product(link(ubuf, 3), link(ubuf, 2)), dagger=True)
        halo[2].wait_recv()
        bring(3, 2)

    pl.when(jnp.logical_not(comes[2]))(lambda: clear(2))
    regular((3, 4), behind_pairs, ((), (3, 4)), total)
    mine[...] = turned(total[0], None) + turned(total[1], 4)

    @pl.when(is_worker)
    def _():
        def bring_cross(n, line):
            def load(block):
                return xbuf[n, block].astype(F32)

            def store(a, half, re, im):
                xfields[n, a * 2 + half] = re
                xfields[n, 6 + a * 2 + half] = im

            transport(load, None if line is None else xwil, line, store)

        bulk(xlink.at[pl.ds(0, 4)], recv_l.at[0]).wait_recv()
        line = link(xlink, 3)
        keep(xwil, 3, line, dagger=True)
        for n in (2, 1, 0):
            line = product(link(xlink, n), line)
            keep(xwil, n, line, dagger=True)
        bulk(xbuf.at[pl.ds(0, 4)], recv_x.at[0]).wait_recv()
        for n in range(4):
            bring_cross(n, n)
        bulk(xlink.at[pl.ds(4, 4)], recv_l.at[1]).wait_recv()
        line = link(xlink, 4)
        keep(xwil, 4, line)
        for n in (5, 6):
            line = product(line, link(xlink, n))
            keep(xwil, n, line)
        bulk(xbuf.at[pl.ds(4, 4)], recv_x.at[1]).wait_recv()
        for n in range(4, 8):
            bring_cross(n, None if n == 4 else n - 1)

        cross = [(i, j) for i in range(4) for j in range(i + 1)]
        total = [[jnp.zeros((8, 128), F32) for _ in range(3)] for _ in range(4)]
        for rr in range(4):
            def add(n, acc):
                acc = list(acc)
                ahead = [(xfields[4 + j, n], xfields[4 + j, 6 + n]) for j in range(4)]
                for i in range(4):
                    behind = (roll4(xfields[i, n], rr), roll4(xfields[i, 6 + n], rr))
                    for j in range(i + 1):
                        mac(acc, cross.index((i, j)), behind, ahead[j])
                return tuple(acc)

            sums = lax.fori_loop(0, 6, add, tuple(jnp.zeros((8, 128), F32) for _ in range(20)), unroll=True)
            for ri in range(2):
                lines = [lane_sum(sums[2 * n + ri]) for n in range(10)]
                for m in range(3):
                    entry = table[m, rr * 2 + ri]
                    for i in range(4):
                        at_k = {4 - i + j: lines[cross.index((i, j))] for j in range(i + 1)}
                        total[i][m] = total[i][m] + entry * pick(at_k, m)
        mine[...] = mine[...] + ((turned(total[0], 0) + turned(total[1], 1)) + (turned(total[2], 2) + turned(total[3], 3)))

    def to_centre():
        return pltpu.make_async_remote_copy(
            src_ref=mine, dst_ref=slot_b.at[chip * 2 + core], send_sem=send_b, recv_sem=recv_b,
            device_id={"gy": 0, "gz_1": 0, "gz_2": 1}, device_id_type=MESH,
        )

    def to_plane(n):
        return pltpu.make_async_remote_copy(
            src_ref=sum_b, dst_ref=slot_c.at[column], send_sem=send_c, recv_sem=recv_c,
            device_id={"ta": n // 4, "gz_0": n % 4}, device_id_type=MESH,
        )

    def to_chip(dst, side):
        return pltpu.make_async_remote_copy(
            src_ref=final.at[0], dst_ref=final.at[0], send_sem=send_d, recv_sem=recv_d,
            device_id={"gy": dst // 8, "gz_1": dst % 8, "gz_2": side}, device_id_type=MESH,
        )

    outward = [(0, 0)] + [(c, side) for c in (1, 2, 3, 4, 24, 8, 16) for side in (0, 1)]
    heads = [(chip == 4, 4), ((chip == 8) | (chip == 16) | (chip == 24), 8)]

    @pl.when(jnp.logical_not(is_centre))
    def _():
        to_centre().start()
        to_chip(0, 1).wait_recv()

        for is_head, end in heads:
            @pl.when(is_head)
            def _():
                for n in range(1, end):
                    to_chip(chip + n, core).start()

    @pl.when(is_centre)
    def _():
        acc = mine[...]
        bulk(slot_b.at[pl.ds(0, 63)], recv_b).wait_recv()
        for n in range(64):
            if n != 1:
                acc = acc + slot_b[n]
        sum_b[...] = acc

        for n in range(16):
            pl.when(column != n)(to_plane(n).start)
        slot_c[column] = acc
        bulk(slot_c.at[pl.ds(0, 15)], recv_c).wait_recv()
        slices = []
        for t in range(4):
            acc = slot_c[4 * t]
            for q in range(1, 4):
                acc = acc + slot_c[4 * t + q]
            slices.append(acc)
        quarter = lax.broadcasted_iota(I32, (4, 128), 1) // 32
        for q in range(4):
            rows = slices[0] if q == 0 else pltpu.roll(slices[0], (128 - 32 * q) % 128, 1)
            for t in range(1, 4):
                turned = slices[t] if t == q else pltpu.roll(slices[t], (128 + 32 * (t - q)) % 128, 1)
                rows = jnp.where(quarter == t, turned, rows)
            for m in range(3):
                if m * 4 + q < 9:
                    final[0, m * 4 + q] = rows[m : m + 1, :]
        for dst, side in outward:
            to_chip(dst, side).start()

    for j in range(9):
        out[j : j + 1, :] = final[0, j]

    for n in range(6):
        pl.when(goes[n])(halo[n].wait_send)
    @pl.when(is_member)
    def _():
        bulk(sbuf.at[0], send_x.at[0]).wait_send()
        bulk(ubuf.at[pl.ds(0, 3)], send_x.at[1]).wait_send()

    @pl.when(jnp.logical_not(is_centre))
    def _():
        to_centre().wait_send()

        for is_head, end in heads:
            @pl.when(is_head)
            def _():
                bulk(final.at[pl.ds(0, end - 1)], send_d).wait_send()

    @pl.when(is_centre)
    def _():
        bulk(slot_c.at[pl.ds(0, 15)], send_c).wait_send()
        bulk(final, send_d).wait_send()


def body(propagator, links, source_z, displacements, momenta, gamma_perm, gamma_phase):
    nz = lax.axis_size(GZ)
    sites_total = propagator.shape[6] * lax.axis_size("gy") * nz
    scaling = 1.0 / (24.0 * math.sqrt(sites_total))
    prop = jnp.transpose(propagator, (0, 2, 3, 1, 4, 5, 6)).reshape(6, 48, 128)
    link = jnp.transpose(links, (1, 2, 0, 3, 4, 5)).reshape(9, 2, 128)
    hbm = pl.BlockSpec(memory_space=pl.ANY)
    dma = pltpu.SemaphoreType.DMA
    out = pl.pallas_call(
        functools.partial(kernel, nz, scaling),
        out_shape=jax.ShapeDtypeStruct((9, 128), F32),
        in_specs=[hbm] * 7,
        out_specs=pl.BlockSpec(memory_space=pltpu.VMEM),
        scratch_shapes=[
            pltpu.SMEM((4, 4), I32),
            pltpu.SMEM((9,), I32),
            pltpu.SMEM((4,), I32),
            pltpu.SMEM((4, 4), I32),
            pltpu.SMEM((4, 4), I32),
            pltpu.VMEM((4, 6, 48, 128), jnp.bfloat16),
            pltpu.VMEM((4, 9, 2, 128), jnp.bfloat16),
            pltpu.VMEM((4, 36, 8, 128), F32),
            pltpu.VMEM((3, 36, 8, 128), F32),
            pltpu.VMEM((3, 18, 8, 128), F32),
            pltpu.VMEM((3, 8, 8, 128), F32),
            pltpu.VMEM((3, 8, 128), I32),
            pltpu.VMEM((4, 128), F32),
            pltpu.VMEM((64, 4, 128), F32),
            pltpu.VMEM((4, 128), F32),
            pltpu.VMEM((16, 4, 128), F32),
            pltpu.VMEM((15, 9, 1, 128), F32),
            pltpu.VMEM((8, 6, 16, 128), jnp.bfloat16),
            pltpu.VMEM((8, 9, 2, 128), jnp.bfloat16),
            pltpu.VMEM((8, 12, 8, 128), F32),
            pltpu.VMEM((7, 18, 8, 128), F32),
            pltpu.VMEM((5, 2, 8, 128), F32),
            dma((7,)),
            dma((6,)),
            dma((6,)),
            dma,
            dma,
            dma,
            dma,
            dma,
            dma,
            dma((2,)),
            dma((2,)),
            dma((2,)),
        ],
        compiler_params=pltpu.CompilerParams(collective_id=0, has_side_effects=True),
    )(prop, link, source_z, displacements, momenta, gamma_perm, gamma_phase)
    return jnp.transpose(out.reshape(9, 4, 4, 4, 2), (1, 0, 2, 3, 4))


def solution(mesh):
    torus = Mesh(
        mesh.devices.reshape(mesh.shape["ta"], 4, 8, 2, mesh.shape["gy"]),
        ("ta", "gz_0", "gz_1", "gz_2", "gy"),
    )
    in_specs = (
        P(None, None, None, None, "ta", GZ, "gy"),
        P(None, None, None, "ta", GZ, "gy"),
        P(),
        P(),
        P(),
        P(),
        P(),
    )
    return jax.shard_map(body, mesh=torus, in_specs=in_specs, out_specs=P(), check_vma=False)
```

```python
import functools
import math

import jax
import jax.numpy as jnp
from jax import lax
from jax.experimental import pallas as pl
from jax.experimental.pallas import tpu as pltpu
from jax.sharding import Mesh
from jax.sharding import PartitionSpec as P

GZ = ("gz_0", "gz_1", "gz_2")
MESH = pl.DeviceIdType.MESH
F32 = jnp.float32
I32 = jnp.int32


def roll4(x, r):
    if r == 0:
        return x
    spin = lax.broadcasted_iota(I32, (8, 128), 0) % 4
    return jnp.where(spin < 4 - r, pltpu.roll(x, 8 - r, 0), pltpu.roll(x, 4 - r, 0))


def kernel(
    nz, scaling, s_hbm, u_hbm, *refs,
):
    ints_hbm, out, ints = refs[:5], refs[5], refs[6:11]
    sbuf, ubuf, left, fields, wil, table, kind, mine, slot_b, sum_b, slot_c, final, xbuf, xlink, xfields, xwil, rot = refs[11:28]
    load_sem, send_sem, recv_sem, send_b, recv_b, send_c, recv_c, send_d, recv_d, send_x, recv_x, recv_l = refs[28:]
    source_z, displacements, momenta, perm, phase = ints
    x = lax.axis_index("ta")
    gy0 = lax.axis_index("gz_0")
    lo = lax.axis_index("gz_1")
    core = lax.axis_index("gz_2")
    hi = lax.axis_index("gy")
    z = gy0 * 16 + lo * 2 + core
    chip = hi * 8 + lo
    is_centre = (chip == 0) & (core == 1)
    column = x * 4 + gy0
    place = lo * 2 + core
    at_end = hi >= 2
    is_member = (place >= 12) | (place < 4)
    member = jnp.where(place >= 12, place - 12, place + 4)
    row_a = jnp.where(place >= 12, gy0, (gy0 + 3) % 4)
    first = jnp.where(at_end, 6, 0)
    is_worker = (place >= first) & (place < first + 3)

    def seat(row, spot):
        return {"gz_0": row % 4, "gz_1": spot // 2, "gz_2": spot % 2}

    def along(offset):
        w = (z + (offset + nz)) % nz
        return {"gz_0": w // 16, "gz_1": (w // 2) % 8, "gz_2": w % 2}

    loads = [pltpu.make_async_copy(s_hbm, sbuf.at[0], load_sem.at[0]), pltpu.make_async_copy(u_hbm, ubuf.at[0], load_sem.at[1])]
    loads += [pltpu.make_async_copy(ints_hbm[n], ints[n], load_sem.at[2 + n]) for n in range(5)]
    for load in loads:
        load.start()

    barrier = pltpu.get_barrier_semaphore()
    @pl.when(is_worker)
    def _():
        row_w = gy0 + jnp.where(at_end, 3, 0)
        for n in range(4):
            other = seat(row_w + jnp.where(at_end, 1, 0), jnp.where(at_end, n, 12 + n))
            pl.semaphore_signal(barrier, inc=1, device_id=other, device_id_type=MESH)
        for n in range(4):
            other = seat(row_w + jnp.where(at_end, 0, 1), jnp.where(at_end, 12 + n, n))
            pl.semaphore_signal(barrier, inc=1, device_id=other, device_id_type=MESH)

    heard = jnp.where(is_centre, 15, 1) + jnp.where(is_member, 3, 0)
    for offset in (-2, -1, 1, 2):
        inside = (place + offset >= 0) & (place + offset < 16)
        heard = heard + jnp.where(inside, 1, 0)

        @pl.when(inside)
        def _():
            pl.semaphore_signal(barrier, inc=1, device_id=along(offset), device_id_type=MESH)

    @pl.when(is_centre)
    def _():
        @pl.loop(1, 64)
        def _(n):
            other = {"gy": (64 - n) // 16, "gz_1": (64 - n) // 2 % 8, "gz_2": (64 - n) % 2}
            pl.when(n != 63)(lambda: pl.semaphore_signal(barrier, inc=1, device_id=other, device_id_type=MESH))

        pl.semaphore_signal(barrier, inc=1, device_id={"gz_2": 0}, device_id_type=MESH)
        for n in range(16):
            other = {"ta": n // 4, "gz_0": n % 4}
            pl.when(column != n)(
                functools.partial(pl.semaphore_signal, barrier, inc=1, device_id=other, device_id_type=MESH)
            )

    loads[0].wait()
    loads[1].wait()
    pl.semaphore_wait(barrier, heard)

    def to(buf, n, dst, offset):
        return pltpu.make_async_remote_copy(
            src_ref=buf.at[0], dst_ref=buf.at[dst], send_sem=send_sem.at[n], recv_sem=recv_sem.at[n],
            device_id=along(offset), device_id_type=MESH,
        )

    halo = [
        to(sbuf, 0, 2, -2), to(sbuf, 1, 1, -1), to(sbuf, 2, 3, 2),
        to(ubuf, 3, 1, -1), to(ubuf, 4, 2, 1), to(ubuf, 5, 3, 2),
    ]
    offsets = (-2, -1, 2, -1, 1, 2)
    goes = [(place + o >= 0) & (place + o < 16) for o in offsets]
    comes = [(place - o >= 0) & (place - o < 16) for o in offsets]
    def bulk(ref, sem):
        return pltpu.make_async_remote_copy(
            src_ref=ref, dst_ref=ref, send_sem=sem, recv_sem=sem, device_id={"gy": (hi + 1) % 4}, device_id_type=MESH
        )

    def to_worker(n):
        third, spot = n % 3, first + n % 3
        row = row_a + jnp.where(at_end, 1, 0)
        src = sbuf.at[0, :, pl.ds(third * 16, 16), :] if n < 3 else ubuf.at[0]
        dst, sem = (xbuf, recv_x) if n < 3 else (xlink, recv_l)
        side = jnp.where(place >= 12, 0, 1)
        return pltpu.make_async_remote_copy(
            src_ref=src, dst_ref=dst.at[member], send_sem=send_x.at[n // 3], recv_sem=sem.at[side],
            device_id=seat(row, spot), device_id_type=MESH,
        )
    @pl.when(is_member)
    def _():
        for n in (3, 4, 5, 0, 1, 2):
            to_worker(n).start()

    for n in (3, 4, 5, 1, 0, 2):
        pl.when(goes[n])(halo[n].start)

    for load in loads[2:]:
        load.wait()

    sub = lax.broadcasted_iota(I32, (8, 128), 0)
    lane = lax.broadcasted_iota(I32, (8, 128), 1)
    u_id = sub % 4
    g_id = (lane % 32) // 8
    p_id = (lane // 2) % 4
    c_id = lane % 2
    perm_t = jnp.zeros((8, 128), I32)
    phase_t = jnp.zeros((8, 128), I32)
    for g in range(4):
        for s in range(4):
            here = (g_id == g) & (u_id == s)
            perm_t = jnp.where(here, perm[g, s], perm_t)
            phase_t = jnp.where(here, phase[g, s], phase_t)
    mom = jnp.zeros((8, 128), I32)
    src = jnp.zeros((8, 128), I32)
    for p in range(4):
        mom = jnp.where(p_id == p, momenta[p], mom)
        src = jnp.where(p_id == p, source_z[x, p], src)
    corner = jnp.where(at_end, -4 - place, 12 - place)
    for n in range(5):
        turns = (mom * (corner + n if n < 4 else -2)) & (nz - 1)
        angle = turns.astype(F32) * (2.0 * math.pi / nz)
        sine = jnp.sin(angle)
        rot[n, 0] = jnp.cos(angle)
        rot[n, 1] = jnp.where(c_id == 0, sine, -sine)
    for m in range(3):
        j_id = m * 4 + lane // 32
        shift = jnp.zeros((8, 128), I32)
        for j in range(4 * m, min(4 * m + 4, 9)):
            shift = jnp.where(j_id == j, displacements[j] - 4, shift)
        neg = shift < 0
        k_id = jnp.where(neg, -shift, shift)
        at = z + jnp.where(neg, k_id, 0)
        turns = (mom * (at - src)) & (nz - 1)
        angle = turns.astype(F32) * (2.0 * math.pi / nz)
        cosine = jnp.cos(angle) * scaling
        sine = jnp.sin(angle) * scaling
        kind[m] = k_id
        for rr in range(4):
            s_id = (u_id + rr) % 4
            perm_r = pltpu.roll(perm_t, 8 - rr, 0) if rr else perm_t
            phase_r = pltpu.roll(phase_t, 8 - rr, 0) if rr else phase_t
            match = jnp.where(neg, perm_t, perm_r) == jnp.where(neg, s_id, u_id)
            power = jnp.where(neg, phase_t, phase_r)
            for ri in range(2):
                if ri == 0:
                    turn = jnp.where(c_id == 0, 0, 3)
                else:
                    turn = jnp.where(c_id == 0, jnp.where(neg, 3, 1), jnp.where(neg, 2, 0))
                h = (power + turn) & 3
                value = jnp.where((h & 1) == 1, sine, cosine)
                value = jnp.where(h >= 2, -value, value)
                table[m, rr * 2 + ri] = jnp.where(match & (j_id < 9), value, 0.0)

    @pl.loop(0, 18)
    def _(n):
        rows = sbuf[0, n // 3, pl.ds(pl.multiple_of(n % 3 * 16, 16), 16), :].astype(F32)
        for half in range(2):
            for rr in range(4):
                left[rr, 2 * n + half] = roll4(rows[half * 8 : half * 8 + 8], rr)

    kinds = [kind[m] for m in range(3)]

    def lane_sum(v):
        return jnp.broadcast_to(jnp.sum(v, axis=1, keepdims=True), (8, 128))

    def pick(lines, m):
        value = jnp.zeros((8, 128), F32)
        for k, line in lines.items():
            value = jnp.where(kinds[m] == k, line, value)
        return value

    def turned(total, n):
        rows = jnp.concatenate([jnp.sum(t, axis=0, keepdims=True) for t in total] + [jnp.zeros((1, 128), F32)], axis=0)
        if n is None:
            return rows
        odd = lax.broadcasted_iota(I32, (4, 128), 1) % 2 == 1
        swapped = jnp.where(odd, pltpu.roll(rows, 1, 1), pltpu.roll(rows, 127, 1))
        return rows * rot[n, 0][0:4] + swapped * rot[n, 1][0:4]

    def mac(acc, n, a_pair, b_pair):
        (ar, ai), (br, bi) = a_pair, b_pair
        acc[2 * n] = acc[2 * n] + (ar * br + ai * bi)
        acc[2 * n + 1] = acc[2 * n + 1] + (ar * bi - ai * br)

    total = [[jnp.zeros((8, 128), F32) for _ in range(3)] for _ in range(2)]

    def own_pairs(rr, n, acc):
        acc = list(acc)
        for a in range(3):
            re_at, im_at = n + 6 * a, 18 + n + 6 * a
            mac(acc, 0, (left[rr, re_at], left[rr, im_at]), (left[0, re_at], left[0, im_at]))
        return tuple(acc)

    def regular(kinds_at, add, groups, total):
        for rr in range(4):
            zero = tuple(jnp.zeros((8, 128), F32) for _ in range(2 * len(kinds_at)))
            sums = lax.fori_loop(0, 6, functools.partial(add, rr), zero, unroll=True)
            for ri in range(2):
                lines = {k: lane_sum(sums[2 * n + ri]) for n, k in enumerate(kinds_at)}
                for m in range(3):
                    entry = table[m, rr * 2 + ri]
                    for g, ks in enumerate(groups):
                        if ks:
                            total[g][m] = total[g][m] + entry * pick({k: lines[k] for k in ks}, m)

    regular((0,), own_pairs, ((0,), ()), total)

    def link(ref, slot):
        block = ref[slot].astype(F32)
        return [
            [tuple(jnp.broadcast_to(block[3 * a + b, ri : ri + 1, :], (8, 128)) for ri in range(2)) for b in range(3)]
            for a in range(3)
        ]

    def product(one, two):
        def entry(a, c):
            re = im = None
            for b in range(3):
                (pr, pi), (qr, qi) = one[a][b], two[b][c]
                r2, i2 = pr * qr - pi * qi, pr * qi + pi * qr
                re, im = (r2, i2) if b == 0 else (re + r2, im + i2)
            return re, im

        return [[entry(a, c) for c in range(3)] for a in range(3)]

    def keep(ref, line, matrix, dagger=False):
        for a in range(3):
            for b in range(3):
                re, im = matrix[b][a] if dagger else matrix[a][b]
                ref[line, (a * 3 + b) * 2] = re
                ref[line, (a * 3 + b) * 2 + 1] = -im if dagger else im

    def transport(load, lines, line, store):
        got = [[load(ri * 3 + b) for ri in range(2)] for b in range(3)]
        for half in range(2):
            part = [[v[half * 8 : half * 8 + 8] for v in pair] for pair in got]
            for a in range(3):
                re = im = None
                for b in range(3):
                    if lines is None:
                        re, im = part[a]
                        break
                    wr, wi = lines[line, (a * 3 + b) * 2], lines[line, (a * 3 + b) * 2 + 1]
                    vr, vi = part[b]
                    r2, i2 = wr * vr - wi * vi, wr * vi + wi * vr
                    re, im = (r2, i2) if b == 0 else (re + r2, im + i2)
                store(a, half, re, im)

    def bring(slot, line):
        @pl.loop(0, 3)
        def _(q):
            def load(block):
                return sbuf[slot, block, pl.ds(pl.multiple_of(q * 16, 16), 16), :].astype(F32)

            def store(a, half, re, im):
                fields[line, a * 6 + q * 2 + half] = re
                fields[line, 18 + a * 6 + q * 2 + half] = im

            transport(load, wil, line, store)

    def clear(line):
        @pl.loop(0, 36)
        def _(n):
            fields[line, n] = jnp.zeros((8, 128), F32)

    keep(wil, 0, link(ubuf, 0))
    for n in (3, 4, 5):
        pl.when(comes[n])(halo[n].wait_recv)

    @pl.when(comes[1])
    def _():
        halo[1].wait_recv()
        bring(1, 0)

    @pl.when(comes[0])
    def _():
        keep(wil, 1, product(link(ubuf, 0), link(ubuf, 1)))
        halo[0].wait_recv()
        bring(2, 1)

    for line, n in ((0, 1), (1, 0)):
        @pl.when(jnp.logical_not(comes[n]))
        def _():
            clear(line)

    def ahead_pairs(rr, n, acc):
        acc = list(acc)
        for a in range(3):
            re_at, im_at = n + 6 * a, 18 + n + 6 * a
            here = (left[rr, re_at], left[rr, im_at])
            mac(acc, 0, here, (fields[0, re_at], fields[0, im_at]))
            mac(acc, 1, here, (fields[1, re_at], fields[1, im_at]))
        return tuple(acc)

    def behind_pairs(rr, n, acc):
        acc = list(acc)
        for a in range(3):
            re_at, im_at = n + 6 * a, 18 + n + 6 * a
            behind = (roll4(fields[2, re_at], rr), roll4(fields[2, im_at], rr))
            mac(acc, 0, behind, (fields[0, re_at], fields[0, im_at]))
            mac(acc, 1, behind, (fields[1, re_at], fields[1, im_at]))
        return tuple(acc)

    regular((1, 2), ahead_pairs, ((1, 2), ()), total)

    @pl.when(comes[2])
    def _():
        keep(wil, 2, product(link(ubuf, 3), link(ubuf, 2)), dagger=True)
        halo[2].wait_recv()
        bring(3, 2)

    pl.when(jnp.logical_not(comes[2]))(lambda: clear(2))
    regular((3, 4), behind_pairs, ((), (3, 4)), total)
    mine[...] = turned(total[0], None) + turned(total[1], 4)

    @pl.when(is_worker)
    def _():
        def bring_cross(n, line):
            def load(block):
                return xbuf[n, block].astype(F32)

            def store(a, half, re, im):
                xfields[n, a * 2 + half] = re
                xfields[n, 6 + a * 2 + half] = im

            transport(load, None if line is None else xwil, line, store)

        bulk(xlink.at[pl.ds(0, 4)], recv_l.at[0]).wait_recv()
        line = link(xlink, 3)
        keep(xwil, 3, line, dagger=True)
        for n in (2, 1, 0):
            line = product(link(xlink, n), line)
            keep(xwil, n, line, dagger=True)
        bulk(xbuf.at[pl.ds(0, 4)], recv_x.at[0]).wait_recv()
        for n in range(4):
            bring_cross(n, n)
        bulk(xlink.at[pl.ds(4, 4)], recv_l.at[1]).wait_recv()
        line = link(xlink, 4)
        keep(xwil, 4, line)
        for n in (5, 6):
            line = product(line, link(xlink, n))
            keep(xwil, n, line)
        bulk(xbuf.at[pl.ds(4, 4)], recv_x.at[1]).wait_recv()
        for n in range(4, 8):
            bring_cross(n, None if n == 4 else n - 1)

        cross = [(i, j) for i in range(4) for j in range(i + 1)]
        total = [[jnp.zeros((8, 128), F32) for _ in range(3)] for _ in range(4)]
        for rr in range(4):
            def add(n, acc):
                acc = list(acc)
                ahead = [(xfields[4 + j, n], xfields[4 + j, 6 + n]) for j in range(4)]
                for i in range(4):
                    behind = (roll4(xfields[i, n], rr), roll4(xfields[i, 6 + n], rr))
                    for j in range(i + 1):
                        mac(acc, cross.index((i, j)), behind, ahead[j])
                return tuple(acc)

            sums = lax.fori_loop(0, 6, add, tuple(jnp.zeros((8, 128), F32) for _ in range(20)), unroll=True)
            for ri in range(2):
                lines = [lane_sum(sums[2 * n + ri]) for n in range(10)]
                for m in range(3):
                    entry = table[m, rr * 2 + ri]
                    for i in range(4):
                        at_k = {4 - i + j: lines[cross.index((i, j))] for j in range(i + 1)}
                        total[i][m] = total[i][m] + entry * pick(at_k, m)
        mine[...] = mine[...] + ((turned(total[0], 0) + turned(total[1], 1)) + (turned(total[2], 2) + turned(total[3], 3)))

    def to_centre():
        return pltpu.make_async_remote_copy(
            src_ref=mine, dst_ref=slot_b.at[chip * 2 + core], send_sem=send_b, recv_sem=recv_b,
            device_id={"gy": 0, "gz_1": 0, "gz_2": 1}, device_id_type=MESH,
        )

    def to_plane(n):
        return pltpu.make_async_remote_copy(
            src_ref=sum_b, dst_ref=slot_c.at[column], send_sem=send_c, recv_sem=recv_c,
            device_id={"ta": n // 4, "gz_0": n % 4}, device_id_type=MESH,
        )

    def to_chip(dst, side):
        return pltpu.make_async_remote_copy(
            src_ref=final.at[0], dst_ref=final.at[0], send_sem=send_d, recv_sem=recv_d,
            device_id={"gy": dst // 8, "gz_1": dst % 8, "gz_2": side}, device_id_type=MESH,
        )

    outward = [(0, 0)] + [(c, side) for c in (1, 2, 3, 4, 24, 8, 16) for side in (0, 1)]
    heads = [(chip == 4, 4), ((chip == 8) | (chip == 16) | (chip == 24), 8)]

    @pl.when(jnp.logical_not(is_centre))
    def _():
        to_centre().start()
        to_chip(0, 1).wait_recv()

        for is_head, end in heads:
            @pl.when(is_head)
            def _():
                for n in range(1, end):
                    to_chip(chip + n, core).start()

    @pl.when(is_centre)
    def _():
        acc = mine[...]
        bulk(slot_b.at[pl.ds(0, 63)], recv_b).wait_recv()
        for n in range(64):
            if n != 1:
                acc = acc + slot_b[n]
        sum_b[...] = acc

        for n in range(16):
            pl.when(column != n)(to_plane(n).start)
        slot_c[column] = acc
        bulk(slot_c.at[pl.ds(0, 15)], recv_c).wait_recv()
        slices = []
        for t in range(4):
            acc = slot_c[4 * t]
            for q in range(1, 4):
                acc = acc + slot_c[4 * t + q]
            slices.append(acc)
        quarter = lax.broadcasted_iota(I32, (4, 128), 1) // 32
        for q in range(4):
            rows = slices[0] if q == 0 else pltpu.roll(slices[0], (128 - 32 * q) % 128, 1)
            for t in range(1, 4):
                turned = slices[t] if t == q else pltpu.roll(slices[t], (128 + 32 * (t - q)) % 128, 1)
                rows = jnp.where(quarter == t, turned, rows)
            for m in range(3):
                if m * 4 + q < 9:
                    final[0, m * 4 + q] = rows[m : m + 1, :]
        for dst, side in outward:
            to_chip(dst, side).start()

    for j in range(9):
        out[j : j + 1, :] = final[0, j]

    for n in range(6):
        pl.when(goes[n])(halo[n].wait_send)
    @pl.when(is_member)
    def _():
        bulk(sbuf.at[0], send_x.at[0]).wait_send()
        bulk(ubuf.at[pl.ds(0, 3)], send_x.at[1]).wait_send()

    @pl.when(jnp.logical_not(is_centre))
    def _():
        to_centre().wait_send()

        for is_head, end in heads:
            @pl.when(is_head)
            def _():
                bulk(final.at[pl.ds(0, end - 1)], send_d).wait_send()

    @pl.when(is_centre)
    def _():
        bulk(slot_c.at[pl.ds(0, 15)], send_c).wait_send()
        bulk(final, send_d).wait_send()


def body(propagator, links, source_z, displacements, momenta, gamma_perm, gamma_phase):
    nz = lax.axis_size(GZ)
    sites_total = propagator.shape[6] * lax.axis_size("gy") * nz
    scaling = 1.0 / (24.0 * math.sqrt(sites_total))
    prop = jnp.transpose(propagator, (0, 2, 3, 1, 4, 5, 6)).reshape(6, 48, 128)
    link = jnp.transpose(links, (1, 2, 0, 3, 4, 5)).reshape(9, 2, 128)
    hbm = pl.BlockSpec(memory_space=pl.ANY)
    dma = pltpu.SemaphoreType.DMA
    out = pl.pallas_call(
        functools.partial(kernel, nz, scaling),
        out_shape=jax.ShapeDtypeStruct((9, 128), F32),
        in_specs=[hbm] * 7,
        out_specs=pl.BlockSpec(memory_space=pltpu.VMEM),
        scratch_shapes=[
            pltpu.SMEM((4, 4), I32),
            pltpu.SMEM((9,), I32),
            pltpu.SMEM((4,), I32),
            pltpu.SMEM((4, 4), I32),
            pltpu.SMEM((4, 4), I32),
            pltpu.VMEM((4, 6, 48, 128), jnp.bfloat16),
            pltpu.VMEM((4, 9, 2, 128), jnp.bfloat16),
            pltpu.VMEM((4, 36, 8, 128), F32),
            pltpu.VMEM((3, 36, 8, 128), F32),
            pltpu.VMEM((3, 18, 8, 128), F32),
            pltpu.VMEM((3, 8, 8, 128), F32),
            pltpu.VMEM((3, 8, 128), I32),
            pltpu.VMEM((4, 128), F32),
            pltpu.VMEM((64, 4, 128), F32),
            pltpu.VMEM((4, 128), F32),
            pltpu.VMEM((16, 4, 128), F32),
            pltpu.VMEM((15, 9, 1, 128), F32),
            pltpu.VMEM((8, 6, 16, 128), jnp.bfloat16),
            pltpu.VMEM((8, 9, 2, 128), jnp.bfloat16),
            pltpu.VMEM((8, 12, 8, 128), F32),
            pltpu.VMEM((7, 18, 8, 128), F32),
            pltpu.VMEM((5, 2, 8, 128), F32),
            dma((7,)),
            dma((6,)),
            dma((6,)),
            dma,
            dma,
            dma,
            dma,
            dma,
            dma,
            dma((2,)),
            dma((2,)),
            dma((2,)),
        ],
        compiler_params=pltpu.CompilerParams(collective_id=0, has_side_effects=True),
    )(prop, link, source_z, displacements, momenta, gamma_perm, gamma_phase)
    return jnp.transpose(out.reshape(9, 4, 4, 4, 2), (1, 0, 2, 3, 4))


def solution(mesh):
    torus = Mesh(
        mesh.devices.reshape(mesh.shape["ta"], 4, 8, 2, mesh.shape["gy"]),
        ("ta", "gz_0", "gz_1", "gz_2", "gy"),
    )
    in_specs = (
        P(None, None, None, None, "ta", GZ, "gy"),
        P(None, None, None, "ta", GZ, "gy"),
        P(),
        P(),
        P(),
        P(),
        P(),
    )
    return jax.shard_map(body, mesh=torus, in_specs=in_specs, out_specs=P(), check_vma=False)
```

```python
import functools
import math

import jax
import jax.numpy as jnp
from jax import lax
from jax.experimental import pallas as pl
from jax.experimental.pallas import tpu as pltpu
from jax.sharding import Mesh
from jax.sharding import PartitionSpec as P

GZ = ("gz_0", "gz_1", "gz_2")
MESH = pl.DeviceIdType.MESH
F32 = jnp.float32
I32 = jnp.int32


def roll4(x, r):
    if r == 0:
        return x
    spin = lax.broadcasted_iota(I32, (8, 128), 0) % 4
    return jnp.where(spin < 4 - r, pltpu.roll(x, 8 - r, 0), pltpu.roll(x, 4 - r, 0))


def kernel(
    nz, scaling, s_hbm, u_hbm, *refs,
):
    ints_hbm, out, ints = refs[:5], refs[5], refs[6:11]
    sbuf, ubuf, left, fields, wil, table, kind, mine, slot_b, sum_b, slot_c, final, xbuf, xlink, xfields, xwil, rot = refs[11:28]
    load_sem, send_sem, recv_sem, send_b, recv_b, send_c, recv_c, send_d, recv_d, send_x, recv_x, recv_l = refs[28:]
    source_z, displacements, momenta, perm, phase = ints
    x = lax.axis_index("ta")
    gy0 = lax.axis_index("gz_0")
    lo = lax.axis_index("gz_1")
    core = lax.axis_index("gz_2")
    hi = lax.axis_index("gy")
    z = gy0 * 16 + lo * 2 + core
    chip = hi * 8 + lo
    is_centre = (chip == 0) & (core == 1)
    column = x * 4 + gy0
    place = lo * 2 + core
    at_end = hi >= 2
    is_member = (place >= 12) | (place < 4)
    member = jnp.where(place >= 12, place - 12, place + 4)
    row_a = jnp.where(place >= 12, gy0, (gy0 + 3) % 4)
    first = jnp.where(at_end, 7, 0)
    is_worker = (place >= first) & (place < first + 3)

    def seat(row, spot):
        return {"gz_0": row % 4, "gz_1": spot // 2, "gz_2": spot % 2}

    def along(offset):
        w = (z + (offset + nz)) % nz
        return {"gz_0": w // 16, "gz_1": (w // 2) % 8, "gz_2": w % 2}

    loads = [pltpu.make_async_copy(s_hbm, sbuf.at[0], load_sem.at[0]), pltpu.make_async_copy(u_hbm, ubuf.at[0], load_sem.at[1])]
    loads += [pltpu.make_async_copy(ints_hbm[n], ints[n], load_sem.at[2 + n]) for n in range(5)]
    for load in loads:
        load.start()

    barrier = pltpu.get_barrier_semaphore()
    @pl.when(is_worker)
    def _():
        row_w = gy0 + jnp.where(at_end, 3, 0)
        for n in range(4):
            other = seat(row_w + jnp.where(at_end, 1, 0), jnp.where(at_end, n, 12 + n))
            pl.semaphore_signal(barrier, inc=1, device_id=other, device_id_type=MESH)
        for n in range(4):
            other = seat(row_w + jnp.where(at_end, 0, 1), jnp.where(at_end, 12 + n, n))
            pl.semaphore_signal(barrier, inc=1, device_id=other, device_id_type=MESH)

    heard = jnp.where(is_centre, 15, 1) + jnp.where(is_member, 3, 0)
    for offset in (-2, -1, 1, 2):
        inside = (place + offset >= 0) & (place + offset < 16)
        heard = heard + jnp.where(inside, 1, 0)

        @pl.when(inside)
        def _():
            pl.semaphore_signal(barrier, inc=1, device_id=along(offset), device_id_type=MESH)

    @pl.when(is_centre)
    def _():
        @pl.loop(1, 64)
        def _(n):
            other = {"gy": (64 - n) // 16, "gz_1": (64 - n) // 2 % 8, "gz_2": (64 - n) % 2}
            pl.when(n != 63)(lambda: pl.semaphore_signal(barrier, inc=1, device_id=other, device_id_type=MESH))

        pl.semaphore_signal(barrier, inc=1, device_id={"gz_2": 0}, device_id_type=MESH)
        for n in range(16):
            other = {"ta": n // 4, "gz_0": n % 4}
            pl.when(column != n)(
                functools.partial(pl.semaphore_signal, barrier, inc=1, device_id=other, device_id_type=MESH)
            )

    loads[0].wait()
    loads[1].wait()
    pl.semaphore_wait(barrier, heard)

    def to(buf, n, dst, offset):
        return pltpu.make_async_remote_copy(
            src_ref=buf.at[0], dst_ref=buf.at[dst], send_sem=send_sem.at[n], recv_sem=recv_sem.at[n],
            device_id=along(offset), device_id_type=MESH,
        )

    halo = [
        to(sbuf, 0, 2, -2), to(sbuf, 1, 1, -1), to(sbuf, 2, 3, 2),
        to(ubuf, 3, 1, -1), to(ubuf, 4, 2, 1), to(ubuf, 5, 3, 2),
    ]
    offsets = (-2, -1, 2, -1, 1, 2)
    goes = [(place + o >= 0) & (place + o < 16) for o in offsets]
    comes = [(place - o >= 0) & (place - o < 16) for o in offsets]
    def bulk(ref, sem):
        return pltpu.make_async_remote_copy(
            src_ref=ref, dst_ref=ref, send_sem=sem, recv_sem=sem, device_id={"gy": (hi + 1) % 4}, device_id_type=MESH
        )

    def to_worker(n):
        third, spot = n % 3, first + n % 3
        row = row_a + jnp.where(at_end, 1, 0)
        src = sbuf.at[0, :, pl.ds(third * 16, 16), :] if n < 3 else ubuf.at[0]
        dst, sem = (xbuf, recv_x) if n < 3 else (xlink, recv_l)
        side = jnp.where(place >= 12, 0, 1)
        return pltpu.make_async_remote_copy(
            src_ref=src, dst_ref=dst.at[member], send_sem=send_x.at[n // 3], recv_sem=sem.at[side],
            device_id=seat(row, spot), device_id_type=MESH,
        )
    @pl.when(is_member)
    def _():
        for n in (3, 4, 5, 0, 1, 2):
            to_worker(n).start()

    for n in (3, 4, 5, 1, 0, 2):
        pl.when(goes[n])(halo[n].start)

    for load in loads[2:]:
        load.wait()

    sub = lax.broadcasted_iota(I32, (8, 128), 0)
    lane = lax.broadcasted_iota(I32, (8, 128), 1)
    u_id = sub % 4
    g_id = (lane % 32) // 8
    p_id = (lane // 2) % 4
    c_id = lane % 2
    perm_t = jnp.zeros((8, 128), I32)
    phase_t = jnp.zeros((8, 128), I32)
    for g in range(4):
        for s in range(4):
            here = (g_id == g) & (u_id == s)
            perm_t = jnp.where(here, perm[g, s], perm_t)
            phase_t = jnp.where(here, phase[g, s], phase_t)
    mom = jnp.zeros((8, 128), I32)
    src = jnp.zeros((8, 128), I32)
    for p in range(4):
        mom = jnp.where(p_id == p, momenta[p], mom)
        src = jnp.where(p_id == p, source_z[x, p], src)
    corner = jnp.where(at_end, -4 - place, 12 - place)
    for n in range(5):
        turns = (mom * (corner + n if n < 4 else -2)) & (nz - 1)
        angle = turns.astype(F32) * (2.0 * math.pi / nz)
        sine = jnp.sin(angle)
        rot[n, 0] = jnp.cos(angle)
        rot[n, 1] = jnp.where(c_id == 0, sine, -sine)
    for m in range(3):
        j_id = m * 4 + lane // 32
        shift = jnp.zeros((8, 128), I32)
        for j in range(4 * m, min(4 * m + 4, 9)):
            shift = jnp.where(j_id == j, displacements[j] - 4, shift)
        neg = shift < 0
        k_id = jnp.where(neg, -shift, shift)
        at = z + jnp.where(neg, k_id, 0)
        turns = (mom * (at - src)) & (nz - 1)
        angle = turns.astype(F32) * (2.0 * math.pi / nz)
        cosine = jnp.cos(angle) * scaling
        sine = jnp.sin(angle) * scaling
        kind[m] = k_id
        for rr in range(4):
            s_id = (u_id + rr) % 4
            perm_r = pltpu.roll(perm_t, 8 - rr, 0) if rr else perm_t
            phase_r = pltpu.roll(phase_t, 8 - rr, 0) if rr else phase_t
            match = jnp.where(neg, perm_t, perm_r) == jnp.where(neg, s_id, u_id)
            power = jnp.where(neg, phase_t, phase_r)
            for ri in range(2):
                if ri == 0:
                    turn = jnp.where(c_id == 0, 0, 3)
                else:
                    turn = jnp.where(c_id == 0, jnp.where(neg, 3, 1), jnp.where(neg, 2, 0))
                h = (power + turn) & 3
                value = jnp.where((h & 1) == 1, sine, cosine)
                value = jnp.where(h >= 2, -value, value)
                table[m, rr * 2 + ri] = jnp.where(match & (j_id < 9), value, 0.0)

    @pl.loop(0, 18)
    def _(n):
        rows = sbuf[0, n // 3, pl.ds(pl.multiple_of(n % 3 * 16, 16), 16), :].astype(F32)
        for half in range(2):
            for rr in range(4):
                left[rr, 2 * n + half] = roll4(rows[half * 8 : half * 8 + 8], rr)

    kinds = [kind[m] for m in range(3)]

    def lane_sum(v):
        return jnp.broadcast_to(jnp.sum(v, axis=1, keepdims=True), (8, 128))

    def pick(lines, m):
        value = jnp.zeros((8, 128), F32)
        for k, line in lines.items():
            value = jnp.where(kinds[m] == k, line, value)
        return value

    def turned(total, n):
        rows = jnp.concatenate([jnp.sum(t, axis=0, keepdims=True) for t in total] + [jnp.zeros((1, 128), F32)], axis=0)
        if n is None:
            return rows
        odd = lax.broadcasted_iota(I32, (4, 128), 1) % 2 == 1
        swapped = jnp.where(odd, pltpu.roll(rows, 1, 1), pltpu.roll(rows, 127, 1))
        return rows * rot[n, 0][0:4] + swapped * rot[n, 1][0:4]

    def mac(acc, n, a_pair, b_pair):
        (ar, ai), (br, bi) = a_pair, b_pair
        acc[2 * n] = acc[2 * n] + (ar * br + ai * bi)
        acc[2 * n + 1] = acc[2 * n + 1] + (ar * bi - ai * br)

    total = [[jnp.zeros((8, 128), F32) for _ in range(3)] for _ in range(2)]

    def own_pairs(rr, n, acc):
        acc = list(acc)
        for a in range(3):
            re_at, im_at = n + 6 * a, 18 + n + 6 * a
            mac(acc, 0, (left[rr, re_at], left[rr, im_at]), (left[0, re_at], left[0, im_at]))
        return tuple(acc)

    def regular(kinds_at, add, groups, total):
        for rr in range(4):
            zero = tuple(jnp.zeros((8, 128), F32) for _ in range(2 * len(kinds_at)))
            sums = lax.fori_loop(0, 6, functools.partial(add, rr), zero, unroll=True)
            for ri in range(2):
                lines = {k: lane_sum(sums[2 * n + ri]) for n, k in enumerate(kinds_at)}
                for m in range(3):
                    entry = table[m, rr * 2 + ri]
                    for g, ks in enumerate(groups):
                        if ks:
                            total[g][m] = total[g][m] + entry * pick({k: lines[k] for k in ks}, m)

    regular((0,), own_pairs, ((0,), ()), total)

    def link(ref, slot):
        block = ref[slot].astype(F32)
        return [
            [tuple(jnp.broadcast_to(block[3 * a + b, ri : ri + 1, :], (8, 128)) for ri in range(2)) for b in range(3)]
            for a in range(3)
        ]

    def product(one, two):
        def entry(a, c):
            re = im = None
            for b in range(3):
                (pr, pi), (qr, qi) = one[a][b], two[b][c]
                r2, i2 = pr * qr - pi * qi, pr * qi + pi * qr
                re, im = (r2, i2) if b == 0 else (re + r2, im + i2)
            return re, im

        return [[entry(a, c) for c in range(3)] for a in range(3)]

    def keep(ref, line, matrix, dagger=False):
        for a in range(3):
            for b in range(3):
                re, im = matrix[b][a] if dagger else matrix[a][b]
                ref[line, (a * 3 + b) * 2] = re
                ref[line, (a * 3 + b) * 2 + 1] = -im if dagger else im

    def transport(load, lines, line, store):
        got = [[load(ri * 3 + b) for ri in range(2)] for b in range(3)]
        for half in range(2):
            part = [[v[half * 8 : half * 8 + 8] for v in pair] for pair in got]
            for a in range(3):
                re = im = None
                for b in range(3):
                    if lines is None:
                        re, im = part[a]
                        break
                    wr, wi = lines[line, (a * 3 + b) * 2], lines[line, (a * 3 + b) * 2 + 1]
                    vr, vi = part[b]
                    r2, i2 = wr * vr - wi * vi, wr * vi + wi * vr
                    re, im = (r2, i2) if b == 0 else (re + r2, im + i2)
                store(a, half, re, im)

    def bring(slot, line):
        @pl.loop(0, 3)
        def _(q):
            def load(block):
                return sbuf[slot, block, pl.ds(pl.multiple_of(q * 16, 16), 16), :].astype(F32)

            def store(a, half, re, im):
                fields[line, a * 6 + q * 2 + half] = re
                fields[line, 18 + a * 6 + q * 2 + half] = im

            transport(load, wil, line, store)

    def clear(line):
        @pl.loop(0, 36)
        def _(n):
            fields[line, n] = jnp.zeros((8, 128), F32)

    keep(wil, 0, link(ubuf, 0))
    for n in (3, 4, 5):
        pl.when(comes[n])(halo[n].wait_recv)

    @pl.when(comes[1])
    def _():
        halo[1].wait_recv()
        bring(1, 0)

    @pl.when(comes[0])
    def _():
        keep(wil, 1, product(link(ubuf, 0), link(ubuf, 1)))
        halo[0].wait_recv()
        bring(2, 1)

    for line, n in ((0, 1), (1, 0)):
        @pl.when(jnp.logical_not(comes[n]))
        def _():
            clear(line)

    def ahead_pairs(rr, n, acc):
        acc = list(acc)
        for a in range(3):
            re_at, im_at = n + 6 * a, 18 + n + 6 * a
            here = (left[rr, re_at], left[rr, im_at])
            mac(acc, 0, here, (fields[0, re_at], fields[0, im_at]))
            mac(acc, 1, here, (fields[1, re_at], fields[1, im_at]))
        return tuple(acc)

    def behind_pairs(rr, n, acc):
        acc = list(acc)
        for a in range(3):
            re_at, im_at = n + 6 * a, 18 + n + 6 * a
            behind = (roll4(fields[2, re_at], rr), roll4(fields[2, im_at], rr))
            mac(acc, 0, behind, (fields[0, re_at], fields[0, im_at]))
            mac(acc, 1, behind, (fields[1, re_at], fields[1, im_at]))
        return tuple(acc)

    regular((1, 2), ahead_pairs, ((1, 2), ()), total)

    @pl.when(comes[2])
    def _():
        keep(wil, 2, product(link(ubuf, 3), link(ubuf, 2)), dagger=True)
        halo[2].wait_recv()
        bring(3, 2)

    pl.when(jnp.logical_not(comes[2]))(lambda: clear(2))
    regular((3, 4), behind_pairs, ((), (3, 4)), total)
    mine[...] = turned(total[0], None) + turned(total[1], 4)

    @pl.when(is_worker)
    def _():
        def bring_cross(n, line):
            def load(block):
                return xbuf[n, block].astype(F32)

            def store(a, half, re, im):
                xfields[n, a * 2 + half] = re
                xfields[n, 6 + a * 2 + half] = im

            transport(load, None if line is None else xwil, line, store)

        bulk(xlink.at[pl.ds(0, 4)], recv_l.at[0]).wait_recv()
        line = link(xlink, 3)
        keep(xwil, 3, line, dagger=True)
        for n in (2, 1, 0):
            line = product(link(xlink, n), line)
            keep(xwil, n, line, dagger=True)
        bulk(xbuf.at[pl.ds(0, 4)], recv_x.at[0]).wait_recv()
        for n in range(4):
            bring_cross(n, n)
        bulk(xlink.at[pl.ds(4, 4)], recv_l.at[1]).wait_recv()
        line = link(xlink, 4)
        keep(xwil, 4, line)
        for n in (5, 6):
            line = product(line, link(xlink, n))
            keep(xwil, n, line)
        bulk(xbuf.at[pl.ds(4, 4)], recv_x.at[1]).wait_recv()
        for n in range(4, 8):
            bring_cross(n, None if n == 4 else n - 1)

        cross = [(i, j) for i in range(4) for j in range(i + 1)]
        total = [[jnp.zeros((8, 128), F32) for _ in range(3)] for _ in range(4)]
        for rr in range(4):
            def add(n, acc):
                acc = list(acc)
                ahead = [(xfields[4 + j, n], xfields[4 + j, 6 + n]) for j in range(4)]
                for i in range(4):
                    behind = (roll4(xfields[i, n], rr), roll4(xfields[i, 6 + n], rr))
                    for j in range(i + 1):
                        mac(acc, cross.index((i, j)), behind, ahead[j])
                return tuple(acc)

            sums = lax.fori_loop(0, 6, add, tuple(jnp.zeros((8, 128), F32) for _ in range(20)), unroll=True)
            for ri in range(2):
                lines = [lane_sum(sums[2 * n + ri]) for n in range(10)]
                for m in range(3):
                    entry = table[m, rr * 2 + ri]
                    for i in range(4):
                        at_k = {4 - i + j: lines[cross.index((i, j))] for j in range(i + 1)}
                        total[i][m] = total[i][m] + entry * pick(at_k, m)
        mine[...] = mine[...] + ((turned(total[0], 0) + turned(total[1], 1)) + (turned(total[2], 2) + turned(total[3], 3)))

    def to_centre():
        return pltpu.make_async_remote_copy(
            src_ref=mine, dst_ref=slot_b.at[chip * 2 + core], send_sem=send_b, recv_sem=recv_b,
            device_id={"gy": 0, "gz_1": 0, "gz_2": 1}, device_id_type=MESH,
        )

    def to_plane(n):
        return pltpu.make_async_remote_copy(
            src_ref=sum_b, dst_ref=slot_c.at[column], send_sem=send_c, recv_sem=recv_c,
            device_id={"ta": n // 4, "gz_0": n % 4}, device_id_type=MESH,
        )

    def to_chip(dst, side):
        return pltpu.make_async_remote_copy(
            src_ref=final.at[0], dst_ref=final.at[0], send_sem=send_d, recv_sem=recv_d,
            device_id={"gy": dst // 8, "gz_1": dst % 8, "gz_2": side}, device_id_type=MESH,
        )

    outward = [(0, 0)] + [(c, side) for c in (1, 2, 3, 4, 24, 8, 16) for side in (0, 1)]
    heads = [(chip == 4, 4), ((chip == 8) | (chip == 16) | (chip == 24), 8)]

    @pl.when(jnp.logical_not(is_centre))
    def _():
        to_centre().start()
        to_chip(0, 1).wait_recv()

        for is_head, end in heads:
            @pl.when(is_head)
            def _():
                for n in range(1, end):
                    to_chip(chip + n, core).start()

    @pl.when(is_centre)
    def _():
        acc = mine[...]
        bulk(slot_b.at[pl.ds(0, 63)], recv_b).wait_recv()
        for n in range(64):
            if n != 1:
                acc = acc + slot_b[n]
        sum_b[...] = acc

        for n in range(16):
            pl.when(column != n)(to_plane(n).start)
        slot_c[column] = acc
        bulk(slot_c.at[pl.ds(0, 15)], recv_c).wait_recv()
        slices = []
        for t in range(4):
            acc = slot_c[4 * t]
            for q in range(1, 4):
                acc = acc + slot_c[4 * t + q]
            slices.append(acc)
        quarter = lax.broadcasted_iota(I32, (4, 128), 1) // 32
        for q in range(4):
            rows = slices[0] if q == 0 else pltpu.roll(slices[0], (128 - 32 * q) % 128, 1)
            for t in range(1, 4):
                turned = slices[t] if t == q else pltpu.roll(slices[t], (128 + 32 * (t - q)) % 128, 1)
                rows = jnp.where(quarter == t, turned, rows)
            for m in range(3):
                if m * 4 + q < 9:
                    final[0, m * 4 + q] = rows[m : m + 1, :]
        for dst, side in outward:
            to_chip(dst, side).start()

    for j in range(9):
        out[j : j + 1, :] = final[0, j]

    for n in range(6):
        pl.when(goes[n])(halo[n].wait_send)
    @pl.when(is_member)
    def _():
        bulk(sbuf.at[0], send_x.at[0]).wait_send()
        bulk(ubuf.at[pl.ds(0, 3)], send_x.at[1]).wait_send()

    @pl.when(jnp.logical_not(is_centre))
    def _():
        to_centre().wait_send()

        for is_head, end in heads:
            @pl.when(is_head)
            def _():
                bulk(final.at[pl.ds(0, end - 1)], send_d).wait_send()

    @pl.when(is_centre)
    def _():
        bulk(slot_c.at[pl.ds(0, 15)], send_c).wait_send()
        bulk(final, send_d).wait_send()


def body(propagator, links, source_z, displacements, momenta, gamma_perm, gamma_phase):
    nz = lax.axis_size(GZ)
    sites_total = propagator.shape[6] * lax.axis_size("gy") * nz
    scaling = 1.0 / (24.0 * math.sqrt(sites_total))
    prop = jnp.transpose(propagator, (0, 2, 3, 1, 4, 5, 6)).reshape(6, 48, 128)
    link = jnp.transpose(links, (1, 2, 0, 3, 4, 5)).reshape(9, 2, 128)
    hbm = pl.BlockSpec(memory_space=pl.ANY)
    dma = pltpu.SemaphoreType.DMA
    out = pl.pallas_call(
        functools.partial(kernel, nz, scaling),
        out_shape=jax.ShapeDtypeStruct((9, 128), F32),
        in_specs=[hbm] * 7,
        out_specs=pl.BlockSpec(memory_space=pltpu.VMEM),
        scratch_shapes=[
            pltpu.SMEM((4, 4), I32),
            pltpu.SMEM((9,), I32),
            pltpu.SMEM((4,), I32),
            pltpu.SMEM((4, 4), I32),
            pltpu.SMEM((4, 4), I32),
            pltpu.VMEM((4, 6, 48, 128), jnp.bfloat16),
            pltpu.VMEM((4, 9, 2, 128), jnp.bfloat16),
            pltpu.VMEM((4, 36, 8, 128), F32),
            pltpu.VMEM((3, 36, 8, 128), F32),
            pltpu.VMEM((3, 18, 8, 128), F32),
            pltpu.VMEM((3, 8, 8, 128), F32),
            pltpu.VMEM((3, 8, 128), I32),
            pltpu.VMEM((4, 128), F32),
            pltpu.VMEM((64, 4, 128), F32),
            pltpu.VMEM((4, 128), F32),
            pltpu.VMEM((16, 4, 128), F32),
            pltpu.VMEM((15, 9, 1, 128), F32),
            pltpu.VMEM((8, 6, 16, 128), jnp.bfloat16),
            pltpu.VMEM((8, 9, 2, 128), jnp.bfloat16),
            pltpu.VMEM((8, 12, 8, 128), F32),
            pltpu.VMEM((7, 18, 8, 128), F32),
            pltpu.VMEM((5, 2, 8, 128), F32),
            dma((7,)),
            dma((6,)),
            dma((6,)),
            dma,
            dma,
            dma,
            dma,
            dma,
            dma,
            dma((2,)),
            dma((2,)),
            dma((2,)),
        ],
        compiler_params=pltpu.CompilerParams(collective_id=0, has_side_effects=True),
    )(prop, link, source_z, displacements, momenta, gamma_perm, gamma_phase)
    return jnp.transpose(out.reshape(9, 4, 4, 4, 2), (1, 0, 2, 3, 4))


def solution(mesh):
    torus = Mesh(
        mesh.devices.reshape(mesh.shape["ta"], 4, 8, 2, mesh.shape["gy"]),
        ("ta", "gz_0", "gz_1", "gz_2", "gy"),
    )
    in_specs = (
        P(None, None, None, None, "ta", GZ, "gy"),
        P(None, None, None, "ta", GZ, "gy"),
        P(),
        P(),
        P(),
        P(),
        P(),
    )
    return jax.shard_map(body, mesh=torus, in_specs=in_specs, out_specs=P(), check_vma=False)
```
